32 devices in a mesh: ctx: 8 (over y, x, core), tp: 4 (over z).
Axes of the slice: x: 2, y: 2, z: 4, core: 2. Of those that a mesh axis runs over, the one named last changes fastest.
Arguments:
- tokens: bfloat16 [4096, 768], P('ctx'), may hold values from -6 to 6
- cotangent: bfloat16 [4096, 768], P('ctx'), may hold values from -8 to 8
- block_pos: int32 [32], replicated, may hold values from 0 to 15, as said below
- block_seq: int32 [32], replicated, may hold values from 0 to 1, as said below
- ln1_gain: float32 [768], replicated, may hold values from 0.5 to 1.5
- ln1_bias: float32 [768], replicated, may hold values from -1.2 to 1.2
- qkv_weight: bfloat16 [768, 3, 768], P(None, None, 'tp'), may hold values from -5 to 5
- qv_bias: float32 [2, 768], P(None, 'tp'), may hold values from -2.5 to 2.5
- out_weight: bfloat16 [768, 768], P('tp'), may hold values from -6 to 6
- out_bias: float32 [768], replicated, may hold values from -1.2 to 1.2
- ln2_gain: float32 [768], replicated, may hold values from 0.5 to 1.5
- ln2_bias: float32 [768], replicated, may hold values from -1.2 to 1.2
- fc_weight: bfloat16 [768, 3072], P(None, 'tp'), may hold values from -0.4375 to 0.4375
- fc_bias: float32 [3072], P('tp'), may hold values from -2.5 to 2.5
- proj_weight: bfloat16 [3072, 768], P('tp'), may hold values from -0.21875 to 0.21875
- proj_bias: float32 [768], replicated, may hold values from -1.2 to 1.2
Outputs:
- output: bfloat16 [4096, 768], P('ctx')
- grad_tokens: bfloat16 [4096, 768], P('ctx')
- grad_ln1_gain: float32 [768], replicated
- grad_ln1_bias: float32 [768], replicated
- grad_qkv_weight: float32 [768, 3, 768], P(None, None, 'tp')
- grad_qv_bias: float32 [2, 768], P(None, 'tp')
- grad_out_weight: float32 [768, 768], P('tp')
- grad_out_bias: float32 [768], replicated
- grad_ln2_gain: float32 [768], replicated
- grad_ln2_bias: float32 [768], replicated
- grad_fc_weight: float32 [768, 3072], P(None, 'tp')
- grad_fc_bias: float32 [3072], P('tp')
- grad_proj_weight: float32 [3072, 768], P('tp')
- grad_proj_bias: float32 [768], replicated
The draws below stay inside these ranges and needn't reach their ends.
Inputs may be any that keep to these rules, and one draw needn't show every extreme that they name: `block_pos`: block b holds tokens [b * 128, (b+1) * 128) of the whole; each index r of ctx holds blocks 4r to 4r+3, two of each sequence, at positions p and 15 - p; every position of each sequence is held by exactly one block. `block_seq`: two sequences; each index of ctx holds two blocks of each.
All inputs are finite; a program needn't handle non-finite values.
Results may differ from the reference program's by a relative error of at most 0.025.
Values may be sent and summed in bfloat16 or wider, within the bound.
A program may use at most 320 MiB of HBM per device.

```python
import math
import jax
import jax.numpy as jnp
from jax import lax

D = 768
HEADS = 12
HEAD = 64
FF = 3072
BLK = 128
NBLK = 32
TOKENS = 4096


def placement_tables(key):
    devices = NBLK // 4
    base = jax.random.fold_in(key, 7)
    first_perm = jax.random.permutation(jax.random.fold_in(base, 1), devices)
    second_perm = jax.random.permutation(jax.random.fold_in(base, 2), devices)
    coin = jax.random.randint(jax.random.fold_in(base, 3), (devices,), 0, 2)
    swapped = jax.random.randint(jax.random.fold_in(base, 4), (devices, 2), 0, 2)
    seq_slots = jnp.stack([coin, coin, 1 - coin, 1 - coin], axis=1)
    base_pos = jnp.where(seq_slots == 0, first_perm[:, None], second_perm[:, None])
    flips = jnp.where(seq_slots == 0, swapped[:, 0:1], swapped[:, 1:2])
    second = (jnp.arange(4, dtype=jnp.int32)[None, :] + flips) % 2
    positions = jnp.where(second == 1, 2 * devices - 1 - base_pos, base_pos)
    return (positions.reshape(-1).astype(jnp.int32), seq_slots.reshape(-1).astype(jnp.int32))


def draw_block_pos(key, part):
    return placement_tables(key)[0]


def draw_block_seq(key, part):
    return placement_tables(key)[1]


def draw_cotangent(key, part):
    rows = jnp.arange(TOKENS, dtype=jnp.float32)
    ramp = (0.5 + rows / TOKENS)[:, None]
    values = ramp * jnp.clip(jax.random.normal(key, (TOKENS, D), jnp.float32), -5.0, 5.0)
    return values.astype(jnp.bfloat16)


def draw_qkv_weight(key, part):
    scale_down = 1.0 / jnp.sqrt(jnp.float32(D))
    raw = jnp.clip(jax.random.normal(key, (D, 3, D), jnp.float32), -6.0, 6.0) * scale_down
    return raw.astype(jnp.bfloat16)


def draw_qv_bias(key, part):
    raw = jnp.clip(jax.random.normal(key, (2, D), jnp.float32), -5.0, 5.0)
    factors = jnp.array([0.5, 0.05], dtype=jnp.float32)[:, None]
    return raw * factors


def level_of(stream_key, extent, split, smallest, high):
    level = 1.0
    for axis_at, parts in split:
        steps = jax.random.uniform(jax.random.fold_in(jax.random.fold_in(stream_key, 6), axis_at), (parts,), jnp.float32, smallest / len(split), high / len(split))
        level = level * jnp.repeat(jnp.exp(steps), extent[axis_at] // parts).reshape((-1,) + (1,) * (len(extent) - 1 - axis_at))
    return level


def centred(key, dims, scale, most, pieces=(), kind=jnp.bfloat16):
    level = level_of(key, dims, pieces, -0.22, 0.18) if pieces else 1.0
    values = jax.random.normal(key, dims, jnp.float32) * scale * level
    return jnp.minimum(jnp.maximum(values, -most), most).astype(kind)


def setup_inputs(seed: int = 0) -> dict:
    arg_keys = jax.random.split(jax.random.key(seed), 17)
    return {
        "tokens": centred(arg_keys[0], (TOKENS, D), 1.0, 6.0, ((0, 8),)),
        "cotangent": draw_cotangent(jax.random.fold_in(arg_keys[16], 71), 0),
        "block_pos": draw_block_pos(jax.random.fold_in(arg_keys[16], 71), 0),
        "block_seq": draw_block_seq(jax.random.fold_in(arg_keys[16], 71), 0),
        "ln1_gain": jnp.clip(1.0 + 0.1 * jax.random.normal(arg_keys[4], (D,), jnp.float32), 0.5, 1.5),
        "ln1_bias": centred(arg_keys[5], (D,), 0.3, 1.2, (), jnp.float32),
        "qkv_weight": draw_qkv_weight(jax.random.fold_in(arg_keys[16], 71), 0),
        "qv_bias": draw_qv_bias(jax.random.fold_in(arg_keys[16], 71), 0),
        "out_weight": centred(arg_keys[8], (D, D), 1 ** -0.5, 6.0, ((0, 4),)),
        "out_bias": centred(arg_keys[9], (D,), 0.3, 1.2, (), jnp.float32),
        "ln2_gain": jnp.clip(1.0 + 0.1 * jax.random.normal(arg_keys[10], (D,), jnp.float32), 0.5, 1.5),
        "ln2_bias": centred(arg_keys[11], (D,), 0.3, 1.2, (), jnp.float32),
        "fc_weight": centred(arg_keys[12], (D, FF), (D // 4) ** -0.5, 0.4375, ((1, 4),)),
        "fc_bias": centred(arg_keys[13], (FF,), 0.5, 2.5, ((0, 4),), jnp.float32),
        "proj_weight": centred(arg_keys[14], (FF, D), (FF // 4) ** -0.5, 0.21875, ((0, 4),)),
        "proj_bias": centred(arg_keys[15], (D,), 0.3, 1.2, (), jnp.float32),
    }


def layer_norm(values, gain, bias):
    centre = lax.optimization_barrier(jnp.mean(values, axis=-1, keepdims=True))
    shifted = values - centre
    spread = lax.optimization_barrier(jnp.mean(shifted * shifted, axis=-1, keepdims=True))
    inverse = lax.rsqrt(spread + 1e-05)
    normed = shifted * inverse
    return (normed, inverse, normed * gain + bias)

def norm_back(grad_normed, normed, inverse):
    first = lax.optimization_barrier(jnp.mean(grad_normed, axis=-1, keepdims=True))
    second = lax.optimization_barrier(jnp.mean(grad_normed * normed, axis=-1, keepdims=True))
    return inverse * (grad_normed - first - normed * second)

def gelu_tanh(values):
    return 0.5 * values * (1.0 + jnp.tanh(0.7978845608028654 * (values + 0.044715 * values * values * values)))

def gelu_back(values, upstream):
    return jax.vjp(gelu_tanh, values)[1](upstream)[0]

def rounded(values):
    return lax.optimization_barrier(values.astype(jnp.bfloat16)).astype(jnp.float32)

def reference(tokens, cotangent, block_pos, block_seq, ln1_gain, ln1_bias, qkv_weight, qv_bias, out_weight, out_bias, ln2_gain, ln2_bias, fc_weight, fc_bias, proj_weight, proj_bias):
    inputs = tokens.astype(jnp.float32)
    rows = jnp.arange(TOKENS, dtype=jnp.int32)
    block_index = rows // BLK
    positions = (jnp.take(block_pos, block_index) * BLK + rows % BLK).astype(jnp.int32)
    sequences = jnp.take(block_seq, block_index).astype(jnp.int32)
    normed1, inverse1, scaled1 = layer_norm(inputs, ln1_gain, ln1_bias)
    act1 = scaled1.astype(jnp.bfloat16)
    flat_qkv = qkv_weight.reshape(D, 3 * D)
    projected = jnp.dot(act1, flat_qkv, preferred_element_type=jnp.float32).reshape(TOKENS, 3, D)
    queries = ((projected[:, 0] + qv_bias[0]) * 0.125).astype(jnp.bfloat16).reshape(TOKENS, HEADS, HEAD)
    keys = projected[:, 1].astype(jnp.bfloat16).reshape(TOKENS, HEADS, HEAD)
    values = (projected[:, 2] + qv_bias[1]).astype(jnp.bfloat16).reshape(TOKENS, HEADS, HEAD)
    key_wide = keys.astype(jnp.float32)
    value_wide = values.astype(jnp.float32)
    block = math.gcd(256, TOKENS)
    count = TOKENS // block

    def visible_block(first):
        query_pos = lax.dynamic_slice_in_dim(positions, first, block)
        query_seq = lax.dynamic_slice_in_dim(sequences, first, block)
        return ((sequences[None, :] == query_seq[:, None]) & (positions[None, :] <= query_pos[:, None]))[None]

    def forward_block(index):
        first = (index * block).astype(jnp.int32)
        query_wide = lax.dynamic_slice_in_dim(queries, first, block).astype(jnp.float32)
        visible = visible_block(first)
        scores = jnp.where(visible, jnp.einsum('qhd,khd->hqk', query_wide, key_wide), -1e+30)
        highest = lax.optimization_barrier(jnp.max(scores, axis=-1))
        weights = jnp.where(visible, jnp.exp(scores - highest[..., None]), 0.0)
        totals = lax.optimization_barrier(jnp.sum(weights, axis=-1))
        mixed = jnp.einsum('hqk,khd->qhd', rounded(weights), value_wide) / totals.T[:, :, None]
        return (mixed.astype(jnp.bfloat16), highest + jnp.log(totals))
    attended_blocks, log_blocks = lax.map(forward_block, jnp.arange(count, dtype=jnp.int32))
    attended = attended_blocks.reshape(TOKENS, D)
    hidden1 = inputs + jnp.dot(attended, out_weight, preferred_element_type=jnp.float32) + out_bias
    normed2, inverse2, scaled2 = layer_norm(hidden1, ln2_gain, ln2_bias)
    act2 = scaled2.astype(jnp.bfloat16)
    pre_gelu = jnp.dot(act2, fc_weight, preferred_element_type=jnp.float32) + fc_bias
    activated = gelu_tanh(pre_gelu).astype(jnp.bfloat16)
    output = (hidden1 + jnp.dot(activated, proj_weight, preferred_element_type=jnp.float32) + proj_bias).astype(jnp.bfloat16)
    upstream = cotangent.astype(jnp.float32)
    grad_proj_bias = lax.optimization_barrier(jnp.sum(upstream, axis=0))
    grad_proj_weight = jnp.dot(activated.T, cotangent, preferred_element_type=jnp.float32)
    grad_act = jnp.dot(cotangent, proj_weight.T, preferred_element_type=jnp.float32)
    grad_pre_wide = gelu_back(pre_gelu, grad_act)
    grad_pre = grad_pre_wide.astype(jnp.bfloat16)
    grad_fc_weight = jnp.dot(act2.T, grad_pre, preferred_element_type=jnp.float32)
    grad_fc_bias = lax.optimization_barrier(jnp.sum(grad_pre_wide, axis=0))
    grad_scaled2 = jnp.dot(grad_pre, fc_weight.T, preferred_element_type=jnp.float32)
    grad_ln2_gain = lax.optimization_barrier(jnp.sum(grad_scaled2 * normed2, axis=0))
    grad_ln2_bias = lax.optimization_barrier(jnp.sum(grad_scaled2, axis=0))
    grad_hidden1 = upstream + norm_back(grad_scaled2 * ln2_gain, normed2, inverse2)
    hidden_half = grad_hidden1.astype(jnp.bfloat16)
    grad_out_bias = lax.optimization_barrier(jnp.sum(grad_hidden1, axis=0))
    grad_out_weight = jnp.dot(attended.T, hidden_half, preferred_element_type=jnp.float32)
    grad_attended = jnp.dot(hidden_half, out_weight.T, preferred_element_type=jnp.float32).astype(jnp.bfloat16)
    grad_heads = grad_attended.reshape(TOKENS, HEADS, HEAD)
    delta_rows = lax.optimization_barrier(jnp.sum(grad_heads.astype(jnp.float32) * attended.reshape(TOKENS, HEADS, HEAD).astype(jnp.float32), axis=-1))

    def backward_block(carried, index):
        grad_keys, grad_values = carried
        first = (index * block).astype(jnp.int32)
        query_wide = lax.dynamic_slice_in_dim(queries, first, block).astype(jnp.float32)
        grad_block = lax.dynamic_slice_in_dim(grad_heads, first, block).astype(jnp.float32)
        delta_block = lax.dynamic_slice_in_dim(delta_rows, first, block).T
        log_total = log_blocks[index]
        visible = visible_block(first)
        scores = jnp.where(visible, jnp.einsum('qhd,khd->hqk', query_wide, key_wide), -1e+30)
        probs = jnp.where(visible, jnp.exp(scores - log_total[..., None]), 0.0)
        grad_probs = jnp.einsum('qhd,khd->hqk', grad_block, value_wide)
        grad_scores = probs * (grad_probs - delta_block[..., None])
        scores_half = rounded(grad_scores)
        grad_query = jnp.einsum('hqk,khd->qhd', scores_half, key_wide)
        grad_keys = grad_keys + jnp.einsum('hqk,qhd->khd', scores_half, query_wide)
        grad_values = grad_values + jnp.einsum('hqk,qhd->khd', rounded(probs), grad_block)
        return ((grad_keys, grad_values), grad_query)
    empty = jnp.zeros((TOKENS, HEADS, HEAD), jnp.float32)
    (grad_keys, grad_values), grad_query_blocks = lax.scan(backward_block, (empty, empty), jnp.arange(count, dtype=jnp.int32))
    grad_queries = grad_query_blocks.reshape(TOKENS, D) * 0.125
    grad_keys = grad_keys.reshape(TOKENS, D)
    grad_values = grad_values.reshape(TOKENS, D)
    grad_qv_bias = jnp.stack([lax.optimization_barrier(jnp.sum(grad_queries, axis=0)), lax.optimization_barrier(jnp.sum(grad_values, axis=0))])
    grad_all = jnp.stack([grad_queries, grad_keys, grad_values], axis=1).reshape(TOKENS, 3 * D).astype(jnp.bfloat16)
    grad_qkv_weight = jnp.dot(act1.T, grad_all, preferred_element_type=jnp.float32).reshape(D, 3, D)
    grad_scaled1 = jnp.dot(grad_all, flat_qkv.T, preferred_element_type=jnp.float32)
    grad_ln1_gain = lax.optimization_barrier(jnp.sum(grad_scaled1 * normed1, axis=0))
    grad_ln1_bias = lax.optimization_barrier(jnp.sum(grad_scaled1, axis=0))
    grad_tokens = (grad_hidden1 + norm_back(grad_scaled1 * ln1_gain, normed1, inverse1)).astype(jnp.bfloat16)
    return (output, grad_tokens, grad_ln1_gain, grad_ln1_bias, grad_qkv_weight, grad_qv_bias, grad_out_weight, grad_out_bias, grad_ln2_gain, grad_ln2_bias, grad_fc_weight, grad_fc_bias, grad_proj_weight, grad_proj_bias)
```

```python
import functools
from types import SimpleNamespace

import jax
import jax.numpy as jnp
from jax import lax
from jax.experimental import pallas as pl
from jax.experimental.pallas import tpu as pltpu
from jax.sharding import PartitionSpec as P

HEAD = 64
BLK = 128
BF = jnp.bfloat16
F32 = jnp.float32
MESH = pl.DeviceIdType.MESH
NEG = -1e30
C0 = 0.7978845608028654
C1 = 0.044715


def dg(a, b, ca, cb):
    return lax.dot_general(a, b, (((ca,), (cb,)), ((), ())), preferred_element_type=F32)


def normed(x):
    centre = jnp.mean(x, axis=-1, keepdims=True)
    shifted = x - centre
    spread = jnp.mean(shifted * shifted, axis=-1, keepdims=True)
    inverse = lax.rsqrt(spread + 1e-05)
    return shifted * inverse, inverse


def fold8(x):
    rows, width = x.shape
    return jnp.sum(x.reshape(rows // 8, 8, width), axis=0)


def roll64(x):
    return pltpu.roll(x, 64, 1)


def scratch_list(R, T, D, F, nh):
    NG = R // 2
    N = 4 * BLK
    v = pltpu.VMEM
    out = [
        ("tok_raw", v((4, BLK, D), BF)),
        ("cot_raw", v((4, BLK, D), BF)),
        ("stage", v((2, 2, BLK, D), BF)),
        ("x", v((4, BLK, D), BF)),
        ("cot", v((4, BLK, D), BF)),
        ("wqt", v((640, D), BF)),
        ("wo", v((T, nh * HEAD, D), BF)),
        ("wolo", v((T, BLK, D), BF)),
        ("wohi", v((T, BLK, D), BF)),
        ("wopad", v((nh * BLK, D), BF)),
        ("fc", v((D, F), BF)),
        ("pw", v((F, D), BF)),
        ("brow", v((1, 640), F32)),
        ("act1", v((4, BLK, D), BF)),
        ("q", v((nh, N, 128), BF)),
        ("kv", v((NG, nh, N, 128), BF)),
        ("pre", v((N, D), F32)),
        ("ga", v((N, F), F32)),
        ("hid", v((N, D), F32)),
        ("act2", v((N, D), BF)),
        ("actd", v((N, F), BF)),
        ("gpre", v((N, F), BF)),
        ("mlo", v((256, 256), F32)),
        ("mhi", v((256, 256), F32)),
        ("m", v((2 * nh, 1, 256), F32)),
        ("l", v((2 * nh, 1, 256), F32)),
        ("delta", v((2 * nh, 1, 256), F32)),
        ("acc", v((2 * nh, 128, 256), F32)),
        ("attp", v((nh, N, 128), BF)),
        ("attn", v((N, 256), BF)),
        ("ab", v((T, 768, 128), BF)),
        ("p1", v((4, BLK, D), BF)),
        ("r1", v((4, BLK, D), BF)),
        ("l1", v((4, BLK, D), BF)),
        ("p2", v((4, BLK, D), BF)),
        ("r2", v((4, BLK, D), BF)),
        ("l2", v((4, BLK, D), BF)),
        ("p3", v((4, BLK, D), BF)),
        ("r3", v((4, BLK, D), BF)),
        ("l3", v((4, BLK, D), BF)),
        ("tot", v((BLK, D), F32)),
        ("gh", v((BLK, D), F32)),
        ("h", v((4, BLK, D), BF)),
        ("do", v((nh, N, 128), BF)),
        ("dk", v((NG, nh, N, 128), BF)),
        ("dkr", v((NG, nh, N, 128), BF)),
        ("dka", v((2, nh, 256, 128), BF)),
        ("gn", v((N, 640), BF)),
        ("gt", v((640, N), BF)),
        ("w1", v((2, NG, D // NG, D), BF)),
        ("w1r", v((NG, D // NG, D), BF)),
        ("w1s", v((NG, D // NG, D), BF)),
        ("w1f", v((2, NG, D // NG, D), BF)),
        ("w2", v((2, NG, D // 2 // NG, D), BF)),
        ("w2r", v((NG, D // 2 // NG, D), BF)),
        ("w2s", v((NG, D // 2 // NG, D), BF)),
        ("w2f", v((2, NG, D // 2 // NG, D), BF)),
        ("osh", v((BLK, D), BF)),
        ("gsh", v((BLK, D), BF)),
        ("fo", v((2, 2, BLK, D), BF)),
        ("fg", v((2, 2, BLK, D), BF)),
        ("vsum", v((16, D), F32)),
        ("vz", v((T, 16, D), BF)),
        ("vc", v((R, 16, D), BF)),
        ("ss", pltpu.SemaphoreType.DMA((96 + 16 * NG,))),
        ("rs", pltpu.SemaphoreType.DMA((96 + 16 * NG,))),
        ("ls", pltpu.SemaphoreType.DMA((16,))),
    ]
    return out


def layer_kernel(R, T, D, F, nh, names, *refs):
    (pos_ref, seq_ref, tok_hbm, cot_hbm, g1_ref, b1_ref, wqt_hbm, qvb_ref, wo_hbm, ob_ref, g2_ref,
     b2_ref, fc_hbm, fcb_ref, pw_hbm, pb_ref, w1_out, w2_out, fo_out, fg_out, v_out) = refs[:21]
    s = SimpleNamespace(**dict(zip(names, refs[21:])))
    NG = R // 2
    N = 4 * BLK
    Q1 = D // NG
    Q2 = D // 2 // NG
    r = lax.axis_index("ctx")
    z = lax.axis_index("tp")
    c = lax.rem(r, 2)
    o = 1 - c
    g = lax.div(r, 2)
    mate = 2 * g + o
    if NG == 4:
        ga_ = g + 1 - 2 * lax.rem(g, 2)
        gb_ = g + 2 - 4 * lax.div(g, 2)
        gc_ = ga_ + 2 - 4 * lax.div(ga_, 2)
        peers = [g, ga_, gb_, gc_]
        sources = peers
    else:
        peers = [lax.rem(g + t, NG) for t in range(NG)]
        sources = [lax.rem(g + NG - t, NG) for t in range(NG)]

    pending = []
    ids = [0]

    def new(count=1):
        first = ids[0]
        ids[0] += count
        assert ids[0] <= 96 + 16 * NG
        return first

    def remote(src, dst, slot, dev):
        return pltpu.make_async_remote_copy(
            src_ref=src, dst_ref=dst, send_sem=s.ss.at[slot], recv_sem=s.rs.at[slot],
            device_id=dev, device_id_type=MESH)

    def send(src, dst, slot, dev, cond=None):
        def go():
            remote(src, dst, slot, dev).start()

        def done():
            remote(src, dst, slot, dev).wait_send()

        if cond is None:
            go()
        else:
            pl.when(cond)(go)
        pending.append((cond, done))

    def arrived(dst, slot, cond=None):
        def go():
            remote(dst, dst, slot, (r, z)).wait_recv()

        if cond is None:
            go()
        else:
            pl.when(cond)(go)

    loads = {}

    def load(name, src, dst, k):
        loads[name] = pltpu.make_async_copy(src, dst, s.ls.at[k])
        loads[name].start()

    load("tok", tok_hbm, s.tok_raw, 0)
    load("wqt", wqt_hbm, s.wqt.at[pl.ds(0, 3 * nh * HEAD)], 1)
    load("cot", cot_hbm, s.cot_raw, 2)
    load("wo", wo_hbm, s.wo.at[z], 3)
    load("pw", pw_hbm, s.pw, 4)
    load("fc", fc_hbm, s.fc, 5)

    barrier = pltpu.get_barrier_semaphore()
    for t in range(1, R):
        pl.semaphore_signal(barrier, inc=1, device_id=(lax.rem(r + t, R), z), device_id_type=MESH)
    for t in range(1, T):
        pl.semaphore_signal(barrier, inc=1, device_id=(r, lax.rem(z + t, T)), device_id_type=MESH)
    pl.semaphore_wait(barrier, R - 1 + T - 1)

    def find(seq):
        low = jnp.int32(0)
        high = jnp.int32(0)
        for b in range(4):
            same = seq_ref[4 * r + b] == seq
            first = pos_ref[4 * r + b] < R
            low = jnp.where(same & first, b, low)
            high = jnp.where(same & jnp.logical_not(first), b, high)
        return low, high

    def low_pos(rank):
        total = jnp.int32(0)
        for b in range(4):
            here = (seq_ref[4 * rank + b] == c) & (pos_ref[4 * rank + b] < R)
            total = total + jnp.where(here, pos_ref[4 * rank + b], 0)
        return total

    other = find(o)
    own = find(c)
    q_low = (low_pos(2 * g), low_pos(2 * g + 1))

    sx = new(4)
    loads["tok"].wait()
    for k in range(2):
        s.stage[0, k] = s.tok_raw[other[k]]
        send(s.stage.at[0, k], s.x.at[2 * k + c], sx + k, (mate, z))
    for k in range(2):
        s.x[2 * k + c] = s.tok_raw[own[k]]
    loads["wo"].wait()

    def line_send(buf, at, base, right, left):
        if right is not None:
            send(buf.at[at], buf.at[at], base + right[1], (r, z + 1), right[0])
        if left is not None:
            send(buf.at[at], buf.at[at], base + left[1], (r, z - 1), left[0])

    class Line:
        def __init__(self, buf):
            self.buf = buf
            self.base = new(2 * (T - 1))

        def start(self):
            send(self.buf.at[z], self.buf.at[z], self.base, (r, z + 1), z < T - 1)
            send(self.buf.at[z], self.buf.at[z], self.base + T - 1, (r, z - 1), z > 0)

        def step(self, k):
            left_src = jnp.maximum(z - k, 0)
            right_src = jnp.minimum(z + k, T - 1)
            arrived(self.buf.at[left_src], self.base + k - 1, z >= k)
            if k < T - 1:
                send(self.buf.at[left_src], self.buf.at[left_src], self.base + k, (r, z + 1),
                     (z >= k) & (z < T - 1))
            arrived(self.buf.at[right_src], self.base + T - 1 + k - 1, z <= T - 1 - k)
            if k < T - 1:
                send(self.buf.at[right_src], self.buf.at[right_src], self.base + T - 1 + k,
                     (r, z - 1), (z <= T - 1 - k) & (z > 0))

    class Fold:
        def __init__(self, part, from_left, from_right):
            self.part, self.fl, self.fr = part, from_left, from_right
            self.base = new(2 * T)

        def _one(self, d, buf, slot, to, inner, more):
            def both():
                arrived(buf.at[d], slot)

            pl.when(inner & (more | (z == d)))(both)

            def add():
                self.part[d] = (self.part[d].astype(F32) + buf[d].astype(F32)).astype(BF)

            pl.when(inner & more)(add)
            send(self.part.at[d], buf.at[d], slot, (r, to), inner & more)

        def begin_right(self, d):
            send(self.part.at[d], self.fl.at[d], self.base + d, (r, z + 1), z == 0)

        def begin_left(self, d):
            send(self.part.at[d], self.fr.at[d], self.base + T + d, (r, z - 1), z == T - 1)

        def step(self, j):
            d = T - 1 - j
            self._one(d, self.fl, self.base + d, z + 1, z > 0, z < d)
            self._one(j, self.fr, self.base + T + j, z - 1, z < T - 1, z > j)

        def total(self):
            s.tot[...] = self.part[z].astype(F32)

            @pl.when(z > 0)
            def _():
                s.tot[...] += self.fl[z].astype(F32)

            @pl.when(z < T - 1)
            def _():
                s.tot[...] += self.fr[z].astype(F32)

    class Spread:
        def __init__(self, shard, out):
            self.shard, self.out = shard, out
            self.base = new(9)
            self.half = lax.div(z, 2)
            self.par = lax.rem(z, 2)

        def start(self):
            @pl.when(self.par == c)
            def _():
                self.out[self.half, c] = self.shard[...]

            send(self.shard, self.out.at[self.half, c], self.base + 8, (mate, z), self.par != c)
            for k in range(2):
                self._go(k, 0, z == c + 2 * k)

        def _go(self, k, item, cond):
            src = c + 2 * k
            q = c if item == 0 else o
            blk = self.out.at[k, q]
            send(blk, blk, self.base + 2 * k + item, (r, z + 1), cond & (z >= src) & (z < T - 1))
            send(blk, blk, self.base + 4 + 2 * k + item, (r, z - 1), cond & (z <= src) & (z > 0))

        def swapped(self):
            arrived(self.out.at[self.half, o], self.base + 8, self.par == c)
            for k in range(2):
                self._go(k, 1, z == c + 2 * k)

        def relay(self, k, item):
            src = c + 2 * k
            q = c if item == 0 else o
            arrived(self.out.at[k, q], self.base + 2 * k + item, z > src)
            arrived(self.out.at[k, q], self.base + 4 + 2 * k + item, z < src)
            self._go(k, item, z != src)

    wo_line = Line(s.wo)
    wo_line.start()

    s.wqt[pl.ds(3 * nh * HEAD, 640 - 3 * nh * HEAD), :] = jnp.zeros((640 - 3 * nh * HEAD, D), BF)
    s.brow[...] = jnp.zeros((1, 640), F32)
    s.brow[:, 0:192] = qvb_ref[0:1, :]
    s.brow[:, 384:576] = qvb_ref[1:2, :]
    g1 = g1_ref[...]
    b1 = b1_ref[...]

    def norm1(j):
        def body(i, _):
            rows = pl.ds(pl.multiple_of(i * 32, 32), 32)
            n, _inv = normed(s.x[j, rows, :].astype(F32))
            s.act1[j, rows, :] = (n * g1 + b1).astype(BF)
            return 0

        lax.fori_loop(0, 4, body, 0)

    norm1(c)
    norm1(2 + c)
    for k in range(2):
        arrived(s.x.at[2 * k + o], sx + k)
    norm1(o)
    norm1(2 + o)
    loads["wqt"].wait()
    s.pre[:, 0:640] = dg(s.act1[...].reshape(N, D), s.wqt[...], 1, 1)

    def split(i, _):
        rows = pl.ds(pl.multiple_of(i * 64, 64), 64)
        low = lax.broadcasted_iota(jnp.int32, (64, 128), 1) < HEAD
        t = [s.pre[rows, 128 * j:128 * (j + 1)] + s.brow[:, 128 * j:128 * (j + 1)] for j in range(5)]
        zero = jnp.zeros((64, 128), F32)
        s.q[0, rows, :] = (jnp.where(low, t[0], zero) * 0.125).astype(BF)
        s.q[1, rows, :] = (jnp.where(low, roll64(t[0]), zero) * 0.125).astype(BF)
        s.q[2, rows, :] = (jnp.where(low, t[1], zero) * 0.125).astype(BF)
        s.kv[g, 0, rows, :] = jnp.where(low, roll64(t[1]), roll64(t[3])).astype(BF)
        s.kv[g, 1, rows, :] = jnp.where(low, t[2], t[3]).astype(BF)
        s.kv[g, 2, rows, :] = jnp.where(low, roll64(t[2]), roll64(t[4])).astype(BF)
        return 0

    lax.fori_loop(0, 8, split, 0)

    half_a = pl.ds(0, 256)
    half_b = pl.ds(256, 256)
    skv = new(NG + 1)
    direct = [1, 2] if NG == 4 else list(range(1, NG))
    for t in direct:
        send(s.kv.at[g], s.kv.at[g], skv + t, (2 * peers[t] + c, z))

    loads["cot"].wait()
    for k in range(2):
        s.stage[1, k] = s.cot_raw[other[k]]
        send(s.stage.at[1, k], s.cot.at[2 * k + c], sx + 2 + k, (mate, z))
    for k in range(2):
        s.cot[2 * k + c] = s.cot_raw[own[k]]

    for i in range(2 * nh):
        s.m[i] = jnp.full((1, 256), NEG, F32)
        s.l[i] = jnp.zeros((1, 256), F32)
        s.acc[i] = jnp.zeros((128, 256), F32)

    def masks(src):
        k_low = (low_pos(2 * src), low_pos(2 * src + 1))
        i0 = lax.broadcasted_iota(jnp.int32, (256, 256), 0)
        i1 = lax.broadcasted_iota(jnp.int32, (256, 256), 1)

        def token(i, a, b):
            return i + jnp.where(i < BLK, a * BLK, b * BLK - BLK)

        last = 2 * R - 1
        s.mlo[...] = jnp.where(token(i0, *k_low) <= token(i1, *q_low), 0.0, NEG)
        s.mhi[...] = jnp.where(
            token(i0, last - k_low[0], last - k_low[1])
            <= token(i1, last - q_low[0], last - q_low[1]), 0.0, NEG)

    def attend(src):
        masks(src)

        def body(h, _):
            klo = s.kv[src, h, 0:256, :]
            khi = s.kv[src, h, 256:512, :]
            s1 = dg(klo, s.q[h, 0:256, :], 1, 1) + s.mlo[...]
            old = s.m[2 * h]
            now = jnp.maximum(old, jnp.max(s1, axis=0, keepdims=True))
            e1 = jnp.exp(s1 - now)
            f = jnp.exp(old - now)
            s.l[2 * h] = s.l[2 * h] * f + jnp.sum(e1, axis=0, keepdims=True)
            s.acc[2 * h] = s.acc[2 * h] * f + dg(klo, e1.astype(BF), 0, 0)
            s.m[2 * h] = now
            qhi = s.q[h, 256:512, :]
            s2 = dg(klo, qhi, 1, 1)
            s3 = dg(khi, qhi, 1, 1) + s.mhi[...]
            old = s.m[2 * h + 1]
            now = jnp.maximum(old, jnp.maximum(jnp.max(s2, axis=0, keepdims=True),
                                               jnp.max(s3, axis=0, keepdims=True)))
            e2 = jnp.exp(s2 - now)
            e3 = jnp.exp(s3 - now)
            f = jnp.exp(old - now)
            s.l[2 * h + 1] = (s.l[2 * h + 1] * f + jnp.sum(e2, axis=0, keepdims=True)
                              + jnp.sum(e3, axis=0, keepdims=True))
            s.acc[2 * h + 1] = (s.acc[2 * h + 1] * f + dg(klo, e2.astype(BF), 0, 0)
                                + dg(khi, e3.astype(BF), 0, 0))
            s.m[2 * h + 1] = now
            return 0

        lax.fori_loop(0, nh, body, 0)

    attend(g)
    wo_line.step(1)
    if NG == 4:
        arrived(s.kv.at[peers[1]], skv + 1)
        send(s.kv.at[peers[1], :, half_a], s.kv.at[peers[1], :, half_a], skv + 3, (2 * peers[2] + c, z))
        arrived(s.kv.at[peers[2]], skv + 2)
        send(s.kv.at[peers[2], :, half_b], s.kv.at[peers[2], :, half_b], skv + 4, (2 * peers[1] + c, z))
        attend(peers[1])
        wo_line.step(2)
        attend(peers[2])
        wo_line.step(3)
        arrived(s.kv.at[peers[3], :, half_a], skv + 3)
        arrived(s.kv.at[peers[3], :, half_b], skv + 4)
        attend(peers[3])
    else:
        for t in range(1, NG):
            arrived(s.kv.at[sources[t]], skv + t)

        def rest(t, _):
            attend(lax.rem(g + t, NG))
            return 0

        lax.fori_loop(1, NG, rest, 0)
        wo_line.step(2)
        wo_line.step(3)

    low = lax.broadcasted_iota(jnp.int32, (256, 128), 1) < HEAD
    thirds = []
    for half in range(2):
        rows = pl.ds(256 * half, 256)
        outs = []
        for h in range(nh):
            outs.append(jnp.transpose(s.acc[2 * h + half] / s.l[2 * h + half]))
            s.attp[h, rows, :] = outs[h].astype(BF)
            s.m[2 * h + half] = s.m[2 * h + half] + jnp.log(s.l[2 * h + half])
        pair = jnp.where(low, roll64(outs[0]), outs[1]).astype(BF)
        s.ab[z, rows, :] = pair
        s.attn[rows, 0:128] = pair
        turned = roll64(outs[2])
        s.attn[rows, 128:256] = jnp.where(low, turned, 0.0).astype(BF)
        thirds.append((turned, outs[2]))
    s.ab[z, 512:768, :] = jnp.where(low, thirds[0][0], thirds[1][1]).astype(BF)
    ab_line = Line(s.ab)
    ab_line.start()

    for k in range(2):
        arrived(s.cot.at[2 * k + o], sx + 2 + k)
    loads["pw"].wait()
    for half in range(2):
        s.ga[256 * half:256 * half + 256, :] = dg(
            s.cot[2 * half:2 * half + 2].reshape(256, D), s.pw[...], 1, 1)
    s.wopad[...] = jnp.zeros((nh * BLK, D), BF)
    for h in range(nh):
        s.wopad[BLK * h + HEAD:BLK * h + BLK, :] = s.wo[z, HEAD * h:HEAD * h + HEAD, :]
    zeros = jnp.zeros((HEAD, D), BF)
    for t in range(T):
        s.wolo[t, 0:HEAD, :] = s.wo[t, 128:192, :]
        s.wolo[t, HEAD:BLK, :] = zeros
        s.wohi[t, 0:HEAD, :] = zeros
        s.wohi[t, HEAD:BLK, :] = s.wo[t, 128:192, :]
    for k in range(1, T):
        ab_line.step(k)

    left = jnp.concatenate([s.ab[t, 0:512, :] for t in range(T)], axis=1)
    s.hid[...] = dg(left, s.wo[:, 0:128, :].reshape(T * 128, D), 1, 0)
    tail = jnp.concatenate([s.ab[t, 512:768, :] for t in range(T)], axis=1)
    s.hid[0:256, :] += dg(tail, s.wolo[...].reshape(T * 128, D), 1, 0)
    s.hid[256:512, :] += dg(tail, s.wohi[...].reshape(T * 128, D), 1, 0)
    g2 = g2_ref[...]
    b2 = b2_ref[...]
    ob = ob_ref[...]

    def norm2(i, _):
        rows = pl.ds(pl.multiple_of(i * 32, 32), 32)
        j = lax.div(i, 4)
        sub = pl.ds(pl.multiple_of(lax.rem(i, 4) * 32, 32), 32)
        x = s.x[j, sub, :].astype(F32) + s.hid[rows, :] + ob
        s.hid[rows, :] = x
        n, _inv = normed(x)
        s.act2[rows, :] = (n * g2 + b2).astype(BF)
        return 0

    lax.fori_loop(0, 16, norm2, 0)

    loads["fc"].wait()
    fcb = fcb_ref[...]
    fold1 = Fold(s.p1, s.r1, s.l1)
    fold2 = Fold(s.p2, s.r2, s.l2)
    fold3 = Fold(s.p3, s.r3, s.l3)
    bias_sum = jnp.zeros((8, F), F32)
    for half in range(2):
        base = 256 * half
        s.pre[base:base + 256, :] = dg(s.act2[base:base + 256, :], s.fc[...], 1, 0)

        def gelu(i, total, base=base):
            rows = pl.ds(pl.multiple_of(base + i * 16, 16), 16)
            v = s.pre[rows, :] + fcb
            square = v * v
            th = jnp.tanh(C0 * (v + C1 * square * v))
            one = 1.0 + th
            s.actd[rows, :] = (0.5 * v * one).astype(BF)
            slope = 0.5 * one + (0.5 * v) * (1.0 - th * th) * (C0 * (1.0 + 3.0 * C1 * square))
            grad = slope * s.ga[rows, :]
            s.gpre[rows, :] = grad.astype(BF)
            return total + fold8(grad)

        bias_sum = lax.fori_loop(0, 16, gelu, bias_sum)
        back = dg(s.gpre[base:base + 256, :], s.fc[...], 1, 1)
        s.p1[2 * half] = back[0:128].astype(BF)
        s.p1[2 * half + 1] = back[128:256].astype(BF)
        if half == 0:
            fold1.begin_left(0)
            fold1.begin_left(1)
        else:
            for d in (3, 2):
                fold1.begin_right(d)
            fold1.begin_right(1)
            fold1.begin_left(2)
    s.vsum[...] = jnp.zeros((16, D), F32)
    s.vsum[8:9, :] = jnp.sum(bias_sum, axis=0, keepdims=True)

    sw1 = new(1 + 2 * NG + 1)

    def weight(dst, index, lhs, rhs):
        for i in range(3):
            part = dg(lhs[:, 256 * i:256 * i + 256], rhs, 0, 0).astype(BF)
            lo, hi = 256 * i, 256 * i + 256
            for qd in range(NG):
                a, b = max(lo, qd * Q1), min(hi, qd * Q1 + Q1)
                if a < b:
                    dst[index, qd, a - qd * Q1:b - qd * Q1, :] = part[a - lo:b - lo]

    weight(s.w1, 0, s.actd, s.cot[...].reshape(N, D))
    fold1.step(0)
    weight(s.w1, 1, s.act2, s.gpre[...])
    send(s.w1.at[o], s.w1r, sw1, (mate, z))
    fold1.step(1)
    fold1.step(2)

    fold1.total()
    zrow = pl.multiple_of(z * BLK, BLK)

    def back2(i, sums):
        rows = pl.ds(pl.multiple_of(i * 16, 16), 16)
        n, inv = normed(s.hid[pl.ds(pl.multiple_of(zrow + i * 16, 16), 16), :])
        grad = s.tot[rows, :]
        up = s.cot[z, rows, :].astype(F32)
        qg = grad * g2
        gh = up + inv * (qg - jnp.mean(qg, axis=-1, keepdims=True)
                         - n * jnp.mean(qg * n, axis=-1, keepdims=True))
        s.gh[rows, :] = gh
        s.h[z, rows, :] = gh.astype(BF)
        return (sums[0] + fold8(grad * n), sums[1] + fold8(grad), sums[2] + fold8(gh),
                sums[3] + fold8(up))

    z8 = jnp.zeros((8, D), F32)
    sums = lax.fori_loop(0, 8, back2, (z8, z8, z8, z8))
    h_line = Line(s.h)
    h_line.start()
    for i in range(4):
        s.vsum[2 + i:3 + i, :] = jnp.sum(sums[i], axis=0, keepdims=True)

    for half in range(2):
        base = 256 * half
        fwd = dg(s.actd[base:base + 256, :], s.pw[...], 1, 0)
        s.p2[2 * half] = fwd[0:128].astype(BF)
        s.p2[2 * half + 1] = fwd[128:256].astype(BF)

    def add_into(buf, index, extra):
        def body(i, _):
            buf[index, i] = (buf[index, i].astype(F32) + extra[i].astype(F32)).astype(BF)
            return 0

        lax.fori_loop(0, NG, body, 0)

    arrived(s.w1r, sw1)
    add_into(s.w1, c, s.w1r)
    for t in range(1, NG):
        send(s.w1.at[c, peers[t]], s.w1s.at[t], sw1 + t, (2 * peers[t] + c, z))
    for k in range(1, T):
        h_line.step(k)
    for d in (3, 2, 1):
        fold2.begin_right(d)
        fold2.begin_left(T - 1 - d)

    grads = dg(s.h[...].reshape(N, D), s.wopad[...], 1, 1)
    for h in range(nh):
        s.do[h] = grads[:, 128 * h:128 * h + 128].astype(BF)
    for h in range(nh):
        for half in range(2):
            rows = pl.ds(256 * half, 256)
            both = s.do[h, rows, :].astype(F32) * s.attp[h, rows, :].astype(F32)
            s.delta[2 * h + half] = jnp.sum(jnp.transpose(both), axis=0, keepdims=True)
    for i in range(2 * nh):
        s.acc[i] = jnp.zeros((128, 256), F32)

    def attend_back(src):
        masks(src)

        def body(h, _):
            klo = s.kv[src, h, 0:256, :]
            khi = s.kv[src, h, 256:512, :]

            def tile(k, half, mask):
                qs = s.q[h, 256 * half:256 * half + 256, :]
                ds_ = s.do[h, 256 * half:256 * half + 256, :]
                sc = dg(k, qs, 1, 1)
                if mask is not None:
                    sc = sc + mask[...]
                p = jnp.exp(sc - s.m[2 * h + half])
                d = p * (dg(k, ds_, 1, 1) - s.delta[2 * h + half])
                p = p.astype(BF)
                d = d.astype(BF)
                return d, dg(d, qs, 1, 0) + dg(p, ds_, 1, 0)

            d1, k1 = tile(klo, 0, s.mlo)
            s.acc[2 * h] += dg(klo, d1, 0, 0)
            d2, k2 = tile(klo, 1, None)
            s.dk[src, h, 0:256, :] = (k1 + k2).astype(BF)
            d3, k3 = tile(khi, 1, s.mhi)
            s.dk[src, h, 256:512, :] = k3.astype(BF)
            s.acc[2 * h + 1] += dg(klo, d2, 0, 0) + dg(khi, d3, 0, 0)
            return 0

        lax.fori_loop(0, nh, body, 0)

    sdk = new(NG + 2)

    def w1_gather():
        def body(i, _):
            rows = pl.ds(pl.multiple_of(i * (Q1 // 3), Q1 // 3), Q1 // 3)
            total = s.w1[c, g, rows, :].astype(F32)
            for t in range(1, NG):
                total = total + s.w1s[t, rows, :].astype(F32)
            s.w1f[c, g, rows, :] = total.astype(BF)
            return 0

        for t in range(1, NG):
            arrived(s.w1s.at[t], sw1 + t)
        lax.fori_loop(0, 3, body, 0)
        for t in range(1, NG):
            send(s.w1f.at[c, g], s.w1f.at[c, g], sw1 + NG + t, (2 * peers[t] + c, z))

    spread_o = Spread(s.osh, s.fo)
    pb = pb_ref[...]

    def finish_output():
        fold2.total()

        def body(i, _):
            rows = pl.ds(pl.multiple_of(i * 32, 32), 32)
            y = s.hid[pl.ds(pl.multiple_of(zrow + i * 32, 32), 32), :] + s.tot[rows, :] + pb
            s.osh[rows, :] = y.astype(BF)
            return 0

        lax.fori_loop(0, 4, body, 0)
        spread_o.start()

    if NG == 4:
        attend_back(peers[3])
        send(s.dk.at[peers[3], :, half_a], s.dka.at[0], sdk + 0, (2 * peers[1] + c, z))
        send(s.dk.at[peers[3], :, half_b], s.dka.at[1], sdk + NG, (2 * peers[2] + c, z))
        attend_back(peers[1])
        fold2.step(0)
        w1_gather()
        attend_back(peers[2])
        fold2.step(1)
        arrived(s.dka.at[0], sdk + 0)
        for h in range(nh):
            s.dk[peers[2], h, half_a, :] = (s.dk[peers[2], h, half_a, :].astype(F32)
                                            + s.dka[0, h].astype(F32)).astype(BF)
        send(s.dk.at[peers[2]], s.dkr.at[2], sdk + 2, (2 * peers[2] + c, z))
        arrived(s.dka.at[1], sdk + NG)
        for h in range(nh):
            s.dk[peers[1], h, half_b, :] = (s.dk[peers[1], h, half_b, :].astype(F32)
                                            + s.dka[1, h].astype(F32)).astype(BF)
        send(s.dk.at[peers[1]], s.dkr.at[1], sdk + 1, (2 * peers[1] + c, z))
        attend_back(g)
        fold2.step(2)
        finish_output()
    else:
        def rest_back(t, _):
            attend_back(lax.rem(g + t, NG))
            return 0

        lax.fori_loop(0, NG, rest_back, 0)
        for t in range(1, NG):
            send(s.dk.at[peers[t]], s.dkr.at[t], sdk + t, (2 * peers[t] + c, z))
        w1_gather()
        for j in range(T - 1):
            fold2.step(j)
        finish_output()

    sw2 = new(1 + 2 * NG + 1)

    def put2(first, value, rows):
        for i in range(rows // Q2):
            at = (first + i * Q2) // Q2
            s.w2[at // NG, at % NG] = value[i * Q2:i * Q2 + Q2].astype(BF)

    for half in range(1):
        gout = dg(s.attn[...], s.h[...].reshape(N, D), 0, 0)
        put2(3 * nh * HEAD, gout, nh * HEAD)
    spread_o.swapped()

    got = [1, 2] if NG == 4 else list(range(1, NG))
    for t in got:
        arrived(s.dkr.at[t], sdk + t)
    col = [jnp.zeros((1, 128), F32) for _ in range(5)]
    for half in range(2):
        rows = pl.ds(256 * half, 256)
        dq = [jnp.transpose(s.acc[2 * h + half]) * 0.125 for h in range(nh)]
        dkv = []
        for h in range(nh):
            total = s.dk[g, h, rows, :].astype(F32)
            for t in got:
                total = total + s.dkr[t, h, rows, :].astype(F32)
            dkv.append(total)
        tiles = [
            jnp.where(low, dq[0], roll64(dq[1])),
            jnp.where(low, dq[2], roll64(dkv[0])),
            jnp.where(low, dkv[1], roll64(dkv[2])),
            jnp.where(low, roll64(dkv[0]), dkv[1]),
            jnp.where(low, roll64(dkv[2]), 0.0),
        ]
        for j in range(5):
            col[j] = col[j] + jnp.sum(tiles[j], axis=0, keepdims=True)
            s.gn[rows, 128 * j:128 * j + 128] = tiles[j].astype(BF)
            s.gt[128 * j:128 * j + 128, 256 * half:256 * half + 256] = jnp.transpose(tiles[j]).astype(BF)
    for j in range(5):
        s.vsum[9:10, 128 * j:128 * j + 128] = col[j]

    for half in range(2):
        base = 256 * half
        back = dg(s.gn[base:base + 256, :], s.wqt[...], 1, 0)
        s.p3[2 * half] = back[0:128].astype(BF)
        s.p3[2 * half + 1] = back[128:256].astype(BF)
        if half == 0:
            fold3.begin_left(0)
            fold3.begin_left(1)
        else:
            for d in (3, 2):
                fold3.begin_right(d)
            fold3.begin_right(1)
            fold3.begin_left(2)

    for i in range(3):
        put2(192 * i, dg(s.gt[192 * i:192 * i + 192, :], s.act1[...].reshape(N, D), 1, 0), 192)
    send(s.w2.at[o], s.w2r, sw2, (mate, z))
    fold3.step(0)
    arrived(s.w2r, sw2)
    add_into(s.w2, c, s.w2r)
    for t in range(1, NG):
        send(s.w2.at[c, peers[t]], s.w2s.at[t], sw2 + t, (2 * peers[t] + c, z))
    fold3.step(1)
    fold3.step(2)

    fold3.total()

    def back1(i, sums):
        rows = pl.ds(pl.multiple_of(i * 16, 16), 16)
        n, inv = normed(s.x[z, rows, :].astype(F32))
        grad = s.tot[rows, :]
        qg = grad * g1
        gx = s.gh[rows, :] + inv * (qg - jnp.mean(qg, axis=-1, keepdims=True)
                                    - n * jnp.mean(qg * n, axis=-1, keepdims=True))
        s.gsh[rows, :] = gx.astype(BF)
        return (sums[0] + fold8(grad * n), sums[1] + fold8(grad))

    sums = lax.fori_loop(0, 8, back1, (z8, z8))
    spread_g = Spread(s.gsh, s.fg)
    spread_g.start()
    for i in range(2):
        s.vsum[i:i + 1, :] = jnp.sum(sums[i], axis=0, keepdims=True)

    svz = new(T)
    s.vz[z] = s.vsum[...].astype(BF)
    for t in range(1, T):
        send(s.vz.at[z], s.vz.at[z], svz + t, (r, lax.rem(z + t, T)))

    for k in range(2):
        spread_o.relay(k, 0)
    for k in range(2):
        spread_o.relay(k, 1)
    spread_g.swapped()

    def w2_gather():
        for t in range(1, NG):
            arrived(s.w2s.at[t], sw2 + t)
        total = s.w2[c, g].astype(F32)
        for t in range(1, NG):
            total = total + s.w2s[t].astype(F32)
        s.w2f[c, g] = total.astype(BF)
        for t in range(1, NG):
            send(s.w2f.at[c, g], s.w2f.at[c, g], sw2 + NG + t, (2 * peers[t] + c, z))

    w2_gather()
    for t in range(1, NG):
        arrived(s.w1f.at[c, sources[t]], sw1 + NG + t)
    send(s.w1f.at[c], s.w1f.at[c], sw1 + 2 * NG, (mate, z))

    for t in range(1, T):
        arrived(s.vz.at[lax.rem(z + T - t, T)], svz + t)
    svc = new(R)
    upper = s.vz[0, 0:8, :].astype(F32)
    for t in range(1, T):
        upper = upper + s.vz[t, 0:8, :].astype(F32)
    s.vc[r] = jnp.concatenate([upper, s.vsum[8:16, :]], axis=0).astype(BF)
    for t in range(1, R):
        send(s.vc.at[r], s.vc.at[r], svc + t, (lax.rem(r + t, R), z))

    for k in range(2):
        spread_g.relay(k, 0)
    for k in range(2):
        spread_g.relay(k, 1)
    for t in range(1, NG):
        arrived(s.w2f.at[c, sources[t]], sw2 + NG + t)
    send(s.w2f.at[c], s.w2f.at[c], sw2 + 2 * NG, (mate, z))
    for t in range(1, R):
        arrived(s.vc.at[lax.rem(r + R - t, R)], svc + t)
    total = s.vc[0].astype(F32)
    for t in range(1, R):
        total = total + s.vc[t].astype(F32)
    s.vsum[...] = total
    arrived(s.w1f.at[o], sw1 + 2 * NG)
    outs = [pltpu.make_async_copy(s.fo, fo_out, s.ls.at[6]), pltpu.make_async_copy(s.fg, fg_out, s.ls.at[7]),
            pltpu.make_async_copy(s.w1f, w1_out, s.ls.at[8]), pltpu.make_async_copy(s.vsum, v_out, s.ls.at[10])]
    for copy in outs:
        copy.start()
    arrived(s.w2f.at[o], sw2 + 2 * NG)
    last = pltpu.make_async_copy(s.w2f, w2_out, s.ls.at[9])
    last.start()
    for cond, done in pending:
        if cond is None:
            done()
        else:
            pl.when(cond)(done)
    for copy in outs:
        copy.wait()
    last.wait()


def finish_kernel(R, NS, pos_ref, seq_ref, rank_ref, w1_ref, w2_ref, fo_ref, fg_ref, v_ref, out_ref, gt_ref,
                  ln1g_ref, ln1b_ref, gq_ref, gqv_ref, go_ref, ob_ref, ln2g_ref, ln2b_ref, gf_ref, fb_ref,
                  gp_ref, pb_ref):
    i = pl.program_id(0)
    gp_ref[...] = w1_ref[0].astype(F32)
    gf_ref[...] = w1_ref[1].astype(F32)

    @pl.when(i < 6)
    def _():
        gq_ref[...] = w2_ref[...].astype(F32)

    @pl.when(i >= 6)
    def _():
        go_ref[...] = w2_ref[...].astype(F32)

    @pl.when(i < 4)
    def _():
        b = 4 * rank_ref[0] + i
        high = jnp.where(pos_ref[b] < R, 0, 1)
        out_ref[...] = fo_ref[high, seq_ref[b]]
        gt_ref[...] = fg_ref[high, seq_ref[b]]

    @pl.when(i == 0)
    def _():
        ln1g_ref[...] = v_ref[0:1, :]
        ln1b_ref[...] = v_ref[1:2, :]
        ln2g_ref[...] = v_ref[2:3, :]
        ln2b_ref[...] = v_ref[3:4, :]
        ob_ref[...] = v_ref[4:5, :]
        pb_ref[...] = v_ref[5:6, :]
        fb_ref[...] = v_ref[8:9, :]
        gqv_ref[0:1, :] = v_ref[9:10, 0:192]
        gqv_ref[1:2, :] = v_ref[9:10, 384:576]


def per_device(R, T, tokens, cotangent, block_pos, block_seq, ln1_gain, ln1_bias, qkv_weight, qv_bias,
               out_weight, out_bias, ln2_gain, ln2_bias, fc_weight, fc_bias, proj_weight, proj_bias):
    D = tokens.shape[1]
    F = fc_weight.shape[1]
    local = qkv_weight.shape[2]
    nh = local // HEAD
    NG = R // 2
    sizes = scratch_list(R, T, D, F, nh)
    names = [n for n, _ in sizes]
    row = lambda v: v.reshape(1, -1)
    wqt = jnp.transpose(qkv_weight, (1, 2, 0)).reshape(3 * local, D)
    sm = pl.BlockSpec(memory_space=pltpu.SMEM)
    vm = pl.BlockSpec(memory_space=pltpu.VMEM)
    hb = pl.BlockSpec(memory_space=pl.ANY)
    w1, w2, fo, fg, vs = pl.pallas_call(
        functools.partial(layer_kernel, R, T, D, F, nh, names),
        out_shape=(
            jax.ShapeDtypeStruct((2, NG, D // NG, D), BF),
            jax.ShapeDtypeStruct((2, NG, D // 2 // NG, D), BF),
            jax.ShapeDtypeStruct((2, 2, BLK, D), BF),
            jax.ShapeDtypeStruct((2, 2, BLK, D), BF),
            jax.ShapeDtypeStruct((16, D), F32),
        ),
        in_specs=[sm, sm, hb, hb, vm, vm, hb, vm, hb, vm, vm, vm, hb, vm, hb, vm],
        out_specs=(hb, hb, hb, hb, hb),
        scratch_shapes=[sp for _, sp in sizes],
        compiler_params=pltpu.CompilerParams(
            collective_id=0, has_side_effects=True, vmem_limit_bytes=67043328),
        name="layer",
    )(block_pos, block_seq, tokens.reshape(4, BLK, D), cotangent.reshape(4, BLK, D), row(ln1_gain),
      row(ln1_bias), wqt, qv_bias, out_weight, row(out_bias), row(ln2_gain), row(ln2_bias), fc_weight,
      row(fc_bias), proj_weight, row(proj_bias))

    rank = lax.axis_index("ctx").astype(jnp.int32).reshape(1)
    NS = 8
    rb = D // NS
    whole = lambda *shape: pl.BlockSpec(shape, lambda i: (0,) * len(shape))
    vec = jax.ShapeDtypeStruct((1, D), F32)
    outs = pl.pallas_call(
        functools.partial(finish_kernel, R, NS),
        grid=(NS,),
        out_shape=(
            jax.ShapeDtypeStruct((4 * BLK, D), BF),
            jax.ShapeDtypeStruct((4 * BLK, D), BF),
            vec, vec,
            jax.ShapeDtypeStruct((3 * local, D), F32),
            jax.ShapeDtypeStruct((2, local), F32),
            jax.ShapeDtypeStruct((local, D), F32),
            vec, vec, vec,
            jax.ShapeDtypeStruct((D, F), F32),
            vec,
            jax.ShapeDtypeStruct((F, D), F32),
            vec,
        ),
        in_specs=[sm, sm, sm,
                  pl.BlockSpec((2, rb, D), lambda i: (0, i, 0)),
                  pl.BlockSpec((rb, D), lambda i: (i, 0)),
                  whole(2, 2, BLK, D), whole(2, 2, BLK, D), whole(16, D)],
        out_specs=(
            pl.BlockSpec((BLK, D), lambda i: (jnp.minimum(i, 3), 0)),
            pl.BlockSpec((BLK, D), lambda i: (jnp.minimum(i, 3), 0)),
            whole(1, D), whole(1, D),
            pl.BlockSpec((rb, D), lambda i: (jnp.minimum(i, 5), 0)),
            whole(2, local),
            pl.BlockSpec((rb, D), lambda i: (jnp.maximum(i - 6, 0), 0)),
            whole(1, D), whole(1, D), whole(1, D),
            pl.BlockSpec((rb, F), lambda i: (i, 0)),
            whole(1, F),
            pl.BlockSpec((rb, D), lambda i: (i, 0)),
            whole(1, D),
        ),
        name="finish",
    )(block_pos, block_seq, rank, w1.reshape(2, D, D), w2.reshape(D, D), fo, fg, vs)
    (output, grad_tokens, ln1g, ln1b, gq, gqv, go, ob, ln2g, ln2b, gf, fb, gp, pb) = outs
    flat = lambda v: v.reshape(-1)
    return (output, grad_tokens, flat(ln1g), flat(ln1b),
            jnp.transpose(gq.reshape(3, local, D), (2, 0, 1)), gqv, go, flat(ob), flat(ln2g), flat(ln2b),
            gf, flat(fb), gp, flat(pb))


def solution(mesh):
    R = mesh.shape["ctx"]
    T = mesh.shape["tp"]
    return jax.shard_map(
        functools.partial(per_device, R, T),
        mesh=mesh,
        in_specs=(
            P("ctx", None), P("ctx", None), P(), P(), P(), P(), P(None, None, "tp"), P(None, "tp"),
            P("tp", None), P(), P(), P(), P(None, "tp"), P("tp"), P("tp", None), P(),
        ),
        out_specs=(
            P("ctx", None), P("ctx", None), P(), P(), P(None, None, "tp"), P(None, "tp"), P("tp", None),
            P(), P(), P(), P(None, "tp"), P("tp"), P("tp", None), P(),
        ),
        check_vma=False,
    )
```

```python
import functools
from types import SimpleNamespace

import jax
import jax.numpy as jnp
from jax import lax
from jax.experimental import pallas as pl
from jax.experimental.pallas import tpu as pltpu
from jax.sharding import PartitionSpec as P

HEAD = 64
BLK = 128
BF = jnp.bfloat16
F32 = jnp.float32
MESH = pl.DeviceIdType.MESH
NEG = -1e30
C0 = 0.7978845608028654
C1 = 0.044715
U = 2
SEMS = 160


def dg(a, b, ca, cb):
    return lax.dot_general(a, b, (((ca,), (cb,)), ((), ())), preferred_element_type=F32)


def normed(x):
    centre = jnp.mean(x, axis=-1, keepdims=True)
    shifted = x - centre
    spread = jnp.mean(shifted * shifted, axis=-1, keepdims=True)
    inverse = lax.rsqrt(spread + 1e-05)
    return shifted * inverse, inverse


def fold8(x):
    rows, width = x.shape
    return jnp.sum(x.reshape(rows // 8, 8, width), axis=0)


def roll64(x):
    return pltpu.roll(x, 64, 1)


def scratch_list(R, T, D, F, nh):
    NG = R // 2
    N = 4 * BLK
    v = pltpu.VMEM
    out = [
        ("tok_raw", v((4, BLK, D), BF)),
        ("cot_raw", v((4, BLK, D), BF)),
        ("stage", v((2, 2, BLK, D), BF)),
        ("x", v((4, BLK, D), BF)),
        ("cot", v((4, BLK, D), BF)),
        ("wqt", v((640, D), BF)),
        ("wo", v((T, 2, nh * HEAD // 2, D), BF)),
        ("wolo", v((T, BLK, D), BF)),
        ("wohi", v((T, BLK, D), BF)),
        ("wopad", v((nh * BLK, D), BF)),
        ("fc", v((D, F), BF)),
        ("pw", v((F, D), BF)),
        ("brow", v((1, 640), F32)),
        ("act1", v((4, BLK, D), BF)),
        ("q", v((nh, N, 128), BF)),
        ("kv", v((NG, 4, nh, BLK, 128), BF)),
        ("pre", v((N, D), F32)),
        ("ga", v((N, F), F32)),
        ("hid", v((4, BLK, D), F32)),
        ("act2", v((N, D), BF)),
        ("actd", v((N, F), BF)),
        ("gpre", v((N, F), BF)),
        ("mlo", v((256, 256), F32)),
        ("mhi", v((256, 256), F32)),
        ("m", v((2 * nh, 1, 256), F32)),
        ("l", v((2 * nh, 1, 256), F32)),
        ("delta", v((2 * nh, 1, 256), F32)),
        ("acc", v((2 * nh, 128, 256), F32)),
        ("attp", v((nh, N, 128), BF)),
        ("attn", v((N, 256), BF)),
        ("ab", v((T, 768, 128), BF)),
        ("p1", v((4, BLK, D), BF)),
        ("r1", v((4, BLK, D), BF)),
        ("l1", v((4, BLK, D), BF)),
        ("p2", v((4, BLK, D), BF)),
        ("r2", v((4, BLK, D), BF)),
        ("l2", v((4, BLK, D), BF)),
        ("p3", v((4, BLK, D), BF)),
        ("r3", v((4, BLK, D), BF)),
        ("l3", v((4, BLK, D), BF)),
        ("gh", v((BLK, D), F32)),
        ("h", v((4, BLK, D), BF)),
        ("do", v((nh, N, 128), BF)),
        ("dk", v((NG, nh, N, 128), BF)),
        ("dkr", v((NG, nh, N, 128), BF)),
        ("dka", v((2, nh, 256, 128), BF)),
        ("gn", v((N, 640), BF)),
        ("w1", v((2, NG, D // NG, D), BF)),
        ("w1r", v((NG, D // NG, D), BF)),
        ("w1s", v((NG, D // NG, D), BF)),
        ("w1f", v((2, NG, D // NG, D), BF)),
        ("w2", v((2, NG, D // 2 // NG, D), BF)),
        ("w2r", v((NG, D // 2 // NG, D), BF)),
        ("w2s", v((NG, D // 2 // NG, D), BF)),
        ("w2f", v((2, NG, D // 2 // NG, D), BF)),
        ("yo", v((4, BLK, D), BF)),
        ("yg", v((4, BLK, D), BF)),
        ("mo", v((2, BLK, D), BF)),
        ("mg", v((2, BLK, D), BF)),
        ("vsum", v((16, D), F32)),
        ("vz", v((T, 16, D), BF)),
        ("vc", v((R, 16, D), BF)),
        ("ss", pltpu.SemaphoreType.DMA((SEMS + 16 * NG,))),
        ("rs", pltpu.SemaphoreType.DMA((SEMS + 16 * NG,))),
        ("ls", pltpu.SemaphoreType.DMA((24,))),
    ]
    return out


def layer_kernel(R, T, D, F, nh, names, *refs):
    (pos_ref, seq_ref, tok_hbm, cot_hbm, g1_ref, b1_ref, wqt_hbm, qvb_ref, wo_hbm, ob_ref, g2_ref,
     b2_ref, fc_hbm, fcb_ref, pw_hbm, pb_ref, w1_out, w2_out, fo_out, fg_out, v_out) = refs[:21]
    s = SimpleNamespace(**dict(zip(names, refs[21:])))
    NG = R // 2
    N = 4 * BLK
    Q1 = D // NG
    Q2 = D // 2 // NG
    RU = BLK // U
    r = lax.axis_index("ctx")
    z = lax.axis_index("tp")
    c = lax.rem(r, 2)
    o = 1 - c
    g = lax.div(r, 2)
    mate = 2 * g + o
    if NG == 4:
        ga_ = g + 1 - 2 * lax.rem(g, 2)
        gb_ = g + 2 - 4 * lax.div(g, 2)
        gc_ = ga_ + 2 - 4 * lax.div(ga_, 2)
        peers = [g, ga_, gb_, gc_]
        sources = peers
    else:
        peers = [lax.rem(g + t, NG) for t in range(NG)]
        sources = [lax.rem(g + NG - t, NG) for t in range(NG)]

    pending = []
    ids = [0]

    def new(count=1):
        first = ids[0]
        ids[0] += count
        assert ids[0] <= SEMS + 16 * NG
        return first

    def remote(src, dst, slot, dev):
        return pltpu.make_async_remote_copy(
            src_ref=src, dst_ref=dst, send_sem=s.ss.at[slot], recv_sem=s.rs.at[slot],
            device_id=dev, device_id_type=MESH)

    def send(src, dst, slot, dev, cond=None):
        def go():
            remote(src, dst, slot, dev).start()

        def done():
            remote(src, dst, slot, dev).wait_send()

        if cond is None:
            go()
        else:
            pl.when(cond)(go)
        pending.append((cond, done))

    def arrived(dst, slot, cond=None):
        def go():
            remote(dst, dst, slot, (r, z)).wait_recv()

        if cond is None:
            go()
        else:
            pl.when(cond)(go)

    loads = {}

    def load(name, src, dst, k):
        loads[name] = pltpu.make_async_copy(src, dst, s.ls.at[k])
        loads[name].start()

    load("tok", tok_hbm, s.tok_raw, 0)
    load("wqt", wqt_hbm, s.wqt.at[pl.ds(0, 3 * nh * HEAD)], 1)
    load("wo", wo_hbm, s.wo.at[z], 3)
    load("cot", cot_hbm, s.cot_raw, 2)
    load("pw", pw_hbm, s.pw, 4)
    load("fc", fc_hbm, s.fc, 5)

    barrier = pltpu.get_barrier_semaphore()
    for t in range(1, R):
        pl.semaphore_signal(barrier, inc=1, device_id=(lax.rem(r + t, R), z), device_id_type=MESH)

    @pl.when(z > 0)
    def _():
        pl.semaphore_signal(barrier, inc=1, device_id=(r, z - 1), device_id_type=MESH)

    @pl.when(z < T - 1)
    def _():
        pl.semaphore_signal(barrier, inc=1, device_id=(r, z + 1), device_id_type=MESH)

    sides = lax.div(z + T - 1, T) + lax.div(2 * T - 2 - z, T)
    pl.semaphore_wait(barrier, R - 1 + sides)

    def find(seq):
        low = jnp.int32(0)
        high = jnp.int32(0)
        for b in range(4):
            same = seq_ref[4 * r + b] == seq
            first = pos_ref[4 * r + b] < R
            low = jnp.where(same & first, b, low)
            high = jnp.where(same & jnp.logical_not(first), b, high)
        return low, high

    def low_pos(rank):
        total = jnp.int32(0)
        for b in range(4):
            here = (seq_ref[4 * rank + b] == c) & (pos_ref[4 * rank + b] < R)
            total = total + jnp.where(here, pos_ref[4 * rank + b], 0)
        return total

    other = find(o)
    own = find(c)
    q_low = (low_pos(2 * g), low_pos(2 * g + 1))

    sx = new(4)
    loads["tok"].wait()
    for k in range(2):
        s.stage[0, k] = s.tok_raw[other[k]]
        send(s.stage.at[0, k], s.x.at[2 * k + c], sx + k, (mate, z))
    for k in range(2):
        s.x[2 * k + c] = s.tok_raw[own[k]]

    class Line:
        def __init__(self, at, pieces, seen=None):
            self.at, self.pieces, self.seen = at, pieces, seen
            self.base = [new(2 * (T - 1)) for _ in range(pieces)]

        def start(self, u):
            a, base = self.at(z, u), self.base[u]
            send(a, a, base, (r, z + 1), z < T - 1)
            send(a, a, base + T - 1, (r, z - 1), z > 0)
            if self.seen is not None:
                self.seen(z, u, None)

        def step(self, u, k):
            base = self.base[u]
            a = jnp.maximum(z - k, 0)
            b = jnp.minimum(z + k, T - 1)
            left, right = self.at(a, u), self.at(b, u)
            arrived(left, base + k - 1, z >= k)
            if k < T - 1:
                send(left, left, base + k, (r, z + 1), (z >= k) & (z < T - 1))
            if self.seen is not None:
                self.seen(a, u, z >= k)
            arrived(right, base + T - 1 + k - 1, z <= T - 1 - k)
            if k < T - 1:
                send(right, right, base + T - 1 + k, (r, z - 1), (z <= T - 1 - k) & (z > 0))
            if self.seen is not None:
                self.seen(b, u, z <= T - 1 - k)

    class Sum:
        def __init__(self, part, from_left, from_right):
            self.part, self.fl, self.fr = part, from_left, from_right
            self.base = [new(2 * T) for _ in range(U)]

            @pl.when(z == 0)
            def _():
                from_left[0] = jnp.zeros((BLK, D), BF)

            @pl.when(z == T - 1)
            def _():
                from_right[T - 1] = jnp.zeros((BLK, D), BF)

        def at(self, buf, d, u):
            return buf.at[d, pl.ds(RU * u, RU)]

        def begin(self, u, ds):
            for d in ds:
                if d > 0:
                    send(self.at(self.part, d, u), self.at(self.fl, d, u), self.base[u] + d, (r, z + 1), z == 0)
                e = T - 1 - d
                if e < T - 1:
                    send(self.at(self.part, e, u), self.at(self.fr, e, u), self.base[u] + T + e, (r, z - 1),
                         z == T - 1)

        def relay(self, u, d, right, where):
            buf, slot = (self.fl, self.base[u] + d) if right else (self.fr, self.base[u] + T + d)
            to = z + 1 if right else z - 1
            cond = z == where

            @pl.when(cond)
            def _():
                arrived(self.at(buf, d, u), slot)
                rows = pl.ds(RU * u, RU)
                self.part[d, rows, :] = (self.part[d, rows, :].astype(F32)
                                         + buf[d, rows, :].astype(F32)).astype(BF)

            send(self.at(self.part, d, u), self.at(buf, d, u), slot, (r, to), cond)

        def hop1(self, u):
            self.relay(u, 3, True, 1)
            self.relay(u, 0, False, 2)
            self.relay(u, 2, True, 1)
            self.relay(u, 1, False, 2)

        def hop2(self, u):
            self.relay(u, 3, True, 2)
            self.relay(u, 0, False, 1)

        def last(self, u):
            arrived(self.at(self.fl, z, u), self.base[u] + z, z > 0)
            arrived(self.at(self.fr, z, u), self.base[u] + T + z, z < T - 1)

        def total(self, rows):
            return (self.part[z, rows, :].astype(F32) + self.fl[z, rows, :].astype(F32)
                    + self.fr[z, rows, :].astype(F32))

    def pieces_of(buf):
        return lambda i, u: buf.at[i, pl.ds(RU * u, RU)]

    class Hand:
        def __init__(self, buf, landing):
            self.buf, self.landing = buf, landing
            self.base = [new(2) for _ in range(U)]

        def __call__(self, i, u, cond):
            k = lax.div(i, 2)
            wanted = lax.rem(i, 2) != c
            if cond is not None:
                wanted = wanted & cond
            send(self.buf.at[i, pl.ds(RU * u, RU)], self.landing.at[k, pl.ds(RU * u, RU)],
                 self.base[u] + k, (mate, z), wanted)

        def wait(self):
            for u in range(U):
                for k in range(2):
                    arrived(self.landing.at[k, pl.ds(RU * u, RU)], self.base[u] + k)

    WH = nh * HEAD // 2
    swo = new(T)

    def hand_wo(i, u, cond):
        send(s.wo.at[i, c], s.wo.at[i, c], swo + i, (mate, z), cond)

    wo_line = Line(lambda i, u: s.wo.at[i, c], 1, lambda i, u, cond: None if cond is None else hand_wo(i, u, cond))
    loads["wo"].wait()
    wo_line.start(0)
    s.wqt[pl.ds(3 * nh * HEAD, 640 - 3 * nh * HEAD), :] = jnp.zeros((640 - 3 * nh * HEAD, D), BF)
    s.brow[...] = jnp.zeros((1, 640), F32)
    s.brow[:, 0:192] = qvb_ref[0:1, :]
    s.brow[:, 384:576] = qvb_ref[1:2, :]
    g1 = g1_ref[...].reshape(1, -1)
    b1 = b1_ref[...].reshape(1, -1)
    skv = new(max(4 * 4, NG + 1))

    def project(first):
        for k in range(2):
            for i in range(2):
                rows = pl.ds(64 * i, 64)
                n, _inv = normed(s.x[2 * k + first, rows, :].astype(F32))
                s.act1[2 * k + first, rows, :] = (n * g1 + b1).astype(BF)
        a = jnp.concatenate([s.act1[first], s.act1[2 + first]], axis=0)
        s.pre[0:256, 0:640] = dg(a, s.wqt[...], 1, 1)
        low = lax.broadcasted_iota(jnp.int32, (BLK, 128), 1) < HEAD
        zero = jnp.zeros((BLK, 128), F32)
        for k in range(2):
            j = 2 * k + first
            t = [s.pre[BLK * k:BLK * k + BLK, 128 * i:128 * i + 128] + s.brow[:, 128 * i:128 * i + 128]
                 for i in range(5)]
            rows = pl.ds(pl.multiple_of(j * BLK, BLK), BLK)
            s.kv[g, j, 0] = jnp.where(low, roll64(t[1]), roll64(t[3])).astype(BF)
            s.kv[g, j, 1] = jnp.where(low, t[2], t[3]).astype(BF)
            s.kv[g, j, 2] = jnp.where(low, roll64(t[2]), roll64(t[4])).astype(BF)
            s.q[0, rows, :] = (jnp.where(low, t[0], zero) * 0.125).astype(BF)
            s.q[1, rows, :] = (jnp.where(low, roll64(t[0]), zero) * 0.125).astype(BF)
            s.q[2, rows, :] = (jnp.where(low, t[1], zero) * 0.125).astype(BF)

    def kv_send(block, t, to):
        send(s.kv.at[block[0], block[1]], s.kv.at[block[0], block[1]], skv + 4 * t + block[1],
             (2 * to + c, z))

    def kv_arrived(src, j, t):
        arrived(s.kv.at[src, j], skv + 4 * t + j)

    loads["wqt"].wait()
    project(c)
    if NG == 4:
        kv_send((g, c), 1, peers[1])
        kv_send((g, 2 + c), 2, peers[2])
        kv_send((g, 2 + c), 1, peers[1])
        kv_send((g, c), 2, peers[2])
    for k in range(2):
        arrived(s.x.at[2 * k + o], sx + k)
    project(o)
    if NG == 4:
        kv_send((g, o), 1, peers[1])
        kv_send((g, 2 + o), 2, peers[2])
        kv_send((g, 2 + o), 1, peers[1])
        kv_send((g, o), 2, peers[2])
    else:
        for t in range(1, NG):
            send(s.kv.at[g], s.kv.at[g], skv + t, (2 * peers[t] + c, z))

    loads["cot"].wait()
    for k in range(2):
        s.stage[1, k] = s.cot_raw[other[k]]
        send(s.stage.at[1, k], s.cot.at[2 * k + c], sx + 2 + k, (mate, z))
    for k in range(2):
        s.cot[2 * k + c] = s.cot_raw[own[k]]
    for i in range(2 * nh):
        s.m[i] = jnp.full((1, 256), NEG, F32)
        s.l[i] = jnp.zeros((1, 256), F32)
        s.acc[i] = jnp.zeros((128, 256), F32)

    def masks(src):
        k_low = (low_pos(2 * src), low_pos(2 * src + 1))
        i0 = lax.broadcasted_iota(jnp.int32, (256, 256), 0)
        i1 = lax.broadcasted_iota(jnp.int32, (256, 256), 1)

        def token(i, a, b):
            return i + jnp.where(i < BLK, a * BLK, b * BLK - BLK)

        last = 2 * R - 1
        s.mlo[...] = jnp.where(token(i0, *k_low) <= token(i1, *q_low), 0.0, NEG)
        s.mhi[...] = jnp.where(
            token(i0, last - k_low[0], last - k_low[1])
            <= token(i1, last - q_low[0], last - q_low[1]), 0.0, NEG)

    def keys_of(src, h):
        return s.kv[src, 0:2, h].reshape(256, 128), s.kv[src, 2:4, h].reshape(256, 128)

    def attend(src):
        masks(src)
        for h in range(nh):
            klo, khi = keys_of(src, h)
            s1 = dg(klo, s.q[h, 0:256, :], 1, 1) + s.mlo[...]
            old = s.m[2 * h]
            now = jnp.maximum(old, jnp.max(s1, axis=0, keepdims=True))
            e1 = jnp.exp(s1 - now)
            f = jnp.exp(old - now)
            s.l[2 * h] = s.l[2 * h] * f + jnp.sum(e1, axis=0, keepdims=True)
            s.acc[2 * h] = s.acc[2 * h] * f + dg(klo, e1.astype(BF), 0, 0)
            s.m[2 * h] = now
            qhi = s.q[h, 256:512, :]
            s2 = dg(klo, qhi, 1, 1)
            s3 = dg(khi, qhi, 1, 1) + s.mhi[...]
            old = s.m[2 * h + 1]
            now = jnp.maximum(old, jnp.maximum(jnp.max(s2, axis=0, keepdims=True),
                                               jnp.max(s3, axis=0, keepdims=True)))
            e2 = jnp.exp(s2 - now)
            e3 = jnp.exp(s3 - now)
            f = jnp.exp(old - now)
            s.l[2 * h + 1] = (s.l[2 * h + 1] * f + jnp.sum(e2, axis=0, keepdims=True)
                              + jnp.sum(e3, axis=0, keepdims=True))
            s.acc[2 * h + 1] = (s.acc[2 * h + 1] * f + dg(klo, e2.astype(BF), 0, 0)
                                + dg(khi, e3.astype(BF), 0, 0))
            s.m[2 * h + 1] = now

    attend(g)
    wo_line.step(0, 1)
    for k in range(2):
        arrived(s.cot.at[2 * k + o], sx + 2 + k)
    loads["pw"].wait()
    for half in range(2):
        s.ga[256 * half:256 * half + 256, :] = dg(
            s.cot[2 * half:2 * half + 2].reshape(256, D), s.pw[...], 1, 1)
    s.wopad[...] = jnp.zeros((nh * BLK, D), BF)
    mine = s.wo[z].reshape(nh * HEAD, D)
    for h in range(nh):
        s.wopad[BLK * h + HEAD:BLK * h + BLK, :] = mine[HEAD * h:HEAD * h + HEAD]
    sum1 = Sum(s.p1, s.r1, s.l1)
    sum2 = Sum(s.p2, s.r2, s.l2)
    sum3 = Sum(s.p3, s.r3, s.l3)
    s.vsum[...] = jnp.zeros((16, D), F32)

    if NG == 4:
        kv_arrived(peers[1], c, 1)
        kv_send((peers[1], c), 3, peers[2])
        kv_arrived(peers[2], 2 + c, 2)
        kv_send((peers[2], 2 + c), 3, peers[1])
        kv_arrived(peers[1], o, 1)
        kv_send((peers[1], o), 3, peers[2])
        kv_arrived(peers[2], 2 + o, 2)
        kv_send((peers[2], 2 + o), 3, peers[1])
        wo_line.step(0, 2)
        kv_arrived(peers[1], 2 + c, 1)
        kv_arrived(peers[1], 2 + o, 1)
        attend(peers[1])
        kv_arrived(peers[2], c, 2)
        kv_arrived(peers[2], o, 2)
        attend(peers[2])
        wo_line.step(0, 3)
        for j in (c, 2 + c, o, 2 + o):
            kv_arrived(peers[3], j, 3)
        attend(peers[3])
    else:
        for t in range(1, NG):
            arrived(s.kv.at[sources[t]], skv + t)

        def rest(t, _):
            attend(lax.rem(g + t, NG))
            return 0

        lax.fori_loop(1, NG, rest, 0)
        wo_line.step(0, 2)
        wo_line.step(0, 3)

    low = lax.broadcasted_iota(jnp.int32, (256, 128), 1) < HEAD
    thirds = []
    for half in range(2):
        rows = pl.ds(256 * half, 256)
        outs = []
        for h in range(nh):
            outs.append(jnp.transpose(s.acc[2 * h + half] / s.l[2 * h + half]))
            s.attp[h, rows, :] = outs[h].astype(BF)
            s.m[2 * h + half] = s.m[2 * h + half] + jnp.log(s.l[2 * h + half])
        pair = jnp.where(low, roll64(outs[0]), outs[1]).astype(BF)
        s.ab[z, rows, :] = pair
        s.attn[rows, 0:128] = pair
        turned = roll64(outs[2])
        s.attn[rows, 128:256] = jnp.where(low, turned, 0.0).astype(BF)
        thirds.append((turned, outs[2]))
    s.ab[z, 512:768, :] = jnp.where(low, thirds[0][0], thirds[1][1]).astype(BF)
    ab_line = Line(lambda i, u: s.ab.at[i, pl.ds(384 * u, 384)], 2)
    ab_line.start(0)
    ab_line.start(1)

    for t in range(1, T):
        arrived(s.wo.at[lax.rem(z + t, T), o], swo + lax.rem(z + t, T))
    zeros = jnp.zeros((HEAD, D), BF)
    for t in range(T):
        third = s.wo[t].reshape(nh * HEAD, D)[128:192]
        s.wolo[t, 0:HEAD, :] = third
        s.wolo[t, HEAD:BLK, :] = zeros
        s.wohi[t, 0:HEAD, :] = zeros
        s.wohi[t, HEAD:BLK, :] = third
    for k in range(1, T):
        ab_line.step(0, k)
        ab_line.step(1, k)

    left = jnp.concatenate([s.ab[t, 0:512, :] for t in range(T)], axis=1)
    pairs = jnp.concatenate([s.wo[t].reshape(nh * HEAD, D)[0:128] for t in range(T)], axis=0)
    tail = jnp.concatenate([s.ab[t, 512:768, :] for t in range(T)], axis=1)
    g2 = g2_ref[...].reshape(1, -1)
    b2 = b2_ref[...].reshape(1, -1)
    ob = ob_ref[...].reshape(1, -1)
    fcb = fcb_ref[...].reshape(1, -1)
    pb = pb_ref[...].reshape(1, -1)
    for half in range(2):
        third = s.wolo if half == 0 else s.wohi
        s.pre[256 * half:256 * half + 256, :] = (
            dg(left[256 * half:256 * half + 256], pairs, 1, 0)
            + dg(tail, third[...].reshape(T * 128, D), 1, 0))

    def norm2(i, _):
        j = lax.div(i, 2)
        sub = pl.ds(pl.multiple_of(lax.rem(i, 2) * 64, 64), 64)
        rows = pl.ds(pl.multiple_of(i * 64, 64), 64)
        x = s.x[j, sub, :].astype(F32) + s.pre[rows, :] + ob
        s.hid[j, sub, :] = x
        n, _inv = normed(x)
        s.act2[rows, :] = (n * g2 + b2).astype(BF)
        return 0

    lax.fori_loop(0, 8, norm2, 0)

    loads["fc"].wait()
    bias_sum = jnp.zeros((8, F), F32)
    first = jnp.where(z < T // 2, 1, 0)
    for turn in range(2):
        half = first if turn == 0 else 1 - first
        base = pl.multiple_of(half * 256, 256)
        part = pl.ds(base, 256)
        s.pre[part, :] = dg(s.act2[part, :], s.fc[...], 1, 0)

        def gelu(i, total, base=base):
            rows = pl.ds(pl.multiple_of(base + i * 32, 32), 32)
            v = s.pre[rows, :] + fcb
            square = v * v
            th = jnp.tanh(C0 * (v + C1 * square * v))
            one = 1.0 + th
            s.actd[rows, :] = (0.5 * v * one).astype(BF)
            slope = 0.5 * one + (0.5 * v) * (1.0 - th * th) * (C0 * (1.0 + 3.0 * C1 * square))
            grad = slope * s.ga[rows, :]
            s.gpre[rows, :] = grad.astype(BF)
            return total + fold8(grad)

        bias_sum = lax.fori_loop(0, 8, gelu, bias_sum)
        back = dg(s.gpre[part, :], s.fc[...], 1, 1)
        s.p1[2 * half] = back[0:128].astype(BF)
        s.p1[2 * half + 1] = back[128:256].astype(BF)
        if turn == 0:
            sum1.begin(0, (3, 2))
    sum1.begin(0, (1,))
    for u in range(1, U):
        sum1.begin(u, (3, 2, 1))
    s.vsum[8:9, :] = jnp.sum(bias_sum, axis=0, keepdims=True)

    sw1 = new(2 + 2 * NG)

    def weight(dst, index, lhs, rhs):
        for i in range(3):
            part = dg(lhs[:, 256 * i:256 * i + 256], rhs, 0, 0).astype(BF)
            lo, hi = 256 * i, 256 * i + 256
            for qd in range(NG):
                a, b = max(lo, qd * Q1), min(hi, qd * Q1 + Q1)
                if a < b:
                    dst[index, qd, a - qd * Q1:b - qd * Q1, :] = part[a - lo:b - lo]

    def add_into(buf, index, extra):
        def body(i, _):
            buf[index, i] = (buf[index, i].astype(F32) + extra[i].astype(F32)).astype(BF)
            return 0

        lax.fori_loop(0, NG, body, 0)

    weight(s.w1, 0, s.actd, s.cot[...].reshape(N, D))
    weight(s.w1, 1, s.act2, s.gpre[...])
    send(s.w1.at[o], s.w1r, sw1, (mate, z))
    sum1.hop1(0)
    for half in range(2):
        base = 256 * half
        fwd = dg(s.actd[base:base + 256, :], s.pw[...], 1, 0)
        s.p2[2 * half] = fwd[0:128].astype(BF)
        s.p2[2 * half + 1] = fwd[128:256].astype(BF)
    sum1.hop2(0)
    arrived(s.w1r, sw1)
    add_into(s.w1, c, s.w1r)
    for t in range(1, NG):
        send(s.w1.at[c, peers[t]], s.w1s.at[t], sw1 + t, (2 * peers[t] + c, z))

    def back2(u):
        sums = [jnp.zeros((8, D), F32)] * 4
        for i in range(RU // 32):
            rows = pl.ds(RU * u + 32 * i, 32)
            n, inv = normed(s.hid[z, rows, :])
            grad = sum1.total(rows)
            up = s.cot[z, rows, :].astype(F32)
            qg = grad * g2
            gh = up + inv * (qg - jnp.mean(qg, axis=-1, keepdims=True)
                             - n * jnp.mean(qg * n, axis=-1, keepdims=True))
            s.gh[rows, :] = gh
            s.h[z, rows, :] = gh.astype(BF)
            for k, part in enumerate((grad * n, grad, gh, up)):
                sums[k] = sums[k] + fold8(part)
        for k in range(4):
            s.vsum[2 + k:3 + k, :] += jnp.sum(sums[k], axis=0, keepdims=True)

    h_line = Line(pieces_of(s.h), U)
    sum1.last(0)
    back2(0)
    h_line.start(0)
    sum1.hop1(1)
    sum1.hop2(1)
    h_line.step(0, 1)
    sum1.last(1)
    back2(1)
    h_line.start(1)
    sum2.begin(0, (3, 2, 1))
    h_line.step(0, 2)
    h_line.step(1, 1)
    h_line.step(0, 3)
    sum2.begin(1, (3, 2, 1))
    h_line.step(1, 2)
    h_line.step(1, 3)

    grads = dg(s.h[...].reshape(N, D), s.wopad[...], 1, 1)
    for h in range(nh):
        s.do[h] = grads[:, 128 * h:128 * h + 128].astype(BF)
    for h in range(nh):
        for half in range(2):
            rows = pl.ds(256 * half, 256)
            both = s.do[h, rows, :].astype(F32) * s.attp[h, rows, :].astype(F32)
            s.delta[2 * h + half] = jnp.sum(jnp.transpose(both), axis=0, keepdims=True)
    for i in range(2 * nh):
        s.acc[i] = jnp.zeros((128, 256), F32)

    def attend_back(src):
        masks(src)
        for h in range(nh):
            klo, khi = keys_of(src, h)

            def tile(k, half, mask):
                qs = s.q[h, 256 * half:256 * half + 256, :]
                ds_ = s.do[h, 256 * half:256 * half + 256, :]
                sc = dg(k, qs, 1, 1)
                if mask is not None:
                    sc = sc + mask[...]
                p = jnp.exp(sc - s.m[2 * h + half])
                d = p * (dg(k, ds_, 1, 1) - s.delta[2 * h + half])
                p = p.astype(BF)
                d = d.astype(BF)
                return d, dg(d, qs, 1, 0) + dg(p, ds_, 1, 0)

            d1, k1 = tile(klo, 0, s.mlo)
            s.acc[2 * h] += dg(klo, d1, 0, 0)
            d2, k2 = tile(klo, 1, None)
            s.dk[src, h, 0:256, :] = (k1 + k2).astype(BF)
            d3, k3 = tile(khi, 1, s.mhi)
            s.dk[src, h, 256:512, :] = k3.astype(BF)
            s.acc[2 * h + 1] += dg(klo, d2, 0, 0) + dg(khi, d3, 0, 0)

    sdk = new(NG + 2)

    def w1_gather():
        for t in range(1, NG):
            arrived(s.w1s.at[t], sw1 + t)

        def body(i, _):
            rows = pl.ds(pl.multiple_of(i * (Q1 // 3), Q1 // 3), Q1 // 3)
            total = s.w1[c, g, rows, :].astype(F32)
            for t in range(1, NG):
                total = total + s.w1s[t, rows, :].astype(F32)
            s.w1f[c, g, rows, :] = total.astype(BF)
            return 0

        lax.fori_loop(0, 3, body, 0)
        for t in range(1, NG):
            send(s.w1f.at[c, g], s.w1f.at[c, g], sw1 + NG + t, (2 * peers[t] + c, z))

    hand_o = Hand(s.yo, s.mo)
    o_line = Line(pieces_of(s.yo), U, hand_o)

    def finish_output(u):
        for i in range(RU // 32):
            rows = pl.ds(RU * u + 32 * i, 32)
            s.yo[z, rows, :] = (s.hid[z, rows, :] + sum2.total(rows) + pb).astype(BF)
        o_line.start(u)

    half_a = pl.ds(0, 256)
    half_b = pl.ds(256, 256)
    sum2.hop1(0)
    if NG == 4:
        attend_back(peers[3])
        send(s.dk.at[peers[3], :, half_a], s.dka.at[0], sdk + 0, (2 * peers[1] + c, z))
        send(s.dk.at[peers[3], :, half_b], s.dka.at[1], sdk + NG, (2 * peers[2] + c, z))
        attend_back(peers[1])
        w1_gather()
        sum2.hop1(1)
        sum2.hop2(0)
        attend_back(peers[2])
        arrived(s.dka.at[0], sdk + 0)
        for h in range(nh):
            s.dk[peers[2], h, half_a, :] = (s.dk[peers[2], h, half_a, :].astype(F32)
                                            + s.dka[0, h].astype(F32)).astype(BF)
        send(s.dk.at[peers[2]], s.dkr.at[2], sdk + 2, (2 * peers[2] + c, z))
        arrived(s.dka.at[1], sdk + NG)
        for h in range(nh):
            s.dk[peers[1], h, half_b, :] = (s.dk[peers[1], h, half_b, :].astype(F32)
                                            + s.dka[1, h].astype(F32)).astype(BF)
        send(s.dk.at[peers[1]], s.dkr.at[1], sdk + 1, (2 * peers[1] + c, z))
        attend_back(g)
    else:
        def rest_back(t, _):
            attend_back(lax.rem(g + t, NG))
            return 0

        lax.fori_loop(0, NG, rest_back, 0)
        for t in range(1, NG):
            send(s.dk.at[peers[t]], s.dkr.at[t], sdk + t, (2 * peers[t] + c, z))
        w1_gather()
        sum2.hop1(1)
        sum2.hop2(0)
    sum2.hop2(1)
    sum2.last(0)
    finish_output(0)

    sw2 = new(2 + 2 * NG)

    def put2(first, value, rows):
        done = 0
        while done < rows:
            at, off = divmod(first + done, Q2)
            n = min(Q2 - off, rows - done)
            s.w2[at // NG, at % NG, off:off + n, :] = value[done:done + n].astype(BF)
            done += n

    gout = dg(s.attn[...], s.h[...].reshape(N, D), 0, 0)
    put2(3 * nh * HEAD, gout, nh * HEAD)
    sum2.last(1)
    finish_output(1)
    o_line.step(0, 1)
    o_line.step(1, 1)

    got = [1, 2] if NG == 4 else list(range(1, NG))
    for t in got:
        arrived(s.dkr.at[t], sdk + t)
    col = [jnp.zeros((1, 128), F32) for _ in range(5)]
    for half in range(2):
        rows = pl.ds(256 * half, 256)
        dq = [jnp.transpose(s.acc[2 * h + half]) * 0.125 for h in range(nh)]
        dkv = []
        for h in range(nh):
            total = s.dk[g, h, rows, :].astype(F32)
            for t in got:
                total = total + s.dkr[t, h, rows, :].astype(F32)
            dkv.append(total)
        tiles = [
            jnp.where(low, dq[0], roll64(dq[1])),
            jnp.where(low, dq[2], roll64(dkv[0])),
            jnp.where(low, dkv[1], roll64(dkv[2])),
            jnp.where(low, roll64(dkv[0]), dkv[1]),
            jnp.where(low, roll64(dkv[2]), 0.0),
        ]
        for j in range(5):
            col[j] = col[j] + jnp.sum(tiles[j], axis=0, keepdims=True)
            s.gn[rows, 128 * j:128 * j + 128] = tiles[j].astype(BF)
    for turn in range(2):
        half = first if turn == 0 else 1 - first
        part = pl.ds(pl.multiple_of(half * 256, 256), 256)
        back = dg(s.gn[part, :], s.wqt[...], 1, 0)
        s.p3[2 * half] = back[0:128].astype(BF)
        s.p3[2 * half + 1] = back[128:256].astype(BF)
        if turn == 0:
            sum3.begin(0, (3, 2))
    sum3.begin(0, (1,))
    for u in range(1, U):
        sum3.begin(u, (3, 2, 1))
    for j in range(5):
        s.vsum[9:10, 128 * j:128 * j + 128] = col[j]

    act1 = s.act1[...].reshape(N, D)
    for j in range(5):
        n = min(128, 3 * nh * HEAD - 128 * j)
        put2(128 * j, dg(s.gn[:, 128 * j:128 * j + 128], act1, 0, 0), n)
    send(s.w2.at[o], s.w2r, sw2, (mate, z))
    sum3.hop1(0)
    o_line.step(0, 2)
    arrived(s.w2r, sw2)
    add_into(s.w2, c, s.w2r)
    for t in range(1, NG):
        send(s.w2.at[c, peers[t]], s.w2s.at[t], sw2 + t, (2 * peers[t] + c, z))
    sum3.hop2(0)
    o_line.step(1, 2)
    o_line.step(0, 3)

    def back1(u):
        sums = [jnp.zeros((8, D), F32)] * 2
        for i in range(RU // 32):
            rows = pl.ds(RU * u + 32 * i, 32)
            n, inv = normed(s.x[z, rows, :].astype(F32))
            grad = sum3.total(rows)
            qg = grad * g1
            gx = s.gh[rows, :] + inv * (qg - jnp.mean(qg, axis=-1, keepdims=True)
                                        - n * jnp.mean(qg * n, axis=-1, keepdims=True))
            s.yg[z, rows, :] = gx.astype(BF)
            for k, part in enumerate((grad * n, grad)):
                sums[k] = sums[k] + fold8(part)
        for k in range(2):
            s.vsum[k:k + 1, :] += jnp.sum(sums[k], axis=0, keepdims=True)

    hand_g = Hand(s.yg, s.mg)
    y_line = Line(pieces_of(s.yg), U, hand_g)
    v_line = Line(lambda i, u: s.vz.at[i], 1)
    sum3.last(0)
    back1(0)
    y_line.start(0)
    sum3.hop1(1)
    sum3.hop2(1)
    o_line.step(1, 3)
    for t in range(1, NG):
        arrived(s.w2s.at[t], sw2 + t)
    total = s.w2[c, g].astype(F32)
    for t in range(1, NG):
        total = total + s.w2s[t].astype(F32)
    s.w2f[c, g] = total.astype(BF)
    for t in range(1, NG):
        send(s.w2f.at[c, g], s.w2f.at[c, g], sw2 + NG + t, (2 * peers[t] + c, z))
    y_line.step(0, 1)
    sum3.last(1)
    back1(1)
    s.vz[z] = s.vsum[...].astype(BF)
    v_line.start(0)
    y_line.start(1)
    for t in range(1, NG):
        arrived(s.w1f.at[c, sources[t]], sw1 + NG + t)
    send(s.w1f.at[c], s.w1f.at[c], sw1 + 2 * NG, (mate, z))
    hand_o.wait()
    copies = []

    def give(src, dst):
        copy = pltpu.make_async_copy(src, dst, s.ls.at[6 + len(copies)])
        copy.start()
        copies.append(copy)

    for k in range(2):
        give(s.yo.at[2 * k + c], fo_out.at[k, c])
        give(s.mo.at[k], fo_out.at[k, o])
    v_line.step(0, 1)
    y_line.step(0, 2)
    y_line.step(1, 1)
    v_line.step(0, 2)
    arrived(s.w1f.at[o], sw1 + 2 * NG)
    give(s.w1f, w1_out)
    y_line.step(0, 3)
    v_line.step(0, 3)

    svc = new(R)
    upper = s.vz[0, 0:8, :].astype(F32)
    for t in range(1, T):
        upper = upper + s.vz[t, 0:8, :].astype(F32)
    s.vc[r] = jnp.concatenate([upper, s.vsum[8:16, :]], axis=0).astype(BF)
    for t in range(1, R):
        send(s.vc.at[r], s.vc.at[r], svc + t, (lax.rem(r + t, R), z))
    y_line.step(1, 2)
    for t in range(1, NG):
        arrived(s.w2f.at[c, sources[t]], sw2 + NG + t)
    send(s.w2f.at[c], s.w2f.at[c], sw2 + 2 * NG, (mate, z))
    for t in range(1, R):
        arrived(s.vc.at[lax.rem(r + R - t, R)], svc + t)
    total = s.vc[0].astype(F32)
    for t in range(1, R):
        total = total + s.vc[t].astype(F32)
    s.vsum[...] = total
    give(s.vsum, v_out)
    arrived(s.w2f.at[o], sw2 + 2 * NG)
    give(s.w2f, w2_out)
    y_line.step(1, 3)
    hand_g.wait()
    for k in range(2):
        give(s.yg.at[2 * k + c], fg_out.at[k, c])
        give(s.mg.at[k], fg_out.at[k, o])
    for cond, done in pending:
        if cond is None:
            done()
        else:
            pl.when(cond)(done)
    for copy in copies:
        copy.wait()


def finish_kernel(R, NS, pos_ref, seq_ref, rank_ref, w1_ref, w2_ref, fo_ref, fg_ref, v_ref, out_ref, gt_ref,
                  ln1g_ref, ln1b_ref, gq_ref, gqv_ref, go_ref, ob_ref, ln2g_ref, ln2b_ref, gf_ref, fb_ref,
                  gp_ref, pb_ref):
    i = pl.program_id(0)
    gp_ref[...] = w1_ref[0].astype(F32)
    gf_ref[...] = w1_ref[1].astype(F32)

    @pl.when(i < 6)
    def _():
        gq_ref[...] = w2_ref[...].astype(F32)

    @pl.when(i >= 6)
    def _():
        go_ref[...] = w2_ref[...].astype(F32)

    @pl.when(i < 4)
    def _():
        b = 4 * rank_ref[0] + i
        high = jnp.where(pos_ref[b] < R, 0, 1)
        out_ref[...] = fo_ref[high, seq_ref[b]]
        gt_ref[...] = fg_ref[high, seq_ref[b]]

    @pl.when(i == 0)
    def _():
        for ref, k in ((ln1g_ref, 0), (ln1b_ref, 1), (ln2g_ref, 2), (ln2b_ref, 3), (ob_ref, 4), (pb_ref, 5),
                       (fb_ref, 8)):
            ref[...] = v_ref[k:k + 1, :].reshape(-1)
        gqv_ref[0:1, :] = v_ref[9:10, 0:192]
        gqv_ref[1:2, :] = v_ref[9:10, 384:576]


def per_device(R, T, tokens, cotangent, block_pos, block_seq, ln1_gain, ln1_bias, qkv_weight, qv_bias,
               out_weight, out_bias, ln2_gain, ln2_bias, fc_weight, fc_bias, proj_weight, proj_bias):
    D = tokens.shape[1]
    F = fc_weight.shape[1]
    local = qkv_weight.shape[2]
    nh = local // HEAD
    NG = R // 2
    sizes = scratch_list(R, T, D, F, nh)
    names = [n for n, _ in sizes]
    row = lambda v: v
    wqt = jnp.transpose(qkv_weight, (1, 2, 0)).reshape(3 * local, D)
    sm = pl.BlockSpec(memory_space=pltpu.SMEM)
    vm = pl.BlockSpec(memory_space=pltpu.VMEM)
    hb = pl.BlockSpec(memory_space=pl.ANY)
    w1, w2, fo, fg, vs = pl.pallas_call(
        functools.partial(layer_kernel, R, T, D, F, nh, names),
        out_shape=(
            jax.ShapeDtypeStruct((2, NG, D // NG, D), BF),
            jax.ShapeDtypeStruct((2, NG, D // 2 // NG, D), BF),
            jax.ShapeDtypeStruct((2, 2, BLK, D), BF),
            jax.ShapeDtypeStruct((2, 2, BLK, D), BF),
            jax.ShapeDtypeStruct((16, D), F32),
        ),
        in_specs=[sm, sm, hb, hb, vm, vm, hb, vm, hb, vm, vm, vm, hb, vm, hb, vm],
        out_specs=(hb, hb, hb, hb, hb),
        scratch_shapes=[sp for _, sp in sizes],
        compiler_params=pltpu.CompilerParams(
            collective_id=0, has_side_effects=True, vmem_limit_bytes=67043328),
        name="layer",
    )(block_pos, block_seq, tokens.reshape(4, BLK, D), cotangent.reshape(4, BLK, D), row(ln1_gain),
      row(ln1_bias), wqt, qv_bias, out_weight.reshape(2, local // 2, D), row(out_bias), row(ln2_gain), row(ln2_bias), fc_weight,
      row(fc_bias), proj_weight, row(proj_bias))

    rank = lax.axis_index("ctx").astype(jnp.int32).reshape(1)
    NS = 8
    rb = D // NS
    whole = lambda *shape: pl.BlockSpec(shape, lambda i: (0,) * len(shape))
    vec = jax.ShapeDtypeStruct((D,), F32)
    outs = pl.pallas_call(
        functools.partial(finish_kernel, R, NS),
        grid=(NS,),
        out_shape=(
            jax.ShapeDtypeStruct((4 * BLK, D), BF),
            jax.ShapeDtypeStruct((4 * BLK, D), BF),
            vec, vec,
            jax.ShapeDtypeStruct((3 * local, D), F32),
            jax.ShapeDtypeStruct((2, local), F32),
            jax.ShapeDtypeStruct((local, D), F32),
            vec, vec, vec,
            jax.ShapeDtypeStruct((D, F), F32),
            vec,
            jax.ShapeDtypeStruct((F, D), F32),
            vec,
        ),
        in_specs=[sm, sm, sm,
                  pl.BlockSpec((2, rb, D), lambda i: (0, i, 0)),
                  pl.BlockSpec((rb, D), lambda i: (i, 0)),
                  whole(2, 2, BLK, D), whole(2, 2, BLK, D), whole(16, D)],
        out_specs=(
            pl.BlockSpec((BLK, D), lambda i: (jnp.minimum(i, 3), 0)),
            pl.BlockSpec((BLK, D), lambda i: (jnp.minimum(i, 3), 0)),
            whole(D), whole(D),
            pl.BlockSpec((rb, D), lambda i: (jnp.minimum(i, 5), 0)),
            whole(2, local),
            pl.BlockSpec((rb, D), lambda i: (jnp.maximum(i - 6, 0), 0)),
            whole(D), whole(D), whole(D),
            pl.BlockSpec((rb, F), lambda i: (i, 0)),
            whole(F),
            pl.BlockSpec((rb, D), lambda i: (i, 0)),
            whole(D),
        ),
        name="finish",
    )(block_pos, block_seq, rank, w1.reshape(2, D, D), w2.reshape(D, D), fo, fg, vs)
    (output, grad_tokens, ln1g, ln1b, gq, gqv, go, ob, ln2g, ln2b, gf, fb, gp, pb) = outs
    flat = lambda v: v
    return (output, grad_tokens, flat(ln1g), flat(ln1b),
            jnp.transpose(gq.reshape(3, local, D), (2, 0, 1)), gqv, go, flat(ob), flat(ln2g), flat(ln2b),
            gf, flat(fb), gp, flat(pb))


def solution(mesh):
    R = mesh.shape["ctx"]
    T = mesh.shape["tp"]
    return jax.shard_map(
        functools.partial(per_device, R, T),
        mesh=mesh,
        in_specs=(
            P("ctx", None), P("ctx", None), P(), P(), P(), P(), P(None, None, "tp"), P(None, "tp"),
            P("tp", None), P(), P(), P(), P(None, "tp"), P("tp"), P("tp", None), P(),
        ),
        out_specs=(
            P("ctx", None), P("ctx", None), P(), P(), P(None, None, "tp"), P(None, "tp"), P("tp", None),
            P(), P(), P(), P(None, "tp"), P("tp"), P("tp", None), P(),
        ),
        check_vma=False,
    )
```

```python
import functools
from types import SimpleNamespace

import jax
import jax.numpy as jnp
from jax import lax
from jax.experimental import pallas as pl
from jax.experimental.pallas import tpu as pltpu
from jax.sharding import PartitionSpec as P

HEAD = 64
BLK = 128

class Names:
    def __getattr__(self, name):
        return name


ID = Names()
BF = jnp.bfloat16
F32 = jnp.float32
MESH = pl.DeviceIdType.MESH
NEG = -1e30
C0 = 0.7978845608028654
C1 = 0.044715
U = 4
SENDS = 90
SPLIT_AT = 26
ARRIVALS = 222
TIDY = (ID.far1, ID.feed1, ID.weights_b, ID.high, ID.low3, ID.collect0, (ID.n1_, 2))

LAT = 1.6
OUT_FROM = 15.0
OUT_GAP = 1.0
DS = (3, 2, 1)


def dg(a, b, ca, cb):
    return lax.dot_general(a, b, (((ca,), (cb,)), ((), ())), preferred_element_type=F32)


def normed(x):
    centre = jnp.mean(x, axis=-1, keepdims=True)
    shifted = x - centre
    spread = jnp.mean(shifted * shifted, axis=-1, keepdims=True)
    inverse = lax.rsqrt(spread + 1e-05)
    return shifted * inverse, inverse


def fold8(x):
    rows, width = x.shape
    return jnp.sum(x.reshape(rows // 8, 8, width), axis=0)


def roll64(x):
    return pltpu.roll(x, 64, 1)


def simulate(T, jobs, marks, lat, order=None):
    free = {}
    seen = [dict() for _ in range(T)]
    inbox = [[] for _ in range(T)]
    now = [0.0] * T
    steps = [dict() for _ in range(T)]
    left = [list(marks) if order is None else list(order) for _ in range(T)]
    out = [[] for _ in range(T)]
    parts = [dict() for _ in range(T)]
    OP = 0.12

    def post(time, z, step, op):
        tau = jobs[op[3]][0][op[2]]
        begin = max(time, free.get((z, step), 0.0))
        free[z, step] = begin + tau
        inbox[z + step].append((begin + tau + lat, op))

    def spread(time, z, op):
        if jobs[op[3]][4]:
            for to in range(T):
                step = 1 if to > z else -1
                begin = time
                for k in range(z, to, step):
                    begin = max(begin + (0.7 if k != z else 0.0), free.get((k, step), 0.0))
                    free[k, step] = begin + jobs[op[3]][0][op[2]]
                if to != z:
                    inbox[to].append((begin + jobs[op[3]][0][op[2]] + lat, op))
            return
        if z >= op[1] and z < T - 1:
            post(time, z, 1, op)
        if z <= op[1] and z > 0:
            post(time, z, -1, op)

    def passive(z, op):
        kind, i, u, name = op
        if kind in (ID.R, ID.L):
            return i == z
        return jobs[name][4] or (z in (0, T - 1) and jobs[name][2])

    def start_of(z, item):
        if item[0] == ID.op:
            time, op = item[1]
            if op[0] in (ID.R, ID.L):
                own = parts[z].get((op[3], op[2]))
                if own is None:
                    return None
                time = max(time, own)
            return max(time, now[z])
        step = marks[item[1]]
        time = max(now[z], step.get(ID.time, 0.0))
        for name, delay in step.get(ID.after, ()):
            if name not in steps[z]:
                return None
            time = max(time, steps[z][name] + delay)
        for event in step.get(ID.needs, ()):
            event = tuple(z if e == ID.z else e for e in event)
            if event[0] in (ID.R, ID.L) and event[1] == (0 if event[0] == ID.R else T - 1):
                continue
            if event[0] == ID.A and event[1] == z:
                continue
            if event not in seen[z]:
                return None
            time = max(time, seen[z][event])
        return time

    while True:
        best = None
        for z in range(T):
            for entry in list(inbox[z]):
                if passive(z, entry[1]):
                    seen[z][entry[1]] = entry[0]
                    inbox[z].remove(entry)
            for entry in inbox[z]:
                time = start_of(z, (ID.op, entry))
                if time is not None:
                    key = (time, 0 if jobs[entry[1][3]][3] == 0 else 1, entry[0], z)
                    if best is None or key < best[0]:
                        best = (key, z, (ID.op, entry))
            choices = left[z][:1] if order is not None else left[z]
            for k, name in enumerate(choices):
                time = start_of(z, (ID.mark, name))
                if time is not None:
                    key = (time + 0.01, 2 + marks[name].get(ID.low, 0), k, z)
                    if best is None or key < best[0]:
                        best = (key, z, (ID.mark, name))
        if best is None:
            break
        key, z, item = best
        begin = start_of(z, item)
        if item[0] == ID.op:
            _, op = item[1]
            inbox[z].remove(item[1])
            out[z].append((begin, item[1][1]))
            now[z] = begin + OP
            if op[0] == ID.A:
                seen[z][op] = begin
                spread(now[z], z, op)
            else:
                post(now[z], z, 1 if op[0] == ID.R else -1, op)
        else:
            name = item[1]
            step = marks[name]
            left[z].remove(name)
            out[z].append((begin, (ID.M, name)))
            now[z] = begin + step[ID.dur]
            steps[z][name] = now[z]
            for job, u, kind in step.get(ID.posts, ()):
                if kind == ID.gather:
                    spread(now[z], z, (ID.A, z, u, job))
                else:
                    parts[z].setdefault((job, u), now[z])
                    for d in kind:
                        if z == 0:
                            post(now[z], z, 1, (ID.R, d, u, job))
                        if z == T - 1:
                            post(now[z], z, -1, (ID.L, T - 1 - d, u, job))
    if order is None:
        spots = {name: sum(t for z in range(T) for t, op in out[z] if op == (ID.M, name)) for name in marks}
        assert all(len(l) == 0 for l in left), left
        return simulate(T, jobs, marks, lat, sorted(marks, key=lambda n: spots[n]))
    assert all(len(l) == 0 for l in left) and all(len(i) == 0 for i in inbox), (left, inbox)
    return out, max(now)

def emit(T, z, timeline, jobs, marks, actors, steps, flush):
    names = [op[1] for _, op in timeline[0] if op[0] == ID.M]
    todo = [[op for _, op in timeline[zz]] for zz in range(T)]
    waited = [set() for _ in range(T)]
    for name in names:
        for zz in range(T):
            now = []
            while todo[zz][0] != (ID.M, name):
                now.append(todo[zz].pop(0))
            todo[zz].pop(0)
            for event in marks[name].get(ID.needs, ()):
                job = jobs.get(event[3])
                if event[0] == ID.A and event[1] != zz and (job[4] or (zz in (0, T - 1) and job[2])):
                    if event not in waited[zz]:
                        waited[zz].add(event)
                        now.append(event)
            if now:
                @pl.when(z == zz)
                def _(now=now, zz=zz):
                    for op in now:
                        actors[op[3]].one(op, zz)
        if name in steps:
            steps[name]()
        if name in TIDY:
            flush()


def timetable(U, T):
    S = U // 2
    tau = 4.18 / U + 0.1
    hi, lo = range(S), range(S, U)
    norm = 0.15 + 0.8 / U
    jobs = {
        ID.wo: ([1.65] * 2, False, True, 0, False), ID.ab: ([1.5] * 2, False, True, 0, False),
        ID.ac: ([0.8] * 2, False, True, 0, False), ID.ga2: ([tau] * U, True, True, 0, False),
        ID.out: ([tau] * U, True, False, 1, False), ID.ga1: ([tau] * U, True, False, 0, False),
        ID.small: ([0.5], False, False, 0, True),
    }
    m = {}

    def step(name, dur, after=(), needs=(), posts=(), low=0, time=0.0):
        m[name] = dict(dur=dur, after=list(after), needs=list(needs), posts=list(posts), low=low, time=time)

    def every(job, pieces):
        return [(ID.A, i, u, job) for i in range(T) for u in pieces]

    step(ID.wo, 0.0, posts=[(ID.wo, 0, ID.gather), (ID.wo, 1, ID.gather)])
    step(ID.go, 0.3, [(ID.wo, 2.2)])
    step(ID.own, 2.4, [(ID.go, 0)])
    step(ID.relay0, 0.1, [(ID.go, 3.3)])
    step(ID.near0, 1.1, [(ID.go, 4.6), (ID.relay0, 0), (ID.own, 0)])
    step(ID.relay1, 0.1, [(ID.go, 6.0), (ID.relay0, 0)])
    step(ID.far0, 1.1, [(ID.relay0, 4.2), (ID.near0, 0)], posts=[(ID.ab, 0, ID.gather)])
    step(ID.near1, 1.1, [(ID.relay1, 2.0), (ID.far0, 0)])
    step(ID.relay2, 0.1, [(ID.relay1, 4.6)])
    step(ID.far1, 1.1, [(ID.relay1, 4.4), (ID.near1, 0)], posts=[(ID.ab, 1, ID.gather)])
    step(ID.upstream, 0.8, [(ID.far1, 0)])
    step(ID.near2, 1.1, [(ID.relay2, 2.0), (ID.upstream, 0)])
    step(ID.far2, 1.2, [(ID.relay2, 4.0), (ID.near2, 0)], posts=[(ID.ac, 0, ID.gather), (ID.ac, 1, ID.gather)])
    step(ID.pads, 0.4, [(ID.far2, 0)], every(ID.wo, [0, 1]))
    step(ID.mix, 1.0, [(ID.pads, 0)], every(ID.ab, [0, 1]))
    step(ID.feed1, 3.1, [(ID.mix, 0)], every(ID.ac, [0]), [(ID.ga2, u, DS) for u in hi])
    step(ID.feed0, 3.1, [(ID.feed1, 0)], every(ID.ac, [1]), [(ID.ga2, u, DS) for u in lo])
    step(ID.weights_a, 0.8, [(ID.feed0, 2.0)], low=1)
    step(ID.weights_a2, 0.8, [(ID.weights_a, 0)], low=1)
    step(ID.out_partial, 0.8, [(ID.weights_a2, 2.0)], low=1)
    step(ID.weights_b, 0.4, [(ID.weights_a2, 4.5)], low=1)
    step(ID.near_w1, 0.3, [(ID.weights_b, 5.0)], low=1)
    for u in range(U):
        sums = lambda job: [(ID.R, ID.z, u, job), (ID.L, ID.z, u, job)]
        step((ID.n2_, u), norm, needs=sums(ID.ga2), posts=[(ID.ga2, u, ID.gather)])
        for d in DS:
            step((ID.begin_out, u, d), 0.0, [(ID.out_partial, 0), (ID.feed0, OUT_FROM + OUT_GAP * (3 * u + 3 - d))],
                 posts=[(ID.out, u, (d,))], low=1)
        step((ID.out_, u), 0.2, needs=sums(ID.out), posts=[(ID.out, u, ID.gather)], low=1)
        step((ID.n1_, u), norm, needs=sums(ID.ga1), posts=[(ID.ga1, u, ID.gather)])
    m[(ID.n1_, U - 1)][ID.posts].insert(0, (ID.small, 0, ID.gather))
    step(ID.high, 1.4, needs=every(ID.ga2, hi))
    step(ID.high2, 0.9, [(ID.high, 0)])
    step(ID.near_k1a, 0.15, [(ID.high, 3.4), (ID.high2, 0)])
    step(ID.high3, 0.9, [(ID.high2, 0)])
    step(ID.near_k1b, 0.15, [(ID.near_k1a, 0), (ID.high3, 0)])
    step(ID.mid3, 0.9, [(ID.high3, 0)])
    step(ID.low, 1.4, [(ID.mid3, 0), (ID.near_k1b, 0)], every(ID.ga2, lo))
    step(ID.low2, 1.7, [(ID.low, 0)])
    step(ID.near_k0a, 0.15, [(ID.low, 3.4), (ID.low2, 0)])
    step(ID.low3, 1.7, [(ID.low2, 0)])
    step(ID.near_k0b, 0.15, [(ID.near_k0a, 0), (ID.low3, 0)])
    step(ID.own_hi, 1.7, [(ID.low3, 0)])
    step(ID.collect1, 0.9, [(ID.own_hi, 0), (ID.near_k1b, 7.0)], posts=[(ID.ga1, u, DS) for u in hi])
    step(ID.own_lo, 0.9, [(ID.collect1, 0)])
    step(ID.finish_w1, 0.3, [(ID.near_w1, 8.0), (ID.near_k0b, 0)], low=1)
    step(ID.aw, 0.6, [(ID.own_lo, 0)], low=1)
    step(ID.collect0, 0.9, [(ID.own_lo, 0), (ID.near_k0b, 7.0)], posts=[(ID.ga1, u, DS) for u in lo])
    step(ID.weights_c, 0.7, [(ID.collect0, 0), (ID.aw, 0)], low=1)
    step(ID.weights_d, 0.3, [(ID.weights_c, 3.0)], low=1)
    step(ID.near_w2, 0.2, [(ID.weights_d, 3.5)], low=1)
    step(ID.relay_w1, 0.05, [(ID.finish_w1, 6.5)], low=1)
    step(ID.finish_w2, 0.2, [(ID.near_w2, 5.0)], low=1)
    step(ID.relay_w2, 0.05, [(ID.finish_w2, 4.0)], low=1)
    step(ID.pair_w1, 0.05, [(ID.relay_w1, 5.0)], low=1)
    step(ID.give_w1, 0.05, [(ID.pair_w1, 4.5)], low=1)
    step(ID.give_o, 0.1, [((ID.out_, U - 1), 2.0)], every(ID.out, range(U)), low=1)
    step(ID.sums, 0.2, needs=every(ID.small, [0]), low=1)
    step(ID.pair_w2, 0.05, [(ID.relay_w2, 3.5)], low=1)
    step(ID.give_v, 0.1, [(ID.sums, 3.0)], low=1)
    step(ID.give_w2, 0.05, [(ID.pair_w2, 3.0)], low=1)
    step(ID.give_hi, 0.1, [(ID.give_o, 0)], every(ID.ga1, hi), low=1)
    step(ID.end, 0.0, [(ID.give_v, 0), (ID.give_hi, 0), (ID.give_w1, 0), (ID.give_w2, 0)], every(ID.ga1, range(U)))
    return jobs, m


def scratch_list(R, T, D, F, nh):
    NG = R // 2
    N = 4 * BLK
    v = pltpu.VMEM
    rows = v((8, 64, D), BF)
    return dict(
        tok_raw=(rows),
        cot_raw=(rows),
        stage=(v((2, 2, 2, 64, D), BF)),
        x=(rows),
        cot=(rows),
        wqt=(v((640, D), BF)),
        wo=(v((T, 2, nh * HEAD // 2, D), BF)),
        wolo=(v((nh, T, BLK, D), BF)),
        wohi=(v((nh, T, BLK, D), BF)),
        wopad=(v((nh * BLK, D), BF)),
        fc=(v((D, F), BF)),
        pw=(v((F, D), BF)),
        brow=(v((1, 640), F32)),
        act1=(rows),
        q=(v((nh, N, 128), BF)),
        kv=(v((NG, nh, N, 128), BF)),
        pre=(v((N, D), F32)),
        ga=(v((N, F), F32)),
        hid=(v((8, 64, D), F32)),
        act2=(v((N, D), BF)),
        actd=(v((N, F), BF)),
        gpre=(v((N, F), BF)),
        mlo=(v((4 if NG == 4 else 1, 256, 256), F32)),
        mhi=(v((4 if NG == 4 else 1, 256, 256), F32)),
        m=(v((2 * nh, 1, 256), F32)),
        l=(v((2 * nh, 1, 256), F32)),
        delta=(v((2 * nh, 1, 256), F32)),
        acc=(v((2 * nh, 128, 256), F32)),
        attp=(v((nh, N, 128), BF)),
        attn=(v((N, 256), BF)),
        ab=(v((T, nh, 256, 128), BF)),
        p1=(rows), r1=(rows), l1=(rows),
        r2=(rows), l2=(rows),
        r3=(rows), l3=(rows),
        gh=(v((2, 64, D), F32)),
        h=(rows),
        do=(v((nh, N, 128), BF)),
        dkf=(v((4 if NG == 4 else 1, nh, 256, 128), F32)),
        dk=(v((NG, nh, N, 128), BF)),
        dkr=(v((NG, nh, N, 128), BF)),
        dka=(v((2, 2, nh, 128, 128), BF)),
        gn=(v((N, 640), BF)),
        w1=(v((2, NG, D // NG, D), BF)),
        w1r=(v((NG, D // NG, D), BF)),
        w1s=(v((NG, D // NG, D), BF)),
        w1a=(v((2, D // NG // 2, D), BF)),
        w1f=(v((2, NG, D // NG, D), BF)),
        w2=(v((2, NG, D // 2 // NG, D), BF)),
        w2r=(v((NG, D // 2 // NG, D), BF)),
        w2s=(v((NG, D // 2 // NG, D), BF)),
        w2a=(v((2, D // 2 // NG // 2, D), BF)),
        w2f=(v((2, NG, D // 2 // NG, D), BF)),
        yo=(rows),
        yg=(rows),
        mo=(v((2, 2, 64, D), BF)),
        mg=(v((2, 2, 64, D), BF)),
        vsum=(v((16, D), F32)),
        vz=(v((T, 16, D), BF)),
        vc=(v((R, 16, D), BF)),
        ss=(pltpu.SemaphoreType.DMA((SENDS if NG == 4 else 200,))),
        rs=(pltpu.SemaphoreType.DMA((ARRIVALS if NG == 4 else 400,))),
        ls=(pltpu.SemaphoreType.DMA((24,))),
    )


def layer_kernel(R, T, D, F, nh, names, *refs):
    (pos_ref, seq_ref, tok_hbm, cot_hbm, g1_ref, b1_ref, wqt_hbm, qvb_ref, wo_hbm, ob_ref, g2_ref,
     b2_ref, fc_hbm, fcb_ref, pw_hbm, pb_ref, w1_out, w2_out, fo_out, fg_out, v_out) = refs[:21]
    s = SimpleNamespace(**dict(zip(names, refs[21:])))
    s.p2, s.p3 = s.tok_raw, s.cot_raw
    NG = R // 2
    N = 4 * BLK
    Q1 = D // NG
    Q2 = D // 2 // NG
    SUB = U // 2
    RU = 64 // SUB
    r = lax.axis_index("ctx")
    z = lax.axis_index("tp")
    c = lax.rem(r, 2)
    o = 1 - c
    g = lax.div(r, 2)
    mate = 2 * g + o
    zp, zm = z + 1, z - 1
    not_core = [c != 0, c != 1]
    if NG == 4:
        ga_ = g + 1 - 2 * lax.rem(g, 2)
        gb_ = g + 2 - 4 * lax.div(g, 2)
        gc_ = ga_ + 2 - 4 * lax.div(ga_, 2)
        peers = [g, ga_, gb_, gc_]
        sources = peers
    else:
        peers = [lax.rem(g + t, NG) for t in range(NG)]
        sources = [lax.rem(g + NG - t, NG) for t in range(NG)]

    most = {ID.common: 0, ID.line: 0}
    spare = {ID.common: [], 0: [], 1: [], 2: [], 3: []}
    started = [[], []]
    ids = [0]
    SPLIT = SPLIT_AT if NG == 4 else 100

    def take(pool):
        if spare[pool]:
            return spare[pool].pop(0)
        kind = ID.common if pool == ID.common else pool
        most[kind] = most.get(kind, 0) + 1
        return most[kind] - 1 + (0 if pool == ID.common else SPLIT)

    def flush(last=False):
        for batch in ([started[0]] if not last else started):
            for pool in (ID.common, 0, 1, 2, 3):
                mine = [e for e in batch if e[0] == pool]
                if pool == ID.common:
                    for _, _, done in mine:
                        done()
                elif mine:
                    @pl.when(z == pool)
                    def _(mine=mine):
                        for _, _, done in mine:
                            done()
                spare[pool].extend(e[1] for e in mine)
        started[0] = started[1]
        started[1] = []

    def new(count=1):
        first = ids[0]
        ids[0] += count
        return first

    def remote(src, dst, mine, slot, dev):
        src = src() if callable(src) else src
        dst = dst() if callable(dst) else dst
        return pltpu.make_async_remote_copy(
            src_ref=src, dst_ref=dst, send_sem=s.ss.at[mine], recv_sem=s.rs.at[slot],
            device_id=dev, device_id_type=MESH)

    def send(src, dst, slot, dev, cond=None, at=None):
        pool = ID.common if at is None else at
        mine = take(pool)

        def go():
            remote(src, dst, mine, slot, dev).start()

        def done():
            remote(src, dst, mine, slot, dev).wait_send()

        if cond is None:
            go()
            started[1].append((pool, mine, done))
        else:
            pl.when(cond)(go)
            started[1].append((pool, mine, lambda: pl.when(cond)(done)))

    def arrived(dst, slot, cond=None):
        def go():
            remote(dst, dst, 0, slot, (r, z)).wait_recv()

        if cond is None:
            go()
        else:
            pl.when(cond)(go)

    loads = {}

    def load(name, src, dst, k):
        loads[name] = pltpu.make_async_copy(src, dst, s.ls.at[k])
        loads[name].start()

    load(ID.tok, tok_hbm, s.tok_raw, 0)
    load(ID.wqt, wqt_hbm, s.wqt.at[pl.ds(0, 3 * nh * HEAD)], 1)
    load(ID.wo, wo_hbm, s.wo.at[z], 3)
    load(ID.cot, cot_hbm, s.cot_raw, 2)
    load(ID.pw, pw_hbm, s.pw, 4)
    load(ID.fc, fc_hbm, s.fc, 5)

    barrier = pltpu.get_barrier_semaphore()
    for t in range(1, R):
        pl.semaphore_signal(barrier, inc=1, device_id=(lax.rem(r + t, R), z), device_id_type=MESH)

    for t in range(1, T):
        pl.semaphore_signal(barrier, inc=1, device_id=(r, lax.rem(z + t, T)), device_id_type=MESH)
    pl.semaphore_wait(barrier, R + T - 2)

    def find(seq):
        low = jnp.int32(0)
        high = jnp.int32(0)
        for b in range(4):
            same = seq_ref[4 * r + b] == seq
            first = pos_ref[4 * r + b] < R
            low = jnp.where(same & first, b, low)
            high = jnp.where(same & jnp.logical_not(first), b, high)
        return low, high

    def low_pos(rank):
        total = jnp.int32(0)
        for b in range(4):
            here = (seq_ref[4 * rank + b] == c) & (pos_ref[4 * rank + b] < R)
            total = total + jnp.where(here, pos_ref[4 * rank + b], 0)
        return total

    other = find(o)
    own = find(c)
    q_low = (low_pos(2 * g), low_pos(2 * g + 1))

    def swap(raw, k_stage, dst, base):
        for k in range(2):
            s.stage[k_stage, k] = raw[pl.ds(2 * other[k], 2)]
            send(s.stage.at[k_stage, k], dst.at[pl.ds(4 * k + 2 * c, 2)], base + k, (mate, z))
        for k in range(2):
            dst[pl.ds(4 * k + 2 * c, 2)] = raw[pl.ds(2 * own[k], 2)]

    def swapped(dst, base):
        for k in range(2):
            arrived(dst.at[pl.ds(4 * k + 2 * o, 2)], base + k)

    sx = new(4)
    loads[ID.tok].wait()
    swap(s.tok_raw, 0, s.x, sx)

    class Gather:
        def __init__(self, at, pieces, pass_on=None):
            self.at, self.hand = at, pass_on
            self.base = [new(T) for _ in range(pieces)]

        def start(self, u):
            for zz in range(T):
                @pl.when(z == zz)
                def _(zz=zz):
                    a = lambda: self.at(zz, u)
                    if zz < T - 1:
                        send(a, a, self.base[u] + zz, (r, zp), at=zz)
                    if zz > 0:
                        send(a, a, self.base[u] + zz, (r, zm), at=zz)

        def one(self, op, at):
            _, i, u, _ = op
            slot = self.base[u] + i
            a = lambda: self.at(i, u)
            arrived(a, slot)
            if at > i and at < T - 1:
                send(a, a, slot, (r, zp), at=at)
            if at < i and at > 0:
                send(a, a, slot, (r, zm), at=at)
            if self.hand is not None:
                self.hand(i, u, at)

    class Direct:
        def __init__(self, at, pieces):
            self.at = at
            self.base = [new(T) for _ in range(pieces)]

        def start(self, u):
            a = self.at(z, u)
            for t in range(1, T):
                send(a, a, self.base[u] + t, (r, lax.rem(z + t, T)))

        def one(self, op, at):
            _, i, u, _ = op
            arrived(lambda: self.at(i, u), self.base[u] + (at - i) % T)

    def piece(buf, i, u):
        half = 1 if u < SUB else 0
        if SUB == 1:
            return buf.at[4 * half + i]
        return buf.at[4 * half + i, pl.ds(RU * (u % SUB), RU)]

    class Sum:
        def __init__(self, part, from_left, from_right, whole, landing=None):
            self.part, self.fl, self.fr = part, from_left, from_right
            self.whole, self.landing = whole, landing
            self.rl = [new(T + 1) for _ in range(U)]
            self.ag = [new(T) for _ in range(U)]
            self.hand = [new(2) for _ in range(U)] if landing is not None else None

            @pl.when(z == 0)
            def _():
                from_left[0] = jnp.zeros((64, D), BF)
                from_left[4] = jnp.zeros((64, D), BF)

            @pl.when(z == T - 1)
            def _():
                from_right[T - 1] = jnp.zeros((64, D), BF)
                from_right[4 + T - 1] = jnp.zeros((64, D), BF)

        def begin(self, u, ds=(3, 2, 1)):
            @pl.when(z == 0)
            def _():
                for d in ds:
                    send(self.see(self.part, d, u), self.see(self.fl, d, u), self.rl[u] + d, (r, zp), at=0)

            @pl.when(z == T - 1)
            def _():
                for d in ds:
                    e = T - 1 - d
                    send(self.see(self.part, e, u), self.see(self.fr, e, u), self.slot(u, e, T - 2), (r, zm), at=T - 1)

        def slot(self, u, d, to):
            return self.rl[u] + (T if d == to else d)

        def see(self, buf, i, u):
            return lambda: piece(buf, i, u)

        def one(self, op, at):
            kind, i, u, _ = op
            if kind == ID.A:
                slot = self.ag[u] + i
                a = self.see(self.whole, i, u)
                arrived(a, slot)
                if at > i and at < T - 1:
                    send(a, a, slot, (r, zp), at=at)
                if at < i and at > 0:
                    send(a, a, slot, (r, zm), at=at)
                self.pass_on(i, u, at)
                return
            right = kind == ID.R
            buf = self.fl if right else self.fr
            arrived(self.see(buf, i, u), self.rl[u] + i)
            slot = self.rl[u] + i if right else self.slot(u, i, at - 1)
            a = piece(self.part, i, u)
            a[...] = (a[...].astype(F32) + piece(buf, i, u)[...].astype(F32)).astype(BF)
            send(self.see(self.part, i, u), self.see(buf, i, u), slot, (r, zp if right else zm), at=at)

        def spot(self, i, u):
            half = 1 if u < SUB else 0
            if SUB == 1:
                return self.landing.at[half, i % 2]
            return self.landing.at[half, i % 2, pl.ds(RU * (u % SUB), RU)]

        def pass_on(self, i, u, at):
            if self.landing is None:
                return
            send(self.see(self.whole, i, u), lambda: self.spot(i, u), self.hand[u] + i % 2, (mate, z),
                 not_core[i // 2], at=at)

        def last(self, u):
            for at in range(T):
                @pl.when(z == at)
                def _(at=at):
                    if at > 0:
                        arrived(self.see(self.fl, at, u), self.rl[u] + at)
                    if at < T - 1:
                        arrived(self.see(self.fr, at, u), self.rl[u] + T)

        def total(self, index, rows):
            return (self.part[index, rows, :].astype(F32) + self.fl[index, rows, :].astype(F32)
                    + self.fr[index, rows, :].astype(F32))

        def gather(self, u):
            for at in range(T):
                @pl.when(z == at)
                def _(at=at):
                    a = self.see(self.whole, at, u)
                    if at < T - 1:
                        send(a, a, self.ag[u] + at, (r, zp), at=at)
                    if at > 0:
                        send(a, a, self.ag[u] + at, (r, zm), at=at)
                    self.pass_on(at, u, at)

        def handed(self, pieces):
            for u in pieces:
                for k in range(2):
                    arrived(self.spot(k, u), self.hand[u] + k)

    class PlaneSum:
        def __init__(self, part, cut, far, near):
            self.part, self.cut, self.fl, self.near_buf = part, cut, far, near
            self.base = new(max(4, NG))

        def far(self):
            if NG == 4:
                for k in range(2):
                    send(self.part(peers[3], k), self.fl(k), self.base + k, (2 * peers[1 + k] + c, z))

        def near(self, ks=(0, 1)):
            if NG == 4:
                for k in ks:
                    to = peers[2 - k]
                    arrived(self.fl(k), self.base + k)
                    self.cut(to, k)
                    send(self.part(to, None), self.near_buf(2 - k), self.base + 2 + k, (2 * to + c, z))
            else:
                for t in range(1, NG):
                    send(self.part(peers[t], None), self.near_buf(t), self.base + t, (2 * peers[t] + c, z))

        def arrived(self):
            if NG == 4:
                for k in range(2):
                    arrived(self.near_buf(2 - k), self.base + 2 + k)
            else:
                for t in range(1, NG):
                    arrived(self.near_buf(t), self.base + t)

    class PlaneGather:
        def __init__(self, at):
            self.at = at
            self.base = new(max(6, NG))

        def start(self):
            if NG == 4:
                for t, first in ((1, 0), (2, 1)):
                    for leg, half in ((0, first), (1, 1 - first)):
                        a = self.at(g, half)
                        send(a, a, self.base + 2 * (t - 1) + leg, (2 * peers[t] + c, z))
            else:
                for t in range(1, NG):
                    send(self.at(g, None), self.at(g, None), self.base + t, (2 * peers[t] + c, z))

        def relay(self):
            if NG == 4:
                for t, half in ((1, 0), (2, 1)):
                    a = self.at(peers[t], half)
                    arrived(a, self.base + 2 * (t - 1))
                    send(a, a, self.base + 3 + t, (2 * peers[3 - t] + c, z))

        def arrived(self):
            if NG == 4:
                for t, half in ((1, 1), (2, 0)):
                    arrived(self.at(peers[t], half), self.base + 2 * (t - 1) + 1)
                for t, half in ((1, 0), (2, 1)):
                    arrived(self.at(peers[3], half), self.base + 3 + t)
            else:
                for t in range(1, NG):
                    arrived(self.at(sources[t], None), self.base + t)

    WP = nh * HEAD // 4
    swo = new(2 * T)

    def wo_at(i, u, core=None):
        return s.wo.at[i, c if core is None else core, pl.ds(WP * u, WP)]

    def hand_wo(i, u, at):
        send(lambda: wo_at(i, u), lambda: wo_at(i, u), swo + T * u + i, (mate, z), at=at)

    wo_line = Gather(wo_at, 2, hand_wo)
    loads[ID.wo].wait()
    wo_line.start(0)
    wo_line.start(1)
    s.wqt[pl.ds(3 * nh * HEAD, 640 - 3 * nh * HEAD), :] = jnp.zeros((640 - 3 * nh * HEAD, D), BF)
    s.brow[...] = jnp.zeros((1, 640), F32)
    s.brow[:, 0:192] = qvb_ref[0:1, :]
    s.brow[:, 384:576] = qvb_ref[1:2, :]
    g1 = g1_ref[...].reshape(1, -1)
    b1 = b1_ref[...].reshape(1, -1)
    lo_a, hi_a = pl.ds(0, 256), pl.ds(256, 256)

    def project(first):
        for k in range(2):
            for i in range(2):
                j = 4 * k + 2 * first + i
                n, _inv = normed(s.x[j].astype(F32))
                s.act1[j] = (n * g1 + b1).astype(BF)
        a = jnp.concatenate([s.act1[pl.ds(4 * k + 2 * first, 2)].reshape(BLK, D) for k in range(2)], axis=0)
        s.pre[0:256, 0:640] = dg(a, s.wqt[...], 1, 1)
        low = lax.broadcasted_iota(jnp.int32, (BLK, 128), 1) < HEAD
        zero = jnp.zeros((BLK, 128), F32)
        for k in range(2):
            t = [s.pre[BLK * k:BLK * k + BLK, 128 * i:128 * i + 128] + s.brow[:, 128 * i:128 * i + 128]
                 for i in range(5)]
            rows = pl.ds(pl.multiple_of((2 * k + first) * BLK, BLK), BLK)
            s.kv[g, 0, rows, :] = jnp.where(low, roll64(t[1]), roll64(t[3])).astype(BF)
            s.kv[g, 1, rows, :] = jnp.where(low, t[2], t[3]).astype(BF)
            s.kv[g, 2, rows, :] = jnp.where(low, roll64(t[2]), roll64(t[4])).astype(BF)
            s.q[0, rows, :] = (jnp.where(low, t[0], zero) * 0.125).astype(BF)
            s.q[1, rows, :] = (jnp.where(low, roll64(t[0]), zero) * 0.125).astype(BF)
            s.q[2, rows, :] = (jnp.where(low, t[1], zero) * 0.125).astype(BF)

    loads[ID.wqt].wait()
    project(c)
    swapped(s.x, sx)
    project(o)

    skv = new(max(6 * nh, NG))

    def kv_go(h, leg):
        for t, halves in ((1, (lo_a, hi_a)), (2, (hi_a, lo_a))):
            a = s.kv.at[g, h, halves[leg]]
            send(a, a, skv + 6 * h + 2 * (t - 1) + leg, (2 * peers[t] + c, z))

    def kv_relay(h):
        for t, to, half in ((1, 2, lo_a), (2, 1, hi_a)):
            a = s.kv.at[peers[t], h, half]
            arrived(a, skv + 6 * h + 2 * (t - 1))
            send(a, a, skv + 6 * h + 3 + t, (2 * peers[to] + c, z))

    def kv_rest(h):
        for t, half in ((1, hi_a), (2, lo_a)):
            arrived(s.kv.at[peers[t], h, half], skv + 6 * h + 2 * (t - 1) + 1)

    def kv_far(h):
        for t, half in ((1, lo_a), (2, hi_a)):
            arrived(s.kv.at[peers[3], h, half], skv + 6 * h + 3 + t)

    def masks(src):
        k_low = (low_pos(2 * src), low_pos(2 * src + 1))
        i0 = lax.broadcasted_iota(jnp.int32, (256, 256), 0)
        i1 = lax.broadcasted_iota(jnp.int32, (256, 256), 1)

        def token(i, a, b):
            return i + jnp.where(i < BLK, a * BLK, b * BLK - BLK)

        last = 2 * R - 1
        low_mask = jnp.where(token(i0, *k_low) <= token(i1, *q_low), 0.0, NEG)
        high_mask = jnp.where(
            token(i0, last - k_low[0], last - k_low[1])
            <= token(i1, last - q_low[0], last - q_low[1]), 0.0, NEG)
        return low_mask, high_mask

    def all_masks():
        for t in range(4):
            s.mlo[t], s.mhi[t] = masks(peers[t])

    def keys_of(src, h):
        return s.kv[src, h, 0:256, :], s.kv[src, h, 256:512, :]

    def attend(groups, h, fresh=False):
        for half in range(2):
            at = 2 * h + half
            qs = s.q[h, 256 * half:256 * half + 256, :]
            tiles = []
            for src, mlo, mhi in groups:
                klo, khi = keys_of(src, h)
                if half == 0:
                    tiles.append((klo, dg(klo, qs, 1, 1) + mlo[...]))
                else:
                    tiles.append((klo, dg(klo, qs, 1, 1)))
                    tiles.append((khi, dg(khi, qs, 1, 1) + mhi[...]))
            now = None if fresh else s.m[at]
            old = now
            for _, sc in tiles:
                top = jnp.max(sc, axis=0, keepdims=True)
                now = top if now is None else jnp.maximum(now, top)
            total = value = None
            for k, sc in tiles:
                e = jnp.exp(sc - now)
                part = jnp.sum(e, axis=0, keepdims=True)
                total = part if total is None else total + part
                part = dg(k, e.astype(BF), 0, 0)
                value = part if value is None else value + part
            if fresh:
                s.l[at] = total
                s.acc[at] = value
            else:
                f = jnp.exp(old - now)
                s.l[at] = s.l[at] * f + total
                s.acc[at] = s.acc[at] * f + value
            s.m[at] = now

    low = lax.broadcasted_iota(jnp.int32, (256, 128), 1) < HEAD
    low_s = lax.broadcasted_iota(jnp.int32, (BLK, 128), 1) < HEAD

    def settle(h):
        outs = []
        for half in range(2):
            rows = pl.ds(256 * half, 256)
            outs.append(jnp.transpose(s.acc[2 * h + half] / s.l[2 * h + half]))
            s.attp[h, rows, :] = outs[half].astype(BF)
            s.m[2 * h + half] = s.m[2 * h + half] + jnp.log(s.l[2 * h + half])
        if h < nh - 1:
            s.ab[z, h] = jnp.where(low, roll64(outs[0]), outs[1]).astype(BF)
        else:
            for place, half in ((0, 1), (1, 0)):
                v = outs[half]
                s.ab[z, h, BLK * place:BLK * place + BLK, :] = jnp.where(
                    low_s, roll64(v[0:BLK]), v[BLK:256]).astype(BF)

    ab_line = Gather(lambda i, u: s.ab.at[i, u], nh - 1)
    ac_line = Gather(lambda i, u: s.ab.at[i, nh - 1, pl.ds(BLK * u, BLK)], 2)

    sum1 = Sum(s.p1, s.r1, s.l1, s.h)
    sum2 = Sum(s.p2, s.r2, s.l2, s.yo, s.mo)
    sum3 = Sum(s.p3, s.r3, s.l3, s.yg, s.mg)
    s.vsum[...] = jnp.zeros((16, D), F32)

    def upstream():
        swapped(s.cot, sx + 2)
        loads[ID.pw].wait()
        for half in range(2):
            s.ga[256 * half:256 * half + 256, :] = dg(
                s.cot[4 * half:4 * half + 4].reshape(256, D), s.pw[...], 1, 1)

    zeros = jnp.zeros((HEAD, D), BF)

    def pad_own():
        mine = s.wo[z].reshape(nh * HEAD, D)
        for h in range(nh):
            s.wopad[BLK * h:BLK * h + HEAD, :] = zeros
            s.wopad[BLK * h + HEAD:BLK * h + BLK, :] = mine[HEAD * h:HEAD * h + HEAD]

    def pad_all():
        for t in range(1, T):
            for u in range(2):
                arrived(wo_at(lax.rem(z + t, T), u, o), swo + T * u + lax.rem(z + t, T))
        for t in range(T):
            w = s.wo[t].reshape(nh * HEAD, D)
            for h in range(nh):
                part = w[HEAD * h:HEAD * h + HEAD]
                s.wolo[h, t, 0:HEAD, :] = part
                s.wolo[h, t, HEAD:BLK, :] = zeros
                s.wohi[h, t, 0:HEAD, :] = zeros
                s.wohi[h, t, HEAD:BLK, :] = part

    def early_mix():
        for half, w in ((1, s.wohi), (0, s.wolo)):
            total = None
            for h in range(nh - 1):
                a = jnp.concatenate([s.ab[t, h] for t in range(T)], axis=1)
                part = dg(a, w[h].reshape(T * BLK, D), 1, 0)
                total = part if total is None else total + part
            s.pre[256 * half:256 * half + 256, :] = total

    def group(t):
        return peers[t], s.mlo.at[t], s.mhi.at[t]

    def own_keys():
        all_masks()
        for h in range(nh):
            attend([group(0)], h, True)

    def near_keys(h):
        attend([group(1), group(2)], h)

    def far_keys(h):
        kv_far(h)
        attend([group(3)], h)
        settle(h)
        if h < nh - 1:
            ab_line.start(h)
        else:
            ac_line.start(0)
            ac_line.start(1)

    def step_a():
        kv_relay(0)
        kv_go(1, 1)

    def step_b():
        kv_rest(0)
        near_keys(0)

    def step_c():
        kv_relay(1)
        kv_go(2, 0)
        kv_go(2, 1)

    def step_d():
        kv_rest(1)
        near_keys(1)

    def step_e():
        kv_rest(2)
        near_keys(2)

    def whole():
        def one_group(src, fresh):
            s.mlo[0], s.mhi[0] = masks(src)
            for h in range(nh):
                attend([(src, s.mlo.at[0], s.mhi.at[0])], h, fresh)

        one_group(g, True)
        for t in range(1, NG):
            arrived(s.kv.at[sources[t]], skv + t)

        def rest(t, _):
            one_group(lax.rem(g + t, NG), False)
            return 0

        lax.fori_loop(1, NG, rest, 0)
        for h in range(nh):
            settle(h)

    def pads():
        pad_own()
        pad_all()

    g2 = g2_ref[...].reshape(1, -1)
    b2 = b2_ref[...].reshape(1, -1)
    ob = ob_ref[...].reshape(1, -1)
    fcb = fcb_ref[...].reshape(1, -1)
    pb = pb_ref[...].reshape(1, -1)

    def feed(half, total):
        place = 1 - half
        a = jnp.concatenate([s.ab[t, nh - 1, BLK * place:BLK * place + BLK, :] for t in range(T)], axis=1)
        base = 256 * half
        for k, w in ((0, s.wolo), (1, s.wohi)):
            s.pre[base + BLK * k:base + BLK * k + BLK, :] += dg(a, w[nh - 1].reshape(T * BLK, D), 1, 0)

        def norm2(i, _):
            j = 4 * half + i
            rows = pl.ds(pl.multiple_of(base + i * 64, 64), 64)
            x = s.x[j].astype(F32) + s.pre[rows, :] + ob
            s.hid[j] = x
            n, _inv = normed(x)
            s.act2[rows, :] = (n * g2 + b2).astype(BF)
            return 0

        lax.fori_loop(0, 4, norm2, 0)
        part = pl.ds(base, 256)
        s.pre[part, :] = dg(s.act2[part, :], s.fc[...], 1, 0)

        def gelu(i, total):
            rows = pl.ds(pl.multiple_of(base + i * 32, 32), 32)
            v = s.pre[rows, :] + fcb
            square = v * v
            th = jnp.tanh(C0 * (v + C1 * square * v))
            one = 1.0 + th
            s.actd[rows, :] = (0.5 * v * one).astype(BF)
            slope = 0.5 * one + (0.5 * v) * (1.0 - th * th) * (C0 * (1.0 + 3.0 * C1 * square))
            grad = slope * s.ga[rows, :]
            s.gpre[rows, :] = grad.astype(BF)
            return total + fold8(grad)

        total = lax.fori_loop(0, 8, gelu, total)
        s.p1[4 * half:4 * half + 4] = dg(s.gpre[part, :], s.fc[...], 1, 1).astype(BF).reshape(4, 64, D)
        return total

    bias = []

    def feed1():
        loads[ID.fc].wait()
        bias.append(feed(1, jnp.zeros((8, F), F32)))
        for u in range(SUB):
            sum1.begin(u)

    def feed0():
        s.vsum[8:9, :] = jnp.sum(feed(0, bias[0]), axis=0, keepdims=True)
        for u in range(SUB, U):
            sum1.begin(u)

    sw1 = new(2)

    def weight(dst, index, lhs, rhs):
        for i in range(3):
            part = dg(lhs[:, 256 * i:256 * i + 256], rhs, 0, 0).astype(BF)
            lo, hi = 256 * i, 256 * i + 256
            for qd in range(NG):
                a, b = max(lo, qd * Q1), min(hi, qd * Q1 + Q1)
                if a < b:
                    dst[index, qd, a - qd * Q1:b - qd * Q1, :] = part[a - lo:b - lo]

    def add_into(buf, index, extra):
        def body(i, _):
            buf[index, i] = (buf[index, i].astype(F32) + extra[i].astype(F32)).astype(BF)
            return 0

        lax.fori_loop(0, NG, body, 0)

    def weights_a():
        weight(s.w1, 0, s.actd, s.cot[...].reshape(N, D))

    def weights_a2():
        weight(s.w1, 1, s.act2, s.gpre[...])
        send(s.w1.at[o], s.w1r, sw1, (mate, z))

    def plane(part, land, near, whole, size):
        half = size // 2

        def of(buf):
            return lambda i, k: buf.at[c, i] if k is None else buf.at[c, i, pl.ds(half * k, half)]

        def cut(to, k):
            rows = pl.ds(half * k, half)
            part[c, to, rows, :] = (part[c, to, rows, :].astype(F32) + land[k].astype(F32)).astype(BF)

        total = PlaneSum(of(part), cut, lambda k: land.at[k], lambda t: near.at[t])
        share = PlaneGather(of(whole))

        def finish():
            total.arrived()
            step = size // 3

            def body(i, _):
                rows = pl.ds(pl.multiple_of(i * step, step), step)
                v = part[c, g, rows, :].astype(F32)
                for t in got:
                    v = v + near[t, rows, :].astype(F32)
                whole[c, g, rows, :] = v.astype(BF)
                return 0

            lax.fori_loop(0, 3, body, 0)
            share.start()

        return total, share, finish

    got = [1, 2] if NG == 4 else list(range(1, NG))
    total1, share1, finish1 = plane(s.w1, s.w1a, s.w1s, s.w1f, Q1)
    total2, share2, finish2 = plane(s.w2, s.w2a, s.w2s, s.w2f, Q2)

    def weights_b():
        arrived(s.w1r, sw1)
        add_into(s.w1, c, s.w1r)
        total1.far()

    def out_partial():
        for half in range(2):
            base = 256 * half
            s.p2[4 * half:4 * half + 4] = dg(
                s.actd[base:base + 256, :], s.pw[...], 1, 0).astype(BF).reshape(4, 64, D)

    def spans(u):
        half = 1 if u < SUB else 0
        step = min(RU, 32)
        return half, 4 * half + z, [pl.ds(RU * (u % SUB) + step * i, step) for i in range(RU // step)]

    def back2(u):
        sum1.last(u)
        half, index, parts = spans(u)
        sums = [jnp.zeros((8, D), F32)] * 4
        for rows in parts:
            n, inv = normed(s.hid[index, rows, :])
            grad = sum1.total(index, rows)
            up = s.cot[index, rows, :].astype(F32)
            qg = grad * g2
            gh = up + inv * (qg - jnp.mean(qg, axis=-1, keepdims=True)
                             - n * jnp.mean(qg * n, axis=-1, keepdims=True))
            s.gh[half, rows, :] = gh
            s.h[index, rows, :] = gh.astype(BF)
            for k, part in enumerate((grad * n, grad, gh, up)):
                sums[k] = sums[k] + fold8(part)
        sum1.gather(u)
        for k in range(4):
            s.vsum[2 + k:3 + k, :] += jnp.sum(sums[k], axis=0, keepdims=True)

    def slopes(half):
        rows = pl.ds(256 * half, 256)
        grads = dg(s.h[4 * half:4 * half + 4].reshape(256, D), s.wopad[...], 1, 1)
        for h in range(nh):
            d = grads[:, 128 * h:128 * h + 128].astype(BF)
            s.do[h, rows, :] = d
            both = d.astype(F32) * s.attp[h, rows, :].astype(F32)
            s.delta[2 * h + half] = jnp.sum(jnp.transpose(both), axis=0, keepdims=True)

    def tile(k, h, half, mask):
        qs = s.q[h, 256 * half:256 * half + 256, :]
        ds_ = s.do[h, 256 * half:256 * half + 256, :]
        sc = dg(k, qs, 1, 1)
        if mask is not None:
            sc = sc + mask[...]
        p = jnp.exp(sc - s.m[2 * h + half])
        d = p * (dg(k, ds_, 1, 1) - s.delta[2 * h + half])
        p = p.astype(BF)
        d = d.astype(BF)
        return d, dg(d, qs, 1, 0) + dg(p, ds_, 1, 0)

    def back_high(src, mhi, fresh):
        for h in range(nh):
            _, khi = keys_of(src, h)
            d3, k3 = tile(khi, h, 1, mhi)
            s.dk[src, h, 256:512, :] = k3.astype(BF)
            if fresh:
                s.acc[2 * h + 1] = dg(khi, d3, 0, 0)
            else:
                s.acc[2 * h + 1] += dg(khi, d3, 0, 0)

    def back_mid(src, t):
        for h in range(nh):
            klo, _ = keys_of(src, h)
            d2, k2 = tile(klo, h, 1, None)
            s.dkf[t, h] = k2
            s.acc[2 * h + 1] += dg(klo, d2, 0, 0)

    def back_low(src, t, mlo, fresh):
        for h in range(nh):
            klo, _ = keys_of(src, h)
            d1, k1 = tile(klo, h, 0, mlo)
            s.dk[src, h, 0:256, :] = (s.dkf[t, h] + k1).astype(BF)
            if fresh:
                s.acc[2 * h] = dg(klo, d1, 0, 0)
            else:
                s.acc[2 * h] += dg(klo, d1, 0, 0)

    def key_sum(half):
        rows = pl.ds(256 * half, 256)

        def part(i, k):
            return s.dk.at[i, :, rows if k is None else pl.ds(256 * half + BLK * k, BLK)]

        def cut(to, k):
            some = pl.ds(256 * half + BLK * k, BLK)
            for h in range(nh):
                s.dk[to, h, some, :] = (s.dk[to, h, some, :].astype(F32) + s.dka[half, k, h].astype(F32)).astype(BF)

        return PlaneSum(part, cut, lambda k: s.dka.at[half, k], lambda t: s.dkr.at[t, :, rows])

    keys = [key_sum(0), key_sum(1)]

    def finish_output(u):
        sum2.last(u)
        half, index, parts = spans(u)
        for rows in parts:
            s.yo[index, rows, :] = (s.hid[index, rows, :] + sum2.total(index, rows) + pb).astype(BF)
        sum2.gather(u)

    col = [jnp.zeros((1, 128), F32) for _ in range(5)]

    def collect(half):
        keys[half].arrived()
        rows = pl.ds(256 * half, 256)
        dq = [jnp.transpose(s.acc[2 * h + half]) * 0.125 for h in range(nh)]
        dkv = []
        for h in range(nh):
            total = s.dk[g, h, rows, :].astype(F32)
            for t in got:
                total = total + s.dkr[t, h, rows, :].astype(F32)
            dkv.append(total)
        tiles = [
            jnp.where(low, dq[0], roll64(dq[1])),
            jnp.where(low, dq[2], roll64(dkv[0])),
            jnp.where(low, dkv[1], roll64(dkv[2])),
            jnp.where(low, roll64(dkv[0]), dkv[1]),
            jnp.where(low, roll64(dkv[2]), 0.0),
        ]
        for j in range(5):
            col[j] = col[j] + jnp.sum(tiles[j], axis=0, keepdims=True)
            s.gn[rows, 128 * j:128 * j + 128] = tiles[j].astype(BF)
        s.p3[4 * half:4 * half + 4] = dg(s.gn[rows, :], s.wqt[...], 1, 0).astype(BF).reshape(4, 64, D)
        for u in range(SUB) if half == 1 else range(SUB, U):
            sum3.begin(u)

    def put2(first, value, rows):
        done = 0
        while done < rows:
            at, off = divmod(first + done, Q2)
            n = min(Q2 - off, rows - done)
            s.w2[at // NG, at % NG, off:off + n, :] = value[done:done + n].astype(BF)
            done += n

    sw2 = new(2)

    def attention_weight():
        for half in range(2):
            rows = pl.ds(256 * half, 256)
            a = [s.attp[h, rows, :].astype(F32) for h in range(nh)]
            s.attn[rows, 0:128] = jnp.where(low, roll64(a[0]), a[1]).astype(BF)
            s.attn[rows, 128:256] = jnp.where(low, roll64(a[2]), 0.0).astype(BF)
        gout = dg(s.attn[...], s.h[...].reshape(N, D), 0, 0)
        put2(3 * nh * HEAD, gout, nh * HEAD)

    def do_high():
        slopes(1)
        back_high(peers[3], s.mhi.at[3], True)
        keys[1].far()

    def do_low():
        slopes(0)
        back_low(peers[3], 3, s.mlo.at[3], True)
        keys[0].far()

    def mid_low(t):
        back_mid(peers[t], t)
        back_low(peers[t], t, s.mlo.at[t], False)

    def own_hi():
        back_high(g, s.mhi.at[0], False)
        back_mid(g, 0)

    def whole_part():
        slopes(0)
        slopes(1)
        for i in range(2 * nh):
            s.acc[i] = jnp.zeros((128, 256), F32)

        def rest_back(t, _):
            src = lax.rem(g + t, NG)
            s.mlo[0], s.mhi[0] = masks(src)
            back_high(src, s.mhi.at[0], False)
            back_mid(src, 0)
            back_low(src, 0, s.mlo.at[0], False)
            return 0

        lax.fori_loop(0, NG, rest_back, 0)
        for half in (1, 0):
            keys[half].near()

    def weights_c():
        for j in range(5):
            s.vsum[9:10, 128 * j:128 * j + 128] = col[j]
        act1 = s.act1[...].reshape(N, D)
        for j in range(5):
            n = min(128, 3 * nh * HEAD - 128 * j)
            put2(128 * j, dg(s.gn[:, 128 * j:128 * j + 128], act1, 0, 0), n)
        send(s.w2.at[o], s.w2r, sw2, (mate, z))

    def weights_d():
        arrived(s.w2r, sw2)
        add_into(s.w2, c, s.w2r)
        total2.far()

    def back1(u):
        sum3.last(u)
        half, index, parts = spans(u)
        sums = [jnp.zeros((8, D), F32)] * 2
        for rows in parts:
            n, inv = normed(s.x[index, rows, :].astype(F32))
            grad = sum3.total(index, rows)
            qg = grad * g1
            gx = s.gh[half, rows, :] + inv * (qg - jnp.mean(qg, axis=-1, keepdims=True)
                                              - n * jnp.mean(qg * n, axis=-1, keepdims=True))
            s.yg[index, rows, :] = gx.astype(BF)
            for k, part in enumerate((grad * n, grad)):
                sums[k] = sums[k] + fold8(part)
        if u < U - 1:
            sum3.gather(u)
        for k in range(2):
            s.vsum[k:k + 1, :] += jnp.sum(sums[k], axis=0, keepdims=True)
        if u == U - 1:
            s.vz[z] = s.vsum[...].astype(BF)
            v_line.start(0)
            sum3.gather(u)

    v_line = Direct(lambda i, u: s.vz.at[i], 1)
    svc = new(R)
    copies = []

    def give(src, dst):
        copy = pltpu.make_async_copy(src, dst, s.ls.at[6 + len(copies)])
        copy.start()
        copies.append(copy)

    def give_rows(whole, landing, out, halves=(0, 1)):
        for k in halves:
            give(whole.at[pl.ds(4 * k + 2 * c, 2)], out.at[k, c])
            give(landing.at[k], out.at[k, o])

    def outputs_a():
        share1.arrived()
        send(s.w1f.at[c], s.w1f.at[c], sw1 + 1, (mate, z))

    def outputs_b():
        arrived(s.w1f.at[o], sw1 + 1)
        give(s.w1f, w1_out)

    def outputs_o():
        sum2.handed(range(U))
        give_rows(s.yo, s.mo, fo_out)

    def outputs_c():
        share2.arrived()
        send(s.w2f.at[c], s.w2f.at[c], sw2 + 1, (mate, z))

    def give_v():
        for t in range(1, R):
            arrived(s.vc.at[lax.rem(r + R - t, R)], svc + t)
        total = s.vc[0].astype(F32)
        for t in range(1, R):
            total = total + s.vc[t].astype(F32)
        s.vsum[...] = total
        give(s.vsum, v_out)

    def give_w2():
        arrived(s.w2f.at[o], sw2 + 1)
        give(s.w2f, w2_out)

    def give_hi():
        sum3.handed(range(SUB))
        give_rows(s.yg, s.mg, fg_out, (1,))

    def small_sums():
        upper = s.vz[0, 0:8, :].astype(F32)
        for t in range(1, T):
            upper = upper + s.vz[t, 0:8, :].astype(F32)
        s.vc[r] = jnp.concatenate([upper, s.vsum[8:16, :]], axis=0).astype(BF)
        for t in range(1, R):
            send(s.vc.at[r], s.vc.at[r], svc + t, (lax.rem(r + t, R), z))

    def go():
        if NG == 4:
            kv_go(0, 0)
            kv_go(0, 1)
            kv_go(1, 0)
        else:
            for t in range(1, NG):
                send(s.kv.at[g], s.kv.at[g], skv + t, (2 * peers[t] + c, z))
        loads[ID.cot].wait()
        swap(s.cot_raw, 1, s.cot, sx + 2)

    steps = {
        ID.go: go, ID.pads: pads, ID.mix: early_mix, ID.feed1: feed1, ID.feed0: feed0, ID.weights_a: weights_a,
        ID.weights_a2: weights_a2, ID.out_partial: out_partial, ID.weights_b: weights_b, ID.near_w1: total1.near,
        ID.collect1: functools.partial(collect, 1), ID.collect0: functools.partial(collect, 0), ID.finish_w1: finish1,
        ID.aw: attention_weight, ID.weights_c: weights_c, ID.weights_d: weights_d, ID.near_w2: total2.near,
        ID.relay_w1: share1.relay, ID.finish_w2: finish2, ID.relay_w2: share2.relay, ID.pair_w1: outputs_a,
        ID.give_w1: outputs_b, ID.give_o: outputs_o, ID.sums: small_sums, ID.pair_w2: outputs_c, ID.give_v: give_v, ID.give_w2: give_w2, ID.give_hi: give_hi,
        ID.upstream: upstream,
    }
    for u in range(U):
        steps[ID.n2_, u] = functools.partial(back2, u)
        for d in DS:
            steps[ID.begin_out, u, d] = functools.partial(sum2.begin, u, (d,))
        steps[ID.out_, u] = functools.partial(finish_output, u)
        steps[ID.n1_, u] = functools.partial(back1, u)
    if NG == 4:
        steps.update({
            ID.own: own_keys, ID.relay0: step_a, ID.near0: step_b, ID.relay1: step_c,
            ID.far0: functools.partial(far_keys, 0), ID.near1: step_d, ID.relay2: functools.partial(kv_relay, 2),
            ID.far1: functools.partial(far_keys, 1), ID.near2: step_e, ID.far2: functools.partial(far_keys, 2),
            ID.high: do_high, ID.high2: functools.partial(back_high, peers[2], s.mhi.at[2], False),
            ID.high3: functools.partial(back_high, peers[1], s.mhi.at[1], False),
            ID.near_k1a: functools.partial(keys[1].near, (0,)), ID.near_k1b: functools.partial(keys[1].near, (1,)),
            ID.mid3: functools.partial(back_mid, peers[3], 3), ID.low: do_low,
            ID.low2: functools.partial(mid_low, 2), ID.low3: functools.partial(mid_low, 1),
            ID.near_k0a: functools.partial(keys[0].near, (0,)), ID.near_k0b: functools.partial(keys[0].near, (1,)),
            ID.own_hi: own_hi, ID.own_lo: functools.partial(back_low, g, 0, s.mlo.at[0], False),
        })
    else:
        steps.update({
            ID.own: whole, ID.far0: lambda: ab_line.start(0), ID.far1: lambda: ab_line.start(1),
            ID.far2: lambda: (ac_line.start(0), ac_line.start(1)), ID.low: whole_part,
        })
    jobs, marks = timetable(U, T)
    timeline, _ = simulate(T, jobs, marks, LAT)
    emit(T, z, timeline, jobs, marks,
         {ID.wo: wo_line, ID.ab: ab_line, ID.ac: ac_line, ID.ga2: sum1, ID.out: sum2, ID.ga1: sum3, ID.small: v_line}, steps, flush)

    sum3.handed(range(SUB, U))
    give_rows(s.yg, s.mg, fg_out, (0,))
    flush(True)
    assert max(v for k, v in most.items() if k != ID.common) + SPLIT <= (SENDS if NG == 4 else 200)
    assert most[ID.common] <= SPLIT and ids[0] <= (ARRIVALS if NG == 4 else 400)
    for copy in copies:
        copy.wait()


def finish_kernel(R, pos_ref, seq_ref, rank_ref, w1_hbm, w2_hbm, fo_hbm, fg_hbm, v_hbm, out_hbm, gt_hbm,
                  ln1g_ref, ln1b_ref, gq_hbm, gqv_ref, go_hbm, ob_ref, ln2g_ref, ln2b_ref, gf_hbm, fb_ref,
                  gp_hbm, pb_ref, w1_in, w2_in, fo_in, fg_in, v_in, w1_wide, w2_wide, sems, back):
    parts = 4
    D = w2_in.shape[0]
    step = D // parts
    reads = []

    def read(src, dst):
        copy = pltpu.make_async_copy(src, dst, sems.at[len(reads)])
        copy.start()
        reads.append(copy)

    for k in range(parts):
        rows = pl.ds(step * k, step)
        for i in range(2):
            read(w1_hbm.at[i, rows], w1_in.at[i, rows])
        read(w2_hbm.at[rows], w2_in.at[rows])
    read(v_hbm, v_in)
    read(fo_hbm, fo_in)
    read(fg_hbm, fg_in)
    writes = []

    def write(src, dst):
        copy = pltpu.make_async_copy(src, dst, back.at[len(writes)])
        copy.start()
        writes.append(copy)

    for k in range(parts):
        rows = pl.ds(step * k, step)
        for i, dst in enumerate((gp_hbm, gf_hbm)):
            reads[3 * k + i].wait()
            w1_wide[i, rows] = w1_in[i, rows].astype(F32)
            write(w1_wide.at[i, rows], dst.at[rows])
        reads[3 * k + 2].wait()
        w2_wide[rows] = w2_in[rows].astype(F32)
        write(w2_wide.at[rows], gq_hbm.at[rows] if k < parts - 1 else go_hbm)
    for copy in reads[3 * parts:]:
        copy.wait()
    for b in range(4):
        at = 4 * rank_ref[0] + b
        high = jnp.where(pos_ref[at] < R, 0, 1)
        write(fo_in.at[high, seq_ref[at]], out_hbm.at[pl.ds(BLK * b, BLK)])
        write(fg_in.at[high, seq_ref[at]], gt_hbm.at[pl.ds(BLK * b, BLK)])
    for ref, k in ((ln1g_ref, 0), (ln1b_ref, 1), (ln2g_ref, 2), (ln2b_ref, 3), (ob_ref, 4), (pb_ref, 5),
                   (fb_ref, 8)):
        ref[...] = v_in[k:k + 1, :].reshape(-1)
    gqv_ref[0:1, :] = v_in[9:10, 0:192]
    gqv_ref[1:2, :] = v_in[9:10, 384:576]
    for copy in writes:
        copy.wait()


def per_device(R, T, tokens, cotangent, block_pos, block_seq, ln1_gain, ln1_bias, qkv_weight, qv_bias,
               out_weight, out_bias, ln2_gain, ln2_bias, fc_weight, fc_bias, proj_weight, proj_bias):
    D = tokens.shape[1]
    F = fc_weight.shape[1]
    local = qkv_weight.shape[2]
    nh = local // HEAD
    NG = R // 2
    sizes = scratch_list(R, T, D, F, nh)
    names = list(sizes)
    row = lambda v: v
    wqt = jnp.transpose(qkv_weight, (1, 2, 0)).reshape(3 * local, D)
    sm = pl.BlockSpec(memory_space=pltpu.SMEM)
    vm = pl.BlockSpec(memory_space=pltpu.VMEM)
    hb = pl.BlockSpec(memory_space=pl.ANY)
    w1, w2, fo, fg, vs = pl.pallas_call(
        functools.partial(layer_kernel, R, T, D, F, nh, names),
        out_shape=(
            jax.ShapeDtypeStruct((2, NG, D // NG, D), BF),
            jax.ShapeDtypeStruct((2, NG, D // 2 // NG, D), BF),
            jax.ShapeDtypeStruct((2, 2, 2, 64, D), BF),
            jax.ShapeDtypeStruct((2, 2, 2, 64, D), BF),
            jax.ShapeDtypeStruct((16, D), F32),
        ),
        in_specs=[sm, sm, hb, hb, vm, vm, hb, vm, hb, vm, vm, vm, hb, vm, hb, vm],
        out_specs=(hb, hb, hb, hb, hb),
        scratch_shapes=list(sizes.values()),
        compiler_params=pltpu.CompilerParams(
            collective_id=0, has_side_effects=True, vmem_limit_bytes=67043328),
        name="layer",
    )(block_pos, block_seq, tokens.reshape(8, 64, D), cotangent.reshape(8, 64, D), row(ln1_gain),
      row(ln1_bias), wqt, qv_bias, out_weight.reshape(2, local // 2, D), row(out_bias), row(ln2_gain), row(ln2_bias), fc_weight,
      row(fc_bias), proj_weight, row(proj_bias))

    rank = lax.axis_index("ctx").astype(jnp.int32).reshape(1)
    vec = jax.ShapeDtypeStruct((D,), F32)
    outs = pl.pallas_call(
        functools.partial(finish_kernel, R),
        out_shape=(
            jax.ShapeDtypeStruct((4 * BLK, D), BF),
            jax.ShapeDtypeStruct((4 * BLK, D), BF),
            vec, vec,
            jax.ShapeDtypeStruct((3 * local, D), F32),
            jax.ShapeDtypeStruct((2, local), F32),
            jax.ShapeDtypeStruct((local, D), F32),
            vec, vec, vec,
            jax.ShapeDtypeStruct((D, F), F32),
            vec,
            jax.ShapeDtypeStruct((F, D), F32),
            vec,
        ),
        in_specs=[sm, sm, sm, hb, hb, hb, hb, hb],
        out_specs=(hb, hb, vm, vm, hb, vm, hb, vm, vm, vm, hb, vm, hb, vm),
        scratch_shapes=[
            pltpu.VMEM((2, D, D), BF), pltpu.VMEM((D, D), BF), pltpu.VMEM((2, 2, BLK, D), BF),
            pltpu.VMEM((2, 2, BLK, D), BF), pltpu.VMEM((16, D), F32), pltpu.VMEM((2, D, D), F32),
            pltpu.VMEM((D, D), F32), pltpu.SemaphoreType.DMA((16,)), pltpu.SemaphoreType.DMA((20,)),
        ],
        name="finish",
    )(block_pos, block_seq, rank, w1.reshape(2, D, D), w2.reshape(D, D),
      fo.reshape(2, 2, BLK, D), fg.reshape(2, 2, BLK, D), vs)
    (output, grad_tokens, ln1g, ln1b, gq, gqv, go, ob, ln2g, ln2b, gf, fb, gp, pb) = outs
    flat = lambda v: v
    return (output, grad_tokens, flat(ln1g), flat(ln1b),
            jnp.transpose(gq.reshape(3, local, D), (2, 0, 1)), gqv, go, flat(ob), flat(ln2g), flat(ln2b),
            gf, flat(fb), gp, flat(pb))


def solution(mesh):
    R = mesh.shape["ctx"]
    T = mesh.shape["tp"]
    return jax.shard_map(
        functools.partial(per_device, R, T),
        mesh=mesh,
        in_specs=(
            P("ctx", None), P("ctx", None), P(), P(), P(), P(), P(None, None, "tp"), P(None, "tp"),
            P("tp", None), P(), P(), P(), P(None, "tp"), P("tp"), P("tp", None), P(),
        ),
        out_specs=(
            P("ctx", None), P("ctx", None), P(), P(), P(None, None, "tp"), P(None, "tp"), P("tp", None),
            P(), P(), P(), P(None, "tp"), P("tp"), P("tp", None), P(),
        ),
        check_vma=False,
    )
```

```python
import functools
from types import SimpleNamespace

import jax
import jax.numpy as jnp
from jax import lax
from jax.experimental import pallas as pl
from jax.experimental.pallas import tpu as pltpu
from jax.sharding import PartitionSpec as P

HEAD = 64
BLK = 128

class Names:
    def __getattr__(self, name):
        return name


ID = Names()
BF = jnp.bfloat16
F32 = jnp.float32
MESH = pl.DeviceIdType.MESH
NEG = -1e30
C0 = 0.7978845608028654
C1 = 0.044715
U = 4
SENDS = 74
SPLIT_AT = 22
ARRIVALS = 174
TIDY = (ID.far1, ID.feed1, ID.weights_b, (ID.n2_, 2), ID.high, ID.low, ID.low3, ID.collect1, ID.collect0, (ID.n1_, 0), (ID.n1_, 2))

LAT = 2.0
OUT_FROM = 15.0
OUT_GAP = 1.0
DS = (3, 2, 1)


def dg(a, b, ca, cb):
    return lax.dot_general(a, b, (((ca,), (cb,)), ((), ())), preferred_element_type=F32)


def normed(x):
    centre = jnp.mean(x, axis=-1, keepdims=True)
    shifted = x - centre
    spread = jnp.mean(shifted * shifted, axis=-1, keepdims=True)
    inverse = lax.rsqrt(spread + 1e-05)
    return shifted * inverse, inverse


def fold8(x):
    rows, width = x.shape
    return jnp.sum(x.reshape(rows // 8, 8, width), axis=0)


def roll64(x):
    return pltpu.roll(x, 64, 1)


def simulate(T, jobs, marks, lat, order=None):
    free = {}
    seen = [dict() for _ in range(T)]
    inbox = [[] for _ in range(T)]
    now = [0.0] * T
    steps = [dict() for _ in range(T)]
    left = [list(marks) if order is None else list(order) for _ in range(T)]
    out = [[] for _ in range(T)]
    parts = [dict() for _ in range(T)]
    OP = 0.12

    def post(time, z, step, op):
        tau = jobs[op[3]][0][op[2]]
        begin = max(time, free.get((z, step), 0.0))
        free[z, step] = begin + tau
        inbox[z + step].append((begin + tau + lat, op))

    transit = []

    def cross(entry):
        time, z, to, op = entry
        step = 1 if to > z else -1
        tau = jobs[op[3]][0][op[2]]
        begin = max(time, free.get((z, step), 0.0))
        free[z, step] = begin + tau
        if z + step == to:
            inbox[to].append((begin + tau + lat, op))
        else:
            transit.append((begin + 0.7, z + step, to, op))

    def spread(time, z, op):
        if jobs[op[3]][4]:
            transit.extend((time, z, to, op) for to in range(T) if to != z)
            return
        if z >= op[1] and z < T - 1:
            post(time, z, 1, op)
        if z <= op[1] and z > 0:
            post(time, z, -1, op)

    def passive(z, op):
        kind, i, u, name = op
        if kind in (ID.R, ID.L):
            return i == z
        return jobs[name][4] or (z in (0, T - 1) and jobs[name][2])

    def start_of(z, item):
        if item[0] == ID.op:
            time, op = item[1]
            if op[0] in (ID.R, ID.L):
                own = parts[z].get((op[3], op[2]))
                if own is None:
                    return None
                time = max(time, own)
            return max(time, now[z])
        step = marks[item[1]]
        time = max(now[z], step.get(ID.time, 0.0))
        for name, delay in step.get(ID.after, ()):
            if name not in steps[z]:
                return None
            time = max(time, steps[z][name] + delay)
        for event in step.get(ID.needs, ()):
            event = tuple(z if e == ID.z else e for e in event)
            if event[0] in (ID.R, ID.L) and event[1] == (0 if event[0] == ID.R else T - 1):
                continue
            if event[0] == ID.A and event[1] == z:
                continue
            if event not in seen[z]:
                return None
            time = max(time, seen[z][event])
        return time

    while True:
        best = None
        for entry in transit:
            key = (entry[0], -1, entry[1], entry[2])
            if best is None or key < best[0]:
                best = (key, entry[1], (ID.cross, entry))
        for z in range(T):
            for entry in list(inbox[z]):
                if passive(z, entry[1]):
                    seen[z][entry[1]] = entry[0]
                    inbox[z].remove(entry)
            for entry in inbox[z]:
                time = start_of(z, (ID.op, entry))
                if time is not None:
                    key = (time, 0 if jobs[entry[1][3]][3] == 0 else 1, entry[0], z)
                    if best is None or key < best[0]:
                        best = (key, z, (ID.op, entry))
            choices = left[z][:1] if order is not None else left[z]
            for k, name in enumerate(choices):
                time = start_of(z, (ID.mark, name))
                if time is not None:
                    key = (time + 0.01, 2 + marks[name].get(ID.low, 0), k, z)
                    if best is None or key < best[0]:
                        best = (key, z, (ID.mark, name))
        if best is None:
            break
        key, z, item = best
        if item[0] == ID.cross:
            transit.remove(item[1])
            cross(item[1])
            continue
        begin = start_of(z, item)
        if item[0] == ID.op:
            _, op = item[1]
            inbox[z].remove(item[1])
            out[z].append((begin, item[1][1]))
            now[z] = begin + OP
            if op[0] == ID.A:
                seen[z][op] = begin
                spread(now[z], z, op)
            else:
                post(now[z], z, 1 if op[0] == ID.R else -1, op)
        else:
            name = item[1]
            step = marks[name]
            left[z].remove(name)
            out[z].append((begin, (ID.M, name)))
            now[z] = begin + step[ID.dur]
            steps[z][name] = now[z]
            for job, u, kind in step.get(ID.posts, ()):
                if kind == ID.gather:
                    spread(now[z], z, (ID.A, z, u, job))
                else:
                    parts[z].setdefault((job, u), now[z])
                    for d in kind:
                        if z == 0:
                            post(now[z], z, 1, (ID.R, d, u, job))
                        if z == T - 1:
                            post(now[z], z, -1, (ID.L, T - 1 - d, u, job))
    if order is None:
        spots = {name: sum(t for z in range(T) for t, op in out[z] if op == (ID.M, name)) for name in marks}
        assert all(len(l) == 0 for l in left), left
        return simulate(T, jobs, marks, lat, sorted(marks, key=lambda n: spots[n]))
    assert all(len(l) == 0 for l in left) and all(len(i) == 0 for i in inbox + [transit]), (left, inbox)
    return out, max(now)

def emit(T, z, timeline, jobs, marks, actors, steps, flush):
    names = [op[1] for _, op in timeline[0] if op[0] == ID.M]
    todo = [[op for _, op in timeline[zz]] for zz in range(T)]
    waited = [set() for _ in range(T)]
    for name in names:
        for zz in range(T):
            now = []
            while todo[zz][0] != (ID.M, name):
                now.append(todo[zz].pop(0))
            todo[zz].pop(0)
            for event in marks[name].get(ID.needs, ()):
                job = jobs.get(event[3])
                if event[0] == ID.A and event[1] != zz and (job[4] or (zz in (0, T - 1) and job[2])):
                    if event not in waited[zz]:
                        waited[zz].add(event)
                        now.append(event)
            if now:
                @pl.when(z == zz)
                def _(now=now, zz=zz):
                    for op in now:
                        actors[op[3]].one(op, zz)
        if name in steps:
            steps[name]()
        if name in TIDY:
            flush()


def timetable(U, T):
    S = U // 2
    tau = 4.18 / U + 0.1
    hi, lo = range(S), range(S, U)
    norm = 0.15 + 0.8 / U
    jobs = {
        ID.wo: ([1.65] * 2, False, True, 0, False), ID.ab: ([1.5] * 2, False, True, 0, False),
        ID.ac: ([0.8] * 2, False, True, 0, False), ID.ga2: ([tau] * U, True, True, 0, False),
        ID.out: ([tau] * U, True, False, 1, False), ID.ga1: ([tau] * U, True, False, 0, False),
        ID.small: ([0.5], False, False, 1, True),
    }
    m = {}

    def step(name, dur, after=(), needs=(), posts=(), low=0, time=0.0):
        m[name] = dict(dur=dur, after=list(after), needs=list(needs), posts=list(posts), low=low, time=time)

    def every(job, pieces):
        return [(ID.A, i, u, job) for i in range(T) for u in pieces]

    step(ID.wo, 0.0, posts=[(ID.wo, 0, ID.gather), (ID.wo, 1, ID.gather)])
    step(ID.go, 0.3, [(ID.wo, 2.2)])
    step(ID.own, 2.4, [(ID.go, 0)])
    step(ID.relay0, 0.1, [(ID.go, 3.3)])
    step(ID.near0, 1.1, [(ID.go, 4.6), (ID.relay0, 0), (ID.own, 0)])
    step(ID.relay1, 0.1, [(ID.go, 6.0), (ID.relay0, 0)])
    step(ID.far0, 1.1, [(ID.relay0, 4.2), (ID.near0, 0)], posts=[(ID.ab, 0, ID.gather)])
    step(ID.near1, 1.1, [(ID.relay1, 2.0), (ID.far0, 0)])
    step(ID.relay2, 0.1, [(ID.relay1, 4.6)])
    step(ID.far1, 1.1, [(ID.relay1, 4.4), (ID.near1, 0)], posts=[(ID.ab, 1, ID.gather)])
    step(ID.upstream, 0.8, [(ID.far1, 0)])
    step(ID.near2, 1.1, [(ID.relay2, 2.0), (ID.upstream, 0)])
    step(ID.far2, 1.2, [(ID.relay2, 4.0), (ID.near2, 0)], posts=[(ID.ac, 0, ID.gather), (ID.ac, 1, ID.gather)])
    step(ID.pads, 0.4, [(ID.far2, 0)], every(ID.wo, [0, 1]))
    step(ID.mix, 1.0, [(ID.pads, 0)], every(ID.ab, [0, 1]))
    step(ID.feed1, 3.1, [(ID.mix, 0)], every(ID.ac, [0]), [(ID.ga2, u, DS) for u in hi])
    step(ID.feed0, 3.1, [(ID.feed1, 0)], every(ID.ac, [1]), [(ID.ga2, u, DS) for u in lo])
    step(ID.weights_a, 0.8, [(ID.feed0, 2.0)], low=1)
    step(ID.weights_a2, 0.8, [(ID.weights_a, 0)], low=1)
    step(ID.out_partial, 0.8, [(ID.weights_a2, 2.0)], low=1)
    step(ID.weights_b, 0.4, [(ID.weights_a2, 4.5)], low=1)
    step(ID.near_w1, 0.3, [(ID.weights_b, 5.0)], low=1)
    for u in range(U):
        sums = lambda job: [(ID.R, ID.z, u, job), (ID.L, ID.z, u, job)]
        step((ID.n2_, u), norm, needs=sums(ID.ga2), posts=[(ID.ga2, u, ID.gather)])
        for d in DS:
            step((ID.begin_out, u, d), 0.0, [(ID.out_partial, 0), (ID.feed0, OUT_FROM + OUT_GAP * (3 * u + 3 - d))],
                 posts=[(ID.out, u, (d,))], low=1)
        step((ID.out_, u), 0.2, needs=sums(ID.out), posts=[(ID.out, u, ID.gather)], low=1)
        step((ID.n1_, u), norm, needs=sums(ID.ga1), posts=[(ID.ga1, u, ID.gather)])
    step(ID.norm_sums, 1.8, [(ID.weights_c, 0)], posts=[(ID.small, 0, ID.gather)], low=1)
    step(ID.high, 1.4, needs=every(ID.ga2, hi))
    step(ID.high2, 0.9, [(ID.high, 0)])
    step(ID.near_k1a, 0.15, [(ID.high, 3.4), (ID.high2, 0)])
    step(ID.high3, 0.9, [(ID.high2, 0)])
    step(ID.near_k1b, 0.15, [(ID.near_k1a, 0), (ID.high3, 0)])
    step(ID.mid3, 0.9, [(ID.high3, 0)])
    step(ID.low, 1.4, [(ID.mid3, 0), (ID.near_k1b, 0)], every(ID.ga2, lo))
    step(ID.low2, 1.7, [(ID.low, 0)])
    step(ID.near_k0a, 0.15, [(ID.low, 3.4), (ID.low2, 0)])
    step(ID.low3, 1.7, [(ID.low2, 0)])
    step(ID.near_k0b, 0.15, [(ID.near_k0a, 0), (ID.low3, 0)])
    step(ID.own_hi, 1.7, [(ID.low3, 0)])
    step(ID.collect1, 0.9, [(ID.own_hi, 0), (ID.near_k1b, 7.0)], posts=[(ID.ga1, u, DS) for u in hi])
    step(ID.own_lo, 0.9, [(ID.collect1, 0)])
    step(ID.finish_w1, 0.3, [(ID.near_w1, 8.0), (ID.near_k0b, 0)], low=1)
    step(ID.aw, 0.6, [(ID.own_lo, 0)], low=1)
    step(ID.collect0, 0.9, [(ID.own_lo, 0), (ID.near_k0b, 7.0)], posts=[(ID.ga1, u, DS) for u in lo])
    step(ID.weights_c, 0.7, [(ID.collect0, 0), (ID.aw, 0)], low=1)
    step(ID.weights_d, 0.3, [(ID.weights_c, 3.0)], low=1)
    step(ID.near_w2, 0.2, [(ID.weights_d, 3.5)], low=1)
    step(ID.relay_w1, 0.05, [(ID.finish_w1, 6.5)], low=1)
    step(ID.finish_w2, 0.2, [(ID.near_w2, 5.0)], low=1)
    step(ID.relay_w2, 0.05, [(ID.finish_w2, 4.0)], low=1)
    step(ID.pair_w1, 0.05, [(ID.relay_w1, 5.0)], low=1)
    step(ID.give_w1, 0.05, [(ID.pair_w1, 4.5)], low=1)
    step(ID.give_o, 0.1, [((ID.out_, U - 1), 2.0)], every(ID.out, range(U)), low=1)
    step(ID.sums, 0.2, needs=every(ID.small, [0]), low=1)
    step(ID.pair_w2, 0.05, [(ID.relay_w2, 3.5)], low=1)
    step(ID.give_v, 0.1, [(ID.sums, 3.0)], low=1)
    step(ID.give_w2, 0.05, [(ID.pair_w2, 3.0)], low=1)
    step(ID.give_hi, 0.1, [(ID.give_o, 0)], every(ID.ga1, hi), low=1)
    step(ID.end, 0.0, [(ID.give_v, 0), (ID.give_hi, 0), (ID.give_w1, 0), (ID.give_w2, 0)], every(ID.ga1, range(U)))
    return jobs, m


def scratch_list(R, T, D, F, nh):
    NG = R // 2
    N = 4 * BLK
    v = pltpu.VMEM
    rows = v((8, 64, D), BF)
    return dict(
        tok_raw=(rows),
        cot_raw=(rows),
        stage=(v((2, 2, 2, 64, D), BF)),
        x=(rows),
        cot=(rows),
        wqt=(v((640, D), BF)),
        wo=(v((T, 2, nh * HEAD // 2, D), BF)),
        wolo=(v((nh, T, BLK, D), BF)),
        wohi=(v((nh, T, BLK, D), BF)),
        wopad=(v((nh * BLK, D), BF)),
        fc=(v((D, F), BF)),
        pw=(v((F, D), BF)),
        brow=(v((1, 640), F32)),
        act1=(rows),
        q=(v((nh, N, 128), BF)),
        kv=(v((NG, nh, N, 128), BF)),
        pre=(v((N, D), F32)),
        ga=(v((N, F), F32)),
        hid=(v((8, 64, D), F32)),
        act2=(v((N, D), BF)),
        actd=(v((N, F), BF)),
        gpre=(v((N, F), BF)),
        mlo=(v((4 if NG == 4 else 1, 256, 256), F32)),
        mhi=(v((4 if NG == 4 else 1, 256, 256), F32)),
        m=(v((2 * nh, 1, 256), F32)),
        l=(v((2 * nh, 1, 256), F32)),
        delta=(v((2 * nh, 1, 256), F32)),
        acc=(v((2 * nh, 128, 256), F32)),
        attp=(v((nh, N, 128), BF)),
        attn=(v((N, 256), BF)),
        ab=(v((T, nh, 256, 128), BF)),
        p1=(rows), r1=(rows), l1=(rows),
        r2=(rows), l2=(rows),
        r3=(rows), l3=(rows),
        gh=(v((2, 64, D), F32)),
        h=(rows),
        do=(v((nh, N, 128), BF)),
        dkf=(v((4 if NG == 4 else 1, nh, 256, 128), F32)),
        dk=(v((NG, nh, N, 128), BF)),
        dkr=(v((NG, nh, N, 128), BF)),
        dka=(v((2, 2, nh, 128, 128), BF)),
        gn=(v((N, 640), BF)),
        w1=(v((2, NG, D // NG, D), BF)),
        w1r=(v((NG, D // NG, D), BF)),
        w1s=(v((NG, D // NG, D), BF)),
        w1a=(v((2, D // NG // 2, D), BF)),
        w1f=(v((2, NG, D // NG, D), BF)),
        w2=(v((2, NG, D // 2 // NG, D), BF)),
        w2r=(v((NG, D // 2 // NG, D), BF)),
        w2s=(v((NG, D // 2 // NG, D), BF)),
        w2a=(v((2, D // 2 // NG // 2, D), BF)),
        w2f=(v((2, NG, D // 2 // NG, D), BF)),
        yo=(rows),
        yg=(rows),
        mo=(v((2, 2, 64, D), BF)),
        mg=(v((2, 2, 64, D), BF)),
        vsum=(v((16, D), F32)),
        vz=(v((T, 16, D), BF)),
        vc=(v((R, 16, D), BF)),
        ss=(pltpu.SemaphoreType.DMA((SENDS if NG == 4 else 200,))),
        rs=(pltpu.SemaphoreType.DMA((ARRIVALS if NG == 4 else 400,))),
        ls=(pltpu.SemaphoreType.DMA((24,))),
    )


def layer_kernel(R, T, D, F, nh, names, *refs):
    (pos_ref, seq_ref, tok_hbm, cot_hbm, g1_ref, b1_ref, wqt_hbm, qvb_ref, wo_hbm, ob_ref, g2_ref,
     b2_ref, fc_hbm, fcb_ref, pw_hbm, pb_ref, w1_out, w2_out, fo_out, fg_out, v_out) = refs[:21]
    s = SimpleNamespace(**dict(zip(names, refs[21:])))
    s.p2, s.p3 = s.tok_raw, s.cot_raw
    NG = R // 2
    N = 4 * BLK
    Q1 = D // NG
    Q2 = D // 2 // NG
    SUB = U // 2
    RU = 64 // SUB
    r = lax.axis_index("ctx")
    z = lax.axis_index("tp")
    c = lax.rem(r, 2)
    o = 1 - c
    g = lax.div(r, 2)
    mate = 2 * g + o
    zp, zm = z + 1, z - 1
    not_core = [c != 0, c != 1]
    if NG == 4:
        ga_ = g + 1 - 2 * lax.rem(g, 2)
        gb_ = g + 2 - 4 * lax.div(g, 2)
        gc_ = ga_ + 2 - 4 * lax.div(ga_, 2)
        peers = [g, ga_, gb_, gc_]
        sources = peers
    else:
        peers = [lax.rem(g + t, NG) for t in range(NG)]
        sources = [lax.rem(g + NG - t, NG) for t in range(NG)]

    most = {ID.common: 0, ID.line: 0}
    spare = {ID.common: [], 0: [], 1: [], 2: [], 3: []}
    started = [[], []]
    ids = [0]
    SPLIT = SPLIT_AT if NG == 4 else 100

    def take(pool):
        if spare[pool]:
            return spare[pool].pop(0)
        kind = ID.common if pool == ID.common else pool
        most[kind] = most.get(kind, 0) + 1
        return most[kind] - 1 + (0 if pool == ID.common else SPLIT)

    def flush(last=False):
        for batch in ([started[0]] if not last else started):
            for pool in (ID.common, 0, 1, 2, 3):
                mine = [e for e in batch if e[0] == pool]
                if pool == ID.common:
                    for _, _, done in mine:
                        done()
                elif mine:
                    @pl.when(z == pool)
                    def _(mine=mine):
                        for _, _, done in mine:
                            done()
                spare[pool].extend(e[1] for e in mine)
        started[0] = started[1]
        started[1] = []

    def new(count=1):
        first = ids[0]
        ids[0] += count
        return first

    def remote(src, dst, mine, slot, dev):
        src = src() if callable(src) else src
        dst = dst() if callable(dst) else dst
        return pltpu.make_async_remote_copy(
            src_ref=src, dst_ref=dst, send_sem=s.ss.at[mine], recv_sem=s.rs.at[slot],
            device_id=dev, device_id_type=MESH)

    def send(src, dst, slot, dev, cond=None, at=None):
        pool = ID.common if at is None else at
        mine = take(pool)

        def go():
            remote(src, dst, mine, slot, dev).start()

        def done():
            remote(src, dst, mine, slot, dev).wait_send()

        if cond is None:
            go()
            started[1].append((pool, mine, done))
        else:
            pl.when(cond)(go)
            started[1].append((pool, mine, lambda: pl.when(cond)(done)))

    def arrived(dst, slot, cond=None):
        def go():
            remote(dst, dst, 0, slot, (r, z)).wait_recv()

        if cond is None:
            go()
        else:
            pl.when(cond)(go)

    loads = {}

    def load(name, src, dst, k):
        loads[name] = pltpu.make_async_copy(src, dst, s.ls.at[k])
        loads[name].start()

    load(ID.tok, tok_hbm, s.tok_raw, 0)
    load(ID.wqt, wqt_hbm, s.wqt.at[pl.ds(0, 3 * nh * HEAD)], 1)
    load(ID.wo, wo_hbm, s.wo.at[z], 3)
    load(ID.cot, cot_hbm, s.cot_raw, 2)
    load(ID.pw, pw_hbm, s.pw, 4)
    load(ID.fc, fc_hbm, s.fc, 5)

    barrier = pltpu.get_barrier_semaphore()
    for t in range(1, R):
        pl.semaphore_signal(barrier, inc=1, device_id=(lax.rem(r + t, R), z), device_id_type=MESH)

    for t in range(1, T):
        pl.semaphore_signal(barrier, inc=1, device_id=(r, lax.rem(z + t, T)), device_id_type=MESH)
    pl.semaphore_wait(barrier, R + T - 2)

    def find(seq):
        low = jnp.int32(0)
        high = jnp.int32(0)
        for b in range(4):
            same = seq_ref[4 * r + b] == seq
            first = pos_ref[4 * r + b] < R
            low = jnp.where(same & first, b, low)
            high = jnp.where(same & jnp.logical_not(first), b, high)
        return low, high

    def low_pos(rank):
        total = jnp.int32(0)
        for b in range(4):
            here = (seq_ref[4 * rank + b] == c) & (pos_ref[4 * rank + b] < R)
            total = total + jnp.where(here, pos_ref[4 * rank + b], 0)
        return total

    other = find(o)
    own = find(c)
    q_low = (low_pos(2 * g), low_pos(2 * g + 1))

    def swap(raw, k_stage, dst, base):
        for k in range(2):
            s.stage[k_stage, k] = raw[pl.ds(2 * other[k], 2)]
            send(s.stage.at[k_stage, k], dst.at[pl.ds(4 * k + 2 * c, 2)], base + k, (mate, z))
        for k in range(2):
            dst[pl.ds(4 * k + 2 * c, 2)] = raw[pl.ds(2 * own[k], 2)]

    def swapped(dst, base):
        for k in range(2):
            arrived(dst.at[pl.ds(4 * k + 2 * o, 2)], base + k)

    sx = new(4)
    loads[ID.tok].wait()
    swap(s.tok_raw, 0, s.x, sx)

    class Gather:
        def __init__(self, at, pieces, pass_on=None):
            self.at, self.hand = at, pass_on
            self.base = [new(T) for _ in range(pieces)]

        def start(self, u):
            for zz in range(T):
                @pl.when(z == zz)
                def _(zz=zz):
                    a = lambda: self.at(zz, u)
                    if zz < T - 1:
                        send(a, a, self.base[u] + zz, (r, zp), at=zz)
                    if zz > 0:
                        send(a, a, self.base[u] + zz, (r, zm), at=zz)

        def one(self, op, at):
            _, i, u, _ = op
            slot = self.base[u] + i
            a = lambda: self.at(i, u)
            arrived(a, slot)
            if at > i and at < T - 1:
                send(a, a, slot, (r, zp), at=at)
            if at < i and at > 0:
                send(a, a, slot, (r, zm), at=at)
            if self.hand is not None:
                self.hand(i, u, at)

    class Direct:
        def __init__(self, at, pieces):
            self.at = at
            self.base = [new(T) for _ in range(pieces)]

        def start(self, u):
            a = self.at(z, u)
            for t in range(1, T):
                send(a, a, self.base[u] + t, (r, lax.rem(z + t, T)))

        def one(self, op, at):
            _, i, u, _ = op
            arrived(lambda: self.at(i, u), self.base[u] + (at - i) % T)

    def piece(buf, i, u):
        half = 1 if u < SUB else 0
        if SUB == 1:
            return buf.at[4 * half + i]
        return buf.at[4 * half + i, pl.ds(RU * (u % SUB), RU)]

    class Sum:
        def __init__(self, part, from_left, from_right, whole, landing=None):
            self.part, self.fl, self.fr = part, from_left, from_right
            self.whole, self.landing = whole, landing
            self.rl = [new(T + 1) for _ in range(U)]
            self.ag = self.rl
            self.hand = [new(2) for _ in range(U)] if landing is not None else None

            @pl.when(z == 0)
            def _():
                from_left[0] = jnp.zeros((64, D), BF)
                from_left[4] = jnp.zeros((64, D), BF)

            @pl.when(z == T - 1)
            def _():
                from_right[T - 1] = jnp.zeros((64, D), BF)
                from_right[4 + T - 1] = jnp.zeros((64, D), BF)

        def begin(self, u, ds=(3, 2, 1)):
            @pl.when(z == 0)
            def _():
                for d in ds:
                    send(self.see(self.part, d, u), self.see(self.fl, d, u), self.rl[u] + d, (r, zp), at=0)

            @pl.when(z == T - 1)
            def _():
                for d in ds:
                    e = T - 1 - d
                    send(self.see(self.part, e, u), self.see(self.fr, e, u), self.slot(u, e, T - 2), (r, zm), at=T - 1)

        def slot(self, u, d, to):
            return self.rl[u] + (T if d == to else d)

        def see(self, buf, i, u):
            return lambda: piece(buf, i, u)

        def one(self, op, at):
            kind, i, u, _ = op
            if kind == ID.A:
                slot = self.ag[u] + i
                a = self.see(self.whole, i, u)
                arrived(a, slot)
                if at > i and at < T - 1:
                    send(a, a, slot, (r, zp), at=at)
                if at < i and at > 0:
                    send(a, a, slot, (r, zm), at=at)
                self.pass_on(i, u, at)
                return
            right = kind == ID.R
            buf = self.fl if right else self.fr
            arrived(self.see(buf, i, u), self.rl[u] + i)
            slot = self.rl[u] + i if right else self.slot(u, i, at - 1)
            a = piece(self.part, i, u)
            a[...] = (a[...].astype(F32) + piece(buf, i, u)[...].astype(F32)).astype(BF)
            send(self.see(self.part, i, u), self.see(buf, i, u), slot, (r, zp if right else zm), at=at)

        def spot(self, i, u):
            half = 1 if u < SUB else 0
            if SUB == 1:
                return self.landing.at[half, i % 2]
            return self.landing.at[half, i % 2, pl.ds(RU * (u % SUB), RU)]

        def pass_on(self, i, u, at):
            if self.landing is None:
                return
            send(self.see(self.whole, i, u), lambda: self.spot(i, u), self.hand[u] + i % 2, (mate, z),
                 not_core[i // 2], at=at)

        def last(self, u):
            for at in range(T):
                @pl.when(z == at)
                def _(at=at):
                    if at > 0:
                        arrived(self.see(self.fl, at, u), self.rl[u] + at)
                    if at < T - 1:
                        arrived(self.see(self.fr, at, u), self.rl[u] + T)

        def total(self, index, rows):
            return (self.part[index, rows, :].astype(F32) + self.fl[index, rows, :].astype(F32)
                    + self.fr[index, rows, :].astype(F32))

        def gather(self, u):
            for at in range(T):
                @pl.when(z == at)
                def _(at=at):
                    a = self.see(self.whole, at, u)
                    if at < T - 1:
                        send(a, a, self.ag[u] + at, (r, zp), at=at)
                    if at > 0:
                        send(a, a, self.ag[u] + at, (r, zm), at=at)
                    self.pass_on(at, u, at)

        def handed(self, pieces):
            for u in pieces:
                for k in range(2):
                    arrived(self.spot(k, u), self.hand[u] + k)

    class PlaneSum:
        def __init__(self, part, cut, far, near):
            self.part, self.cut, self.fl, self.near_buf = part, cut, far, near
            self.base = new(max(4, NG))

        def far(self):
            if NG == 4:
                for k in range(2):
                    send(self.part(peers[3], k), self.fl(k), self.base + k, (2 * peers[1 + k] + c, z))

        def near(self, ks=(0, 1)):
            if NG == 4:
                for k in ks:
                    to = peers[2 - k]
                    arrived(self.fl(k), self.base + k)
                    self.cut(to, k)
                    send(self.part(to, None), self.near_buf(2 - k), self.base + 2 + k, (2 * to + c, z))
            else:
                for t in range(1, NG):
                    send(self.part(peers[t], None), self.near_buf(t), self.base + t, (2 * peers[t] + c, z))

        def arrived(self):
            if NG == 4:
                for k in range(2):
                    arrived(self.near_buf(2 - k), self.base + 2 + k)
            else:
                for t in range(1, NG):
                    arrived(self.near_buf(t), self.base + t)

    class PlaneGather:
        def __init__(self, at):
            self.at = at
            self.base = new(max(6, NG))

        def start(self):
            if NG == 4:
                for t, first in ((1, 0), (2, 1)):
                    for leg, half in ((0, first), (1, 1 - first)):
                        a = self.at(g, half)
                        send(a, a, self.base + 2 * (t - 1) + leg, (2 * peers[t] + c, z))
            else:
                for t in range(1, NG):
                    send(self.at(g, None), self.at(g, None), self.base + t, (2 * peers[t] + c, z))

        def relay(self):
            if NG == 4:
                for t, half in ((1, 0), (2, 1)):
                    a = self.at(peers[t], half)
                    arrived(a, self.base + 2 * (t - 1))
                    send(a, a, self.base + 3 + t, (2 * peers[3 - t] + c, z))

        def arrived(self):
            if NG == 4:
                for t, half in ((1, 1), (2, 0)):
                    arrived(self.at(peers[t], half), self.base + 2 * (t - 1) + 1)
                for t, half in ((1, 0), (2, 1)):
                    arrived(self.at(peers[3], half), self.base + 3 + t)
            else:
                for t in range(1, NG):
                    arrived(self.at(sources[t], None), self.base + t)

    WP = nh * HEAD // 4
    swo = new(2 * T)

    def wo_at(i, u, core=None):
        return s.wo.at[i, c if core is None else core, pl.ds(WP * u, WP)]

    def hand_wo(i, u, at):
        send(lambda: wo_at(i, u), lambda: wo_at(i, u), swo + T * u + i, (mate, z), at=at)

    wo_line = Gather(wo_at, 2, hand_wo)
    loads[ID.wo].wait()
    wo_line.start(0)
    wo_line.start(1)
    s.wqt[pl.ds(3 * nh * HEAD, 640 - 3 * nh * HEAD), :] = jnp.zeros((640 - 3 * nh * HEAD, D), BF)
    s.brow[...] = jnp.zeros((1, 640), F32)
    s.brow[:, 0:192] = qvb_ref[0:1, :]
    s.brow[:, 384:576] = qvb_ref[1:2, :]
    g1 = g1_ref[...].reshape(1, -1)
    b1 = b1_ref[...].reshape(1, -1)
    lo_a, hi_a = pl.ds(0, 256), pl.ds(256, 256)

    def project(first):
        for k in range(2):
            for i in range(2):
                j = 4 * k + 2 * first + i
                n, _inv = normed(s.x[j].astype(F32))
                s.act1[j] = (n * g1 + b1).astype(BF)
        a = jnp.concatenate([s.act1[pl.ds(4 * k + 2 * first, 2)].reshape(BLK, D) for k in range(2)], axis=0)
        s.pre[0:256, 0:640] = dg(a, s.wqt[...], 1, 1)
        low = lax.broadcasted_iota(jnp.int32, (BLK, 128), 1) < HEAD
        zero = jnp.zeros((BLK, 128), F32)
        for k in range(2):
            t = [s.pre[BLK * k:BLK * k + BLK, 128 * i:128 * i + 128] + s.brow[:, 128 * i:128 * i + 128]
                 for i in range(5)]
            rows = pl.ds(pl.multiple_of((2 * k + first) * BLK, BLK), BLK)
            s.kv[g, 0, rows, :] = jnp.where(low, roll64(t[1]), roll64(t[3])).astype(BF)
            s.kv[g, 1, rows, :] = jnp.where(low, t[2], t[3]).astype(BF)
            s.kv[g, 2, rows, :] = jnp.where(low, roll64(t[2]), roll64(t[4])).astype(BF)
            s.q[0, rows, :] = (jnp.where(low, t[0], zero) * 0.125).astype(BF)
            s.q[1, rows, :] = (jnp.where(low, roll64(t[0]), zero) * 0.125).astype(BF)
            s.q[2, rows, :] = (jnp.where(low, t[1], zero) * 0.125).astype(BF)

    loads[ID.wqt].wait()
    project(c)
    swapped(s.x, sx)
    project(o)

    skv = new(max(6 * nh, NG))

    def kv_go(h, leg):
        for t, halves in ((1, (lo_a, hi_a)), (2, (hi_a, lo_a))):
            a = s.kv.at[g, h, halves[leg]]
            send(a, a, skv + 6 * h + 2 * (t - 1) + leg, (2 * peers[t] + c, z))

    def kv_relay(h):
        for t, to, half in ((1, 2, lo_a), (2, 1, hi_a)):
            a = s.kv.at[peers[t], h, half]
            arrived(a, skv + 6 * h + 2 * (t - 1))
            send(a, a, skv + 6 * h + 3 + t, (2 * peers[to] + c, z))

    def kv_rest(h):
        for t, half in ((1, hi_a), (2, lo_a)):
            arrived(s.kv.at[peers[t], h, half], skv + 6 * h + 2 * (t - 1) + 1)

    def kv_far(h):
        for t, half in ((1, lo_a), (2, hi_a)):
            arrived(s.kv.at[peers[3], h, half], skv + 6 * h + 3 + t)

    def masks(src):
        k_low = (low_pos(2 * src), low_pos(2 * src + 1))
        i0 = lax.broadcasted_iota(jnp.int32, (256, 256), 0)
        i1 = lax.broadcasted_iota(jnp.int32, (256, 256), 1)

        def token(i, a, b):
            return i + jnp.where(i < BLK, a * BLK, b * BLK - BLK)

        last = 2 * R - 1
        low_mask = jnp.where(token(i0, *k_low) <= token(i1, *q_low), 0.0, NEG)
        high_mask = jnp.where(
            token(i0, last - k_low[0], last - k_low[1])
            <= token(i1, last - q_low[0], last - q_low[1]), 0.0, NEG)
        return low_mask, high_mask

    def all_masks():
        for t in range(4):
            s.mlo[t], s.mhi[t] = masks(peers[t])

    def keys_of(src, h):
        return s.kv[src, h, 0:256, :], s.kv[src, h, 256:512, :]

    def attend(groups, h, fresh=False):
        for half in range(2):
            at = 2 * h + half
            qs = s.q[h, 256 * half:256 * half + 256, :]
            tiles = []
            for src, mlo, mhi in groups:
                klo, khi = keys_of(src, h)
                if half == 0:
                    tiles.append((klo, dg(klo, qs, 1, 1) + mlo[...]))
                else:
                    tiles.append((klo, dg(klo, qs, 1, 1)))
                    tiles.append((khi, dg(khi, qs, 1, 1) + mhi[...]))
            now = None if fresh else s.m[at]
            old = now
            for _, sc in tiles:
                top = jnp.max(sc, axis=0, keepdims=True)
                now = top if now is None else jnp.maximum(now, top)
            total = value = None
            for k, sc in tiles:
                e = jnp.exp(sc - now)
                part = jnp.sum(e, axis=0, keepdims=True)
                total = part if total is None else total + part
                part = dg(k, e.astype(BF), 0, 0)
                value = part if value is None else value + part
            if fresh:
                s.l[at] = total
                s.acc[at] = value
            else:
                f = jnp.exp(old - now)
                s.l[at] = s.l[at] * f + total
                s.acc[at] = s.acc[at] * f + value
            s.m[at] = now

    low = lax.broadcasted_iota(jnp.int32, (256, 128), 1) < HEAD
    low_s = lax.broadcasted_iota(jnp.int32, (BLK, 128), 1) < HEAD

    def settle(h):
        outs = []
        for half in range(2):
            rows = pl.ds(256 * half, 256)
            outs.append(jnp.transpose(s.acc[2 * h + half] / s.l[2 * h + half]))
            s.attp[h, rows, :] = outs[half].astype(BF)
            s.m[2 * h + half] = s.m[2 * h + half] + jnp.log(s.l[2 * h + half])
        if h < nh - 1:
            s.ab[z, h] = jnp.where(low, roll64(outs[0]), outs[1]).astype(BF)
        else:
            for place, half in ((0, 1), (1, 0)):
                v = outs[half]
                s.ab[z, h, BLK * place:BLK * place + BLK, :] = jnp.where(
                    low_s, roll64(v[0:BLK]), v[BLK:256]).astype(BF)

    ab_line = Gather(lambda i, u: s.ab.at[i, u], nh - 1)
    ac_line = Gather(lambda i, u: s.ab.at[i, nh - 1, pl.ds(BLK * u, BLK)], 2)

    sum1 = Sum(s.p1, s.r1, s.l1, s.h)
    sum2 = Sum(s.p2, s.r2, s.l2, s.yo, s.mo)
    sum3 = Sum(s.p3, s.r3, s.l3, s.yg, s.mg)
    s.vsum[...] = jnp.zeros((16, D), F32)

    def upstream():
        swapped(s.cot, sx + 2)
        loads[ID.pw].wait()
        for half in range(2):
            s.ga[256 * half:256 * half + 256, :] = dg(
                s.cot[4 * half:4 * half + 4].reshape(256, D), s.pw[...], 1, 1)

    zeros = jnp.zeros((HEAD, D), BF)

    def pad_own():
        mine = s.wo[z].reshape(nh * HEAD, D)
        for h in range(nh):
            s.wopad[BLK * h:BLK * h + HEAD, :] = zeros
            s.wopad[BLK * h + HEAD:BLK * h + BLK, :] = mine[HEAD * h:HEAD * h + HEAD]

    def pad_all():
        for t in range(1, T):
            for u in range(2):
                arrived(wo_at(lax.rem(z + t, T), u, o), swo + T * u + lax.rem(z + t, T))
        for t in range(T):
            w = s.wo[t].reshape(nh * HEAD, D)
            for h in range(nh):
                part = w[HEAD * h:HEAD * h + HEAD]
                s.wolo[h, t, 0:HEAD, :] = part
                s.wolo[h, t, HEAD:BLK, :] = zeros
                s.wohi[h, t, 0:HEAD, :] = zeros
                s.wohi[h, t, HEAD:BLK, :] = part

    def early_mix():
        for half, w in ((1, s.wohi), (0, s.wolo)):
            total = None
            for h in range(nh - 1):
                a = jnp.concatenate([s.ab[t, h] for t in range(T)], axis=1)
                part = dg(a, w[h].reshape(T * BLK, D), 1, 0)
                total = part if total is None else total + part
            s.pre[256 * half:256 * half + 256, :] = total

    def group(t):
        return peers[t], s.mlo.at[t], s.mhi.at[t]

    def own_keys():
        all_masks()
        for h in range(nh):
            attend([group(0)], h, True)

    def near_keys(h):
        attend([group(1), group(2)], h)

    def far_keys(h):
        kv_far(h)
        attend([group(3)], h)
        settle(h)
        if h < nh - 1:
            ab_line.start(h)
        else:
            ac_line.start(0)
            ac_line.start(1)

    def step_a():
        kv_relay(0)
        kv_go(1, 1)

    def step_b():
        kv_rest(0)
        near_keys(0)

    def step_c():
        kv_relay(1)
        kv_go(2, 0)
        kv_go(2, 1)

    def step_d():
        kv_rest(1)
        near_keys(1)

    def step_e():
        kv_rest(2)
        near_keys(2)

    def whole():
        def one_group(src, fresh):
            s.mlo[0], s.mhi[0] = masks(src)
            for h in range(nh):
                attend([(src, s.mlo.at[0], s.mhi.at[0])], h, fresh)

        one_group(g, True)
        for t in range(1, NG):
            arrived(s.kv.at[sources[t]], skv + t)

        def rest(t, _):
            one_group(lax.rem(g + t, NG), False)
            return 0

        lax.fori_loop(1, NG, rest, 0)
        for h in range(nh):
            settle(h)

    def pads():
        pad_own()
        pad_all()

    g2 = g2_ref[...].reshape(1, -1)
    b2 = b2_ref[...].reshape(1, -1)
    ob = ob_ref[...].reshape(1, -1)
    fcb = fcb_ref[...].reshape(1, -1)
    pb = pb_ref[...].reshape(1, -1)

    def feed(half, total):
        place = 1 - half
        a = jnp.concatenate([s.ab[t, nh - 1, BLK * place:BLK * place + BLK, :] for t in range(T)], axis=1)
        base = 256 * half
        for k, w in ((0, s.wolo), (1, s.wohi)):
            s.pre[base + BLK * k:base + BLK * k + BLK, :] += dg(a, w[nh - 1].reshape(T * BLK, D), 1, 0)

        def norm2(i, _):
            j = 4 * half + i
            rows = pl.ds(pl.multiple_of(base + i * 64, 64), 64)
            x = s.x[j].astype(F32) + s.pre[rows, :] + ob
            s.hid[j] = x
            n, _inv = normed(x)
            s.act2[rows, :] = (n * g2 + b2).astype(BF)
            return 0

        lax.fori_loop(0, 4, norm2, 0)
        part = pl.ds(base, 256)
        s.pre[part, :] = dg(s.act2[part, :], s.fc[...], 1, 0)

        def gelu(i, total):
            rows = pl.ds(pl.multiple_of(base + i * 32, 32), 32)
            v = s.pre[rows, :] + fcb
            square = v * v
            th = jnp.tanh(C0 * (v + C1 * square * v))
            one = 1.0 + th
            s.actd[rows, :] = (0.5 * v * one).astype(BF)
            slope = 0.5 * one + (0.5 * v) * (1.0 - th * th) * (C0 * (1.0 + 3.0 * C1 * square))
            grad = slope * s.ga[rows, :]
            s.gpre[rows, :] = grad.astype(BF)
            return total + fold8(grad)

        total = lax.fori_loop(0, 8, gelu, total)
        s.p1[4 * half:4 * half + 4] = dg(s.gpre[part, :], s.fc[...], 1, 1).astype(BF).reshape(4, 64, D)
        return total

    bias = []

    def feed1():
        loads[ID.fc].wait()
        bias.append(feed(1, jnp.zeros((8, F), F32)))
        for u in range(SUB):
            sum1.begin(u)

    def feed0():
        s.vsum[8:9, :] = jnp.sum(feed(0, bias[0]), axis=0, keepdims=True)
        for u in range(SUB, U):
            sum1.begin(u)

    sw1 = new(2)

    def weight(dst, index, lhs, rhs):
        for i in range(3):
            part = dg(lhs[:, 256 * i:256 * i + 256], rhs, 0, 0).astype(BF)
            lo, hi = 256 * i, 256 * i + 256
            for qd in range(NG):
                a, b = max(lo, qd * Q1), min(hi, qd * Q1 + Q1)
                if a < b:
                    dst[index, qd, a - qd * Q1:b - qd * Q1, :] = part[a - lo:b - lo]

    def add_into(buf, index, extra):
        def body(i, _):
            buf[index, i] = (buf[index, i].astype(F32) + extra[i].astype(F32)).astype(BF)
            return 0

        lax.fori_loop(0, NG, body, 0)

    def weights_a():
        weight(s.w1, 0, s.actd, s.cot[...].reshape(N, D))

    def weights_a2():
        weight(s.w1, 1, s.act2, s.gpre[...])
        send(s.w1.at[o], s.w1r, sw1, (mate, z))

    def plane(part, land, near, whole, size):
        half = size // 2

        def of(buf):
            return lambda i, k: buf.at[c, i] if k is None else buf.at[c, i, pl.ds(half * k, half)]

        def cut(to, k):
            rows = pl.ds(half * k, half)
            part[c, to, rows, :] = (part[c, to, rows, :].astype(F32) + land[k].astype(F32)).astype(BF)

        total = PlaneSum(of(part), cut, lambda k: land.at[k], lambda t: near.at[t])
        share = PlaneGather(of(whole))

        def finish():
            total.arrived()
            step = size // 3

            def body(i, _):
                rows = pl.ds(pl.multiple_of(i * step, step), step)
                v = part[c, g, rows, :].astype(F32)
                for t in got:
                    v = v + near[t, rows, :].astype(F32)
                whole[c, g, rows, :] = v.astype(BF)
                return 0

            lax.fori_loop(0, 3, body, 0)
            share.start()

        return total, share, finish

    got = [1, 2] if NG == 4 else list(range(1, NG))
    total1, share1, finish1 = plane(s.w1, s.w1a, s.w1s, s.w1f, Q1)
    total2, share2, finish2 = plane(s.w2, s.w2a, s.w2s, s.w2f, Q2)

    def weights_b():
        arrived(s.w1r, sw1)
        add_into(s.w1, c, s.w1r)
        total1.far()

    def out_partial():
        for half in range(2):
            base = 256 * half
            s.p2[4 * half:4 * half + 4] = dg(
                s.actd[base:base + 256, :], s.pw[...], 1, 0).astype(BF).reshape(4, 64, D)

    def spans(u):
        half = 1 if u < SUB else 0
        step = min(RU, 32)
        return half, 4 * half + z, [pl.ds(RU * (u % SUB) + step * i, step) for i in range(RU // step)]

    def back2(u):
        sum1.last(u)
        half, index, parts = spans(u)
        sums = [jnp.zeros((8, D), F32)] * 4
        for rows in parts:
            n, inv = normed(s.hid[index, rows, :])
            grad = sum1.total(index, rows)
            up = s.cot[index, rows, :].astype(F32)
            qg = grad * g2
            gh = up + inv * (qg - jnp.mean(qg, axis=-1, keepdims=True)
                             - n * jnp.mean(qg * n, axis=-1, keepdims=True))
            s.gh[half, rows, :] = gh
            s.h[index, rows, :] = gh.astype(BF)
            for k, part in enumerate((grad * n, grad, gh, up)):
                sums[k] = sums[k] + fold8(part)
        sum1.gather(u)
        for k in range(4):
            s.vsum[2 + k:3 + k, :] += jnp.sum(sums[k], axis=0, keepdims=True)

    def slopes(half):
        rows = pl.ds(256 * half, 256)
        grads = dg(s.h[4 * half:4 * half + 4].reshape(256, D), s.wopad[...], 1, 1)
        for h in range(nh):
            d = grads[:, 128 * h:128 * h + 128].astype(BF)
            s.do[h, rows, :] = d
            both = d.astype(F32) * s.attp[h, rows, :].astype(F32)
            s.delta[2 * h + half] = jnp.sum(jnp.transpose(both), axis=0, keepdims=True)

    def tile(k, h, half, mask):
        qs = s.q[h, 256 * half:256 * half + 256, :]
        ds_ = s.do[h, 256 * half:256 * half + 256, :]
        sc = dg(k, qs, 1, 1)
        if mask is not None:
            sc = sc + mask[...]
        p = jnp.exp(sc - s.m[2 * h + half])
        d = p * (dg(k, ds_, 1, 1) - s.delta[2 * h + half])
        p = p.astype(BF)
        d = d.astype(BF)
        return d, dg(d, qs, 1, 0) + dg(p, ds_, 1, 0)

    def back_high(src, mhi, fresh):
        for h in range(nh):
            _, khi = keys_of(src, h)
            d3, k3 = tile(khi, h, 1, mhi)
            s.dk[src, h, 256:512, :] = k3.astype(BF)
            if fresh:
                s.acc[2 * h + 1] = dg(khi, d3, 0, 0)
            else:
                s.acc[2 * h + 1] += dg(khi, d3, 0, 0)

    def back_mid(src, t):
        for h in range(nh):
            klo, _ = keys_of(src, h)
            d2, k2 = tile(klo, h, 1, None)
            s.dkf[t, h] = k2
            s.acc[2 * h + 1] += dg(klo, d2, 0, 0)

    def back_low(src, t, mlo, fresh):
        for h in range(nh):
            klo, _ = keys_of(src, h)
            d1, k1 = tile(klo, h, 0, mlo)
            s.dk[src, h, 0:256, :] = (s.dkf[t, h] + k1).astype(BF)
            if fresh:
                s.acc[2 * h] = dg(klo, d1, 0, 0)
            else:
                s.acc[2 * h] += dg(klo, d1, 0, 0)

    def key_sum(half):
        rows = pl.ds(256 * half, 256)

        def part(i, k):
            return s.dk.at[i, :, rows if k is None else pl.ds(256 * half + BLK * k, BLK)]

        def cut(to, k):
            some = pl.ds(256 * half + BLK * k, BLK)
            for h in range(nh):
                s.dk[to, h, some, :] = (s.dk[to, h, some, :].astype(F32) + s.dka[half, k, h].astype(F32)).astype(BF)

        return PlaneSum(part, cut, lambda k: s.dka.at[half, k], lambda t: s.dkr.at[t, :, rows])

    keys = [key_sum(0), key_sum(1)]

    def finish_output(u):
        sum2.last(u)
        half, index, parts = spans(u)
        for rows in parts:
            s.yo[index, rows, :] = (s.hid[index, rows, :] + sum2.total(index, rows) + pb).astype(BF)
        sum2.gather(u)

    col = [jnp.zeros((1, 128), F32) for _ in range(5)]

    def collect(half):
        keys[half].arrived()
        rows = pl.ds(256 * half, 256)
        dq = [jnp.transpose(s.acc[2 * h + half]) * 0.125 for h in range(nh)]
        dkv = []
        for h in range(nh):
            total = s.dk[g, h, rows, :].astype(F32)
            for t in got:
                total = total + s.dkr[t, h, rows, :].astype(F32)
            dkv.append(total)
        tiles = [
            jnp.where(low, dq[0], roll64(dq[1])),
            jnp.where(low, dq[2], roll64(dkv[0])),
            jnp.where(low, dkv[1], roll64(dkv[2])),
            jnp.where(low, roll64(dkv[0]), dkv[1]),
            jnp.where(low, roll64(dkv[2]), 0.0),
        ]
        for j in range(5):
            col[j] = col[j] + jnp.sum(tiles[j], axis=0, keepdims=True)
            s.gn[rows, 128 * j:128 * j + 128] = tiles[j].astype(BF)
        back = dg(s.gn[rows, :], s.wqt[...], 1, 0)
        s.p3[4 * half:4 * half + 4] = back.astype(BF).reshape(4, 64, D)
        s.ga[rows, 0:D] = back
        for u in range(SUB) if half == 1 else range(SUB, U):
            sum3.begin(u)

    def put2(first, value, rows):
        done = 0
        while done < rows:
            at, off = divmod(first + done, Q2)
            n = min(Q2 - off, rows - done)
            s.w2[at // NG, at % NG, off:off + n, :] = value[done:done + n].astype(BF)
            done += n

    sw2 = new(2)

    def attention_weight():
        for half in range(2):
            rows = pl.ds(256 * half, 256)
            a = [s.attp[h, rows, :].astype(F32) for h in range(nh)]
            s.attn[rows, 0:128] = jnp.where(low, roll64(a[0]), a[1]).astype(BF)
            s.attn[rows, 128:256] = jnp.where(low, roll64(a[2]), 0.0).astype(BF)
        gout = dg(s.attn[...], s.h[...].reshape(N, D), 0, 0)
        put2(3 * nh * HEAD, gout, nh * HEAD)

    def do_high():
        slopes(1)
        back_high(peers[3], s.mhi.at[3], True)
        keys[1].far()

    def do_low():
        slopes(0)
        back_low(peers[3], 3, s.mlo.at[3], True)
        keys[0].far()

    def mid_low(t):
        back_mid(peers[t], t)
        back_low(peers[t], t, s.mlo.at[t], False)

    def own_hi():
        back_high(g, s.mhi.at[0], False)
        back_mid(g, 0)

    def whole_part():
        slopes(0)
        slopes(1)
        for i in range(2 * nh):
            s.acc[i] = jnp.zeros((128, 256), F32)

        def rest_back(t, _):
            src = lax.rem(g + t, NG)
            s.mlo[0], s.mhi[0] = masks(src)
            back_high(src, s.mhi.at[0], False)
            back_mid(src, 0)
            back_low(src, 0, s.mlo.at[0], False)
            return 0

        lax.fori_loop(0, NG, rest_back, 0)
        for half in (1, 0):
            keys[half].near()

    def weights_c():
        for j in range(5):
            s.vsum[9:10, 128 * j:128 * j + 128] = col[j]
        act1 = s.act1[...].reshape(N, D)
        for j in range(5):
            n = min(128, 3 * nh * HEAD - 128 * j)
            put2(128 * j, dg(s.gn[:, 128 * j:128 * j + 128], act1, 0, 0), n)
        send(s.w2.at[o], s.w2r, sw2, (mate, z))

    def weights_d():
        arrived(s.w2r, sw2)
        add_into(s.w2, c, s.w2r)
        total2.far()

    def back1(u):
        sum3.last(u)
        half, index, parts = spans(u)
        for rows in parts:
            n, inv = normed(s.x[index, rows, :].astype(F32))
            qg = sum3.total(index, rows) * g1
            gx = s.gh[half, rows, :] + inv * (qg - jnp.mean(qg, axis=-1, keepdims=True)
                                              - n * jnp.mean(qg * n, axis=-1, keepdims=True))
            s.yg[index, rows, :] = gx.astype(BF)
        sum3.gather(u)

    def norm_sums():
        def body(i, sums):
            n, _inv = normed(s.x[i].astype(F32))
            grad = s.ga[pl.ds(pl.multiple_of(i * 64, 64), 64), 0:D]
            return sums[0] + fold8(grad * n), sums[1] + fold8(grad)

        sums = lax.fori_loop(0, 8, body, (z8, z8))
        for k in range(2):
            s.vsum[k:k + 1, :] = jnp.sum(sums[k], axis=0, keepdims=True)
        s.vz[z] = s.vsum[...].astype(BF)
        v_line.start(0)

    z8 = jnp.zeros((8, D), F32)
    v_line = Direct(lambda i, u: s.vz.at[i], 1)
    svc = new(R)
    copies = []

    def give(src, dst):
        copy = pltpu.make_async_copy(src, dst, s.ls.at[6 + len(copies)])
        copy.start()
        copies.append(copy)

    def give_rows(whole, landing, out, halves=(0, 1)):
        for k in halves:
            give(whole.at[pl.ds(4 * k + 2 * c, 2)], out.at[k, c])
            give(landing.at[k], out.at[k, o])

    def outputs_a():
        share1.arrived()
        send(s.w1f.at[c], s.w1f.at[c], sw1 + 1, (mate, z))

    def outputs_b():
        arrived(s.w1f.at[o], sw1 + 1)
        give(s.w1f, w1_out)

    def outputs_o():
        sum2.handed(range(U))
        give_rows(s.yo, s.mo, fo_out)

    def outputs_c():
        share2.arrived()
        send(s.w2f.at[c], s.w2f.at[c], sw2 + 1, (mate, z))

    def give_v():
        for t in range(1, R):
            arrived(s.vc.at[lax.rem(r + R - t, R)], svc + t)
        total = s.vc[0].astype(F32)
        for t in range(1, R):
            total = total + s.vc[t].astype(F32)
        s.vsum[...] = total
        give(s.vsum, v_out)

    def give_w2():
        arrived(s.w2f.at[o], sw2 + 1)
        give(s.w2f, w2_out)

    def give_hi():
        sum3.handed(range(SUB))
        give_rows(s.yg, s.mg, fg_out, (1,))

    def small_sums():
        upper = s.vz[0, 0:8, :].astype(F32)
        for t in range(1, T):
            upper = upper + s.vz[t, 0:8, :].astype(F32)
        s.vc[r] = jnp.concatenate([upper, s.vsum[8:16, :]], axis=0).astype(BF)
        for t in range(1, R):
            send(s.vc.at[r], s.vc.at[r], svc + t, (lax.rem(r + t, R), z))

    def go():
        if NG == 4:
            kv_go(0, 0)
            kv_go(0, 1)
            kv_go(1, 0)
        else:
            for t in range(1, NG):
                send(s.kv.at[g], s.kv.at[g], skv + t, (2 * peers[t] + c, z))
        loads[ID.cot].wait()
        swap(s.cot_raw, 1, s.cot, sx + 2)

    steps = {
        ID.go: go, ID.pads: pads, ID.mix: early_mix, ID.feed1: feed1, ID.feed0: feed0, ID.weights_a: weights_a,
        ID.weights_a2: weights_a2, ID.out_partial: out_partial, ID.weights_b: weights_b, ID.near_w1: total1.near,
        ID.collect1: functools.partial(collect, 1), ID.collect0: functools.partial(collect, 0), ID.finish_w1: finish1,
        ID.aw: attention_weight, ID.weights_c: weights_c, ID.weights_d: weights_d, ID.near_w2: total2.near,
        ID.relay_w1: share1.relay, ID.finish_w2: finish2, ID.relay_w2: share2.relay, ID.pair_w1: outputs_a,
        ID.give_w1: outputs_b, ID.give_o: outputs_o, ID.sums: small_sums, ID.norm_sums: norm_sums, ID.pair_w2: outputs_c, ID.give_v: give_v, ID.give_w2: give_w2, ID.give_hi: give_hi,
        ID.upstream: upstream,
    }
    for u in range(U):
        steps[ID.n2_, u] = functools.partial(back2, u)
        for d in DS:
            steps[ID.begin_out, u, d] = functools.partial(sum2.begin, u, (d,))
        steps[ID.out_, u] = functools.partial(finish_output, u)
        steps[ID.n1_, u] = functools.partial(back1, u)
    if NG == 4:
        steps.update({
            ID.own: own_keys, ID.relay0: step_a, ID.near0: step_b, ID.relay1: step_c,
            ID.far0: functools.partial(far_keys, 0), ID.near1: step_d, ID.relay2: functools.partial(kv_relay, 2),
            ID.far1: functools.partial(far_keys, 1), ID.near2: step_e, ID.far2: functools.partial(far_keys, 2),
            ID.high: do_high, ID.high2: functools.partial(back_high, peers[2], s.mhi.at[2], False),
            ID.high3: functools.partial(back_high, peers[1], s.mhi.at[1], False),
            ID.near_k1a: functools.partial(keys[1].near, (0,)), ID.near_k1b: functools.partial(keys[1].near, (1,)),
            ID.mid3: functools.partial(back_mid, peers[3], 3), ID.low: do_low,
            ID.low2: functools.partial(mid_low, 2), ID.low3: functools.partial(mid_low, 1),
            ID.near_k0a: functools.partial(keys[0].near, (0,)), ID.near_k0b: functools.partial(keys[0].near, (1,)),
            ID.own_hi: own_hi, ID.own_lo: functools.partial(back_low, g, 0, s.mlo.at[0], False),
        })
    else:
        steps.update({
            ID.own: whole, ID.far0: lambda: ab_line.start(0), ID.far1: lambda: ab_line.start(1),
            ID.far2: lambda: (ac_line.start(0), ac_line.start(1)), ID.low: whole_part,
        })
    jobs, marks = timetable(U, T)
    timeline, _ = simulate(T, jobs, marks, LAT)
    emit(T, z, timeline, jobs, marks,
         {ID.wo: wo_line, ID.ab: ab_line, ID.ac: ac_line, ID.ga2: sum1, ID.out: sum2, ID.ga1: sum3, ID.small: v_line}, steps, flush)

    sum3.handed(range(SUB, U))
    give_rows(s.yg, s.mg, fg_out, (0,))
    flush(True)
    assert max(v for k, v in most.items() if k != ID.common) + SPLIT <= (SENDS if NG == 4 else 200)
    assert most[ID.common] <= SPLIT and ids[0] <= (ARRIVALS if NG == 4 else 400)
    for copy in copies:
        copy.wait()


def finish_kernel(R, pos_ref, seq_ref, rank_ref, w1_hbm, w2_hbm, fo_hbm, fg_hbm, v_hbm, out_hbm, gt_hbm,
                  ln1g_ref, ln1b_ref, gq_hbm, gqv_ref, go_hbm, ob_ref, ln2g_ref, ln2b_ref, gf_hbm, fb_ref,
                  gp_hbm, pb_ref, w1_in, w2_in, fo_in, fg_in, v_in, w1_wide, w2_wide, sems, back):
    parts = 2
    D = w2_in.shape[0]
    step = D // parts
    reads = []

    def read(src, dst):
        copy = pltpu.make_async_copy(src, dst, sems.at[len(reads)])
        copy.start()
        reads.append(copy)

    for k in range(parts):
        rows = pl.ds(step * k, step)
        for i in range(2):
            read(w1_hbm.at[i, rows], w1_in.at[i, rows])
        read(w2_hbm.at[rows], w2_in.at[rows])
    read(v_hbm, v_in)
    read(fo_hbm, fo_in)
    read(fg_hbm, fg_in)
    writes = []

    def write(src, dst):
        copy = pltpu.make_async_copy(src, dst, back.at[len(writes)])
        copy.start()
        writes.append(copy)

    for k in range(parts):
        rows = pl.ds(step * k, step)
        for i, dst in enumerate((gp_hbm, gf_hbm)):
            reads[3 * k + i].wait()
            w1_wide[i, rows] = w1_in[i, rows].astype(F32)
            write(w1_wide.at[i, rows], dst.at[rows])
        reads[3 * k + 2].wait()
        w2_wide[rows] = w2_in[rows].astype(F32)
        low, most = step * k, min(step * k + step, gq_hbm.shape[0])
        write(w2_wide.at[pl.ds(low, most - low)], gq_hbm.at[pl.ds(low, most - low)])
    write(w2_wide.at[pl.ds(most, D - most)], go_hbm)
    for copy in reads[3 * parts:]:
        copy.wait()
    for b in range(4):
        at = 4 * rank_ref[0] + b
        high = jnp.where(pos_ref[at] < R, 0, 1)
        write(fo_in.at[high, seq_ref[at]], out_hbm.at[pl.ds(BLK * b, BLK)])
        write(fg_in.at[high, seq_ref[at]], gt_hbm.at[pl.ds(BLK * b, BLK)])
    for ref, k in ((ln1g_ref, 0), (ln1b_ref, 1), (ln2g_ref, 2), (ln2b_ref, 3), (ob_ref, 4), (pb_ref, 5),
                   (fb_ref, 8)):
        ref[...] = v_in[k:k + 1, :].reshape(-1)
    gqv_ref[0:1, :] = v_in[9:10, 0:192]
    gqv_ref[1:2, :] = v_in[9:10, 384:576]
    for copy in writes:
        copy.wait()


def per_device(R, T, tokens, cotangent, block_pos, block_seq, ln1_gain, ln1_bias, qkv_weight, qv_bias,
               out_weight, out_bias, ln2_gain, ln2_bias, fc_weight, fc_bias, proj_weight, proj_bias):
    D = tokens.shape[1]
    F = fc_weight.shape[1]
    local = qkv_weight.shape[2]
    nh = local // HEAD
    NG = R // 2
    sizes = scratch_list(R, T, D, F, nh)
    names = list(sizes)
    row = lambda v: v
    wqt = jnp.transpose(qkv_weight, (1, 2, 0)).reshape(3 * local, D)
    sm = pl.BlockSpec(memory_space=pltpu.SMEM)
    vm = pl.BlockSpec(memory_space=pltpu.VMEM)
    hb = pl.BlockSpec(memory_space=pl.ANY)
    w1, w2, fo, fg, vs = pl.pallas_call(
        functools.partial(layer_kernel, R, T, D, F, nh, names),
        out_shape=(
            jax.ShapeDtypeStruct((2, NG, D // NG, D), BF),
            jax.ShapeDtypeStruct((2, NG, D // 2 // NG, D), BF),
            jax.ShapeDtypeStruct((2, 2, 2, 64, D), BF),
            jax.ShapeDtypeStruct((2, 2, 2, 64, D), BF),
            jax.ShapeDtypeStruct((16, D), F32),
        ),
        in_specs=[sm, sm, hb, hb, vm, vm, hb, vm, hb, vm, vm, vm, hb, vm, hb, vm],
        out_specs=(hb, hb, hb, hb, hb),
        scratch_shapes=list(sizes.values()),
        compiler_params=pltpu.CompilerParams(
            collective_id=0, has_side_effects=True, vmem_limit_bytes=67043328),
        name="layer",
    )(block_pos, block_seq, tokens.reshape(8, 64, D), cotangent.reshape(8, 64, D), row(ln1_gain),
      row(ln1_bias), wqt, qv_bias, out_weight.reshape(2, local // 2, D), row(out_bias), row(ln2_gain), row(ln2_bias), fc_weight,
      row(fc_bias), proj_weight, row(proj_bias))

    rank = lax.axis_index("ctx").astype(jnp.int32).reshape(1)
    vec = jax.ShapeDtypeStruct((D,), F32)
    outs = pl.pallas_call(
        functools.partial(finish_kernel, R),
        out_shape=(
            jax.ShapeDtypeStruct((4 * BLK, D), BF),
            jax.ShapeDtypeStruct((4 * BLK, D), BF),
            vec, vec,
            jax.ShapeDtypeStruct((3 * local, D), F32),
            jax.ShapeDtypeStruct((2, local), F32),
            jax.ShapeDtypeStruct((local, D), F32),
            vec, vec, vec,
            jax.ShapeDtypeStruct((D, F), F32),
            vec,
            jax.ShapeDtypeStruct((F, D), F32),
            vec,
        ),
        in_specs=[sm, sm, sm, hb, hb, hb, hb, hb],
        out_specs=(hb, hb, vm, vm, hb, vm, hb, vm, vm, vm, hb, vm, hb, vm),
        scratch_shapes=[
            pltpu.VMEM((2, D, D), BF), pltpu.VMEM((D, D), BF), pltpu.VMEM((2, 2, BLK, D), BF),
            pltpu.VMEM((2, 2, BLK, D), BF), pltpu.VMEM((16, D), F32), pltpu.VMEM((2, D, D), F32),
            pltpu.VMEM((D, D), F32), pltpu.SemaphoreType.DMA((9,)), pltpu.SemaphoreType.DMA((15,)),
        ],
        name="finish",
    )(block_pos, block_seq, rank, w1.reshape(2, D, D), w2.reshape(D, D),
      fo.reshape(2, 2, BLK, D), fg.reshape(2, 2, BLK, D), vs)
    (output, grad_tokens, ln1g, ln1b, gq, gqv, go, ob, ln2g, ln2b, gf, fb, gp, pb) = outs
    flat = lambda v: v
    return (output, grad_tokens, flat(ln1g), flat(ln1b),
            jnp.transpose(gq.reshape(3, local, D), (2, 0, 1)), gqv, go, flat(ob), flat(ln2g), flat(ln2b),
            gf, flat(fb), gp, flat(pb))


def solution(mesh):
    R = mesh.shape["ctx"]
    T = mesh.shape["tp"]
    return jax.shard_map(
        functools.partial(per_device, R, T),
        mesh=mesh,
        in_specs=(
            P("ctx", None), P("ctx", None), P(), P(), P(), P(), P(None, None, "tp"), P(None, "tp"),
            P("tp", None), P(), P(), P(), P(None, "tp"), P("tp"), P("tp", None), P(),
        ),
        out_specs=(
            P("ctx", None), P("ctx", None), P(), P(), P(None, None, "tp"), P(None, "tp"), P("tp", None),
            P(), P(), P(), P(None, "tp"), P("tp"), P("tp", None), P(),
        ),
        check_vma=False,
    )
```

```python
import functools
from types import SimpleNamespace

import jax
import jax.numpy as jnp
from jax import lax
from jax.experimental import pallas as pl
from jax.experimental.pallas import tpu as pltpu
from jax.sharding import PartitionSpec as P

HEAD = 64
BLK = 128

class Names:
    def __getattr__(self, name):
        return name


ID = Names()
BF = jnp.bfloat16
F32 = jnp.float32
MESH = pl.DeviceIdType.MESH
NEG = -1e30
C0 = 0.7978845608028654
C1 = 0.044715
U = 4
SENDS = 70
SPLIT_AT = 22
ARRIVALS = 154
TIDY = (ID.far1, ID.feed1, ID.weights_b, (ID.n2_, 2), ID.high, ID.low, ID.low3, ID.collect1, ID.collect0, (ID.n1_, 0), (ID.n1_, 2))

LAT = 2.3
OUT_FROM = 14.0
OUT_GAP = 1.0
DS = (3, 2, 1)


def dg(a, b, ca, cb):
    return lax.dot_general(a, b, (((ca,), (cb,)), ((), ())), preferred_element_type=F32)


def normed(x):
    centre = jnp.mean(x, axis=-1, keepdims=True)
    shifted = x - centre
    spread = jnp.mean(shifted * shifted, axis=-1, keepdims=True)
    inverse = lax.rsqrt(spread + 1e-05)
    return shifted * inverse, inverse


def fold8(x):
    rows, width = x.shape
    return jnp.sum(x.reshape(rows // 8, 8, width), axis=0)


def roll64(x):
    return pltpu.roll(x, 64, 1)


def simulate(T, jobs, marks, lat, order=None):
    free = {}
    seen = [dict() for _ in range(T)]
    inbox = [[] for _ in range(T)]
    now = [0.0] * T
    steps = [dict() for _ in range(T)]
    left = [list(marks) if order is None else list(order) for _ in range(T)]
    out = [[] for _ in range(T)]
    parts = [dict() for _ in range(T)]
    OP = 0.12

    def post(time, z, step, op):
        tau = jobs[op[3]][0][op[2]]
        begin = max(time, free.get((z, step), 0.0))
        free[z, step] = begin + tau
        inbox[z + step].append((begin + tau + lat, op))

    transit = []

    def cross(entry):
        time, z, to, op = entry
        step = 1 if to > z else -1
        tau = jobs[op[3]][0][op[2]]
        begin = max(time, free.get((z, step), 0.0))
        free[z, step] = begin + tau
        if z + step == to:
            inbox[to].append((begin + tau + lat, op))
        else:
            transit.append((begin + 0.7, z + step, to, op))

    def spread(time, z, op):
        if jobs[op[3]][4]:
            transit.extend((time, z, to, op) for to in range(T) if to != z)
            return
        if z >= op[1] and z < T - 1:
            post(time, z, 1, op)
        if z <= op[1] and z > 0:
            post(time, z, -1, op)

    def passive(z, op):
        kind, i, u, name = op
        if kind in (ID.R, ID.L):
            return i == z
        return jobs[name][4] or (z in (0, T - 1) and jobs[name][2])

    def start_of(z, item):
        if item[0] == ID.op:
            time, op = item[1]
            if op[0] in (ID.R, ID.L):
                own = parts[z].get((op[3], op[2]))
                if own is None:
                    return None
                time = max(time, own)
            return max(time, now[z])
        step = marks[item[1]]
        time = max(now[z], step.get(ID.time, 0.0))
        for name, delay in step.get(ID.after, ()):
            if name not in steps[z]:
                return None
            time = max(time, steps[z][name] + delay)
        for event in step.get(ID.needs, ()):
            event = tuple(z if e == ID.z else e for e in event)
            if event[0] in (ID.R, ID.L) and event[1] == (0 if event[0] == ID.R else T - 1):
                continue
            if event[0] == ID.A and event[1] == z:
                continue
            if event not in seen[z]:
                return None
            time = max(time, seen[z][event])
        return time

    while True:
        best = None
        for entry in transit:
            key = (entry[0], -1, entry[1], entry[2])
            if best is None or key < best[0]:
                best = (key, entry[1], (ID.cross, entry))
        for z in range(T):
            for entry in list(inbox[z]):
                if passive(z, entry[1]):
                    seen[z][entry[1]] = entry[0]
                    inbox[z].remove(entry)
            for entry in inbox[z]:
                time = start_of(z, (ID.op, entry))
                if time is not None:
                    key = (time, 0 if jobs[entry[1][3]][3] == 0 else 1, entry[0], z)
                    if best is None or key < best[0]:
                        best = (key, z, (ID.op, entry))
            choices = left[z][:1] if order is not None else left[z]
            for k, name in enumerate(choices):
                time = start_of(z, (ID.mark, name))
                if time is not None:
                    key = (time + 0.01, 2 + marks[name].get(ID.low, 0), k, z)
                    if best is None or key < best[0]:
                        best = (key, z, (ID.mark, name))
        if best is None:
            break
        key, z, item = best
        if item[0] == ID.cross:
            transit.remove(item[1])
            cross(item[1])
            continue
        begin = start_of(z, item)
        if item[0] == ID.op:
            _, op = item[1]
            inbox[z].remove(item[1])
            out[z].append((begin, item[1][1]))
            now[z] = begin + OP
            if op[0] == ID.A:
                seen[z][op] = begin
                spread(now[z], z, op)
            else:
                post(now[z], z, 1 if op[0] == ID.R else -1, op)
        else:
            name = item[1]
            step = marks[name]
            left[z].remove(name)
            out[z].append((begin, (ID.M, name)))
            now[z] = begin + step[ID.dur]
            steps[z][name] = now[z]
            for job, u, kind in step.get(ID.posts, ()):
                if kind == ID.gather:
                    spread(now[z], z, (ID.A, z, u, job))
                else:
                    parts[z].setdefault((job, u), now[z])
                    for d in kind:
                        if z == 0:
                            post(now[z], z, 1, (ID.R, d, u, job))
                        if z == T - 1:
                            post(now[z], z, -1, (ID.L, T - 1 - d, u, job))
    if order is None:
        spots = {name: sum(t for z in range(T) for t, op in out[z] if op == (ID.M, name)) for name in marks}
        assert all(len(l) == 0 for l in left), left
        return simulate(T, jobs, marks, lat, sorted(marks, key=lambda n: spots[n]))
    assert all(len(l) == 0 for l in left) and all(len(i) == 0 for i in inbox + [transit]), (left, inbox)
    return out, max(now)

def emit(T, z, timeline, jobs, marks, actors, steps, flush):
    names = [op[1] for _, op in timeline[0] if op[0] == ID.M]
    todo = [[op for _, op in timeline[zz]] for zz in range(T)]
    waited = [set() for _ in range(T)]
    for name in names:
        for zz in range(T):
            now = []
            while todo[zz][0] != (ID.M, name):
                now.append(todo[zz].pop(0))
            todo[zz].pop(0)
            for event in marks[name].get(ID.needs, ()):
                job = jobs.get(event[3])
                if event[0] == ID.A and event[1] != zz and (job[4] or (zz in (0, T - 1) and job[2])):
                    if event not in waited[zz]:
                        waited[zz].add(event)
                        now.append(event)
            if now:
                @pl.when(z == zz)
                def _(now=now, zz=zz):
                    for op in now:
                        actors[op[3]].one(op, zz)
        if name in steps:
            steps[name]()
        if name in TIDY:
            flush()


def timetable(U, T):
    S = U // 2
    tau = 4.18 / U + 0.1
    hi, lo = range(S), range(S, U)
    norm = 0.15 + 0.8 / U
    jobs = {
        ID.wo: ([1.65] * 2, False, True, 0, False), ID.ab: ([1.5] * 2, False, True, 0, False),
        ID.ac: ([0.8] * 2, False, True, 0, False), ID.ga2: ([tau] * U, True, True, 0, False),
        ID.out: ([tau] * U, True, False, 1, False), ID.ga1: ([tau] * U, True, False, 0, False),
        ID.small: ([0.5], False, False, 1, True),
    }
    m = {}

    def step(name, dur, after=(), needs=(), posts=(), low=0, time=0.0):
        m[name] = dict(dur=dur, after=list(after), needs=list(needs), posts=list(posts), low=low, time=time)

    def every(job, pieces):
        return [(ID.A, i, u, job) for i in range(T) for u in pieces]

    step(ID.wo, 0.0, posts=[(ID.wo, 0, ID.gather), (ID.wo, 1, ID.gather)])
    step(ID.go, 0.3, [(ID.wo, 2.2)])
    step(ID.own, 2.4, [(ID.go, 0)])
    step(ID.relay0, 0.1, [(ID.go, 3.3)])
    step(ID.near0, 1.1, [(ID.go, 4.6), (ID.relay0, 0), (ID.own, 0)])
    step(ID.relay1, 0.1, [(ID.go, 6.0), (ID.relay0, 0)])
    step(ID.far0, 1.1, [(ID.relay0, 4.2), (ID.near0, 0)], posts=[(ID.ab, 0, ID.gather)])
    step(ID.near1, 1.1, [(ID.relay1, 2.0), (ID.far0, 0)])
    step(ID.relay2, 0.1, [(ID.relay1, 4.6)])
    step(ID.far1, 1.1, [(ID.relay1, 4.4), (ID.near1, 0)], posts=[(ID.ab, 1, ID.gather)])
    step(ID.upstream, 0.8, [(ID.far1, 0)])
    step(ID.near2, 1.1, [(ID.relay2, 2.0), (ID.upstream, 0)])
    step(ID.far2, 1.2, [(ID.relay2, 4.0), (ID.near2, 0)], posts=[(ID.ac, 0, ID.gather), (ID.ac, 1, ID.gather)])
    step(ID.pads, 0.4, [(ID.far2, 0)], every(ID.wo, [0, 1]))
    step(ID.mix, 1.0, [(ID.pads, 0)], every(ID.ab, [0, 1]))
    step(ID.feed1, 3.1, [(ID.mix, 0)], every(ID.ac, [0]), [(ID.ga2, u, DS) for u in hi])
    step(ID.feed0, 3.1, [(ID.feed1, 0)], every(ID.ac, [1]), [(ID.ga2, u, DS) for u in lo])
    step(ID.weights_a, 0.8, [(ID.feed0, 2.0)], low=1)
    step(ID.weights_a2, 0.8, [(ID.weights_a, 0)], low=1)
    step(ID.out_partial, 0.8, [(ID.weights_a2, 2.0)], low=1)
    step(ID.weights_b, 0.4, [(ID.weights_a2, 4.5)], low=1)
    step(ID.near_w1, 0.3, [(ID.weights_b, 5.0)], low=1)
    for u in range(U):
        sums = lambda job: [(ID.R, ID.z, u, job), (ID.L, ID.z, u, job)]
        step((ID.n2_, u), norm, needs=sums(ID.ga2), posts=[(ID.ga2, u, ID.gather)])
        for d in DS:
            step((ID.begin_out, u, d), 0.0, [(ID.out_partial, 0), (ID.feed0, OUT_FROM + OUT_GAP * (3 * u + 3 - d))],
                 posts=[(ID.out, u, (d,))], low=1)
        step((ID.out_, u), 0.2, needs=sums(ID.out), posts=[(ID.out, u, ID.gather)], low=1)
        step((ID.n1_, u), norm, needs=sums(ID.ga1), posts=[(ID.ga1, u, ID.gather)])
    step(ID.norm_sums, 1.8, [(ID.weights_c, 0)], posts=[(ID.small, 0, ID.gather)], low=1)
    step(ID.high, 1.4, needs=every(ID.ga2, hi))
    step(ID.high2, 0.9, [(ID.high, 0)])
    step(ID.near_k1a, 0.15, [(ID.high, 3.4), (ID.high2, 0)])
    step(ID.high3, 0.9, [(ID.high2, 0)])
    step(ID.near_k1b, 0.15, [(ID.near_k1a, 0), (ID.high3, 0)])
    step(ID.mid3, 0.9, [(ID.high3, 0)])
    step(ID.mid2, 0.9, [(ID.mid3, 0)])
    step(ID.mid1, 0.9, [(ID.mid2, 0)])
    step(ID.low, 1.4, [(ID.mid3, 0), (ID.near_k1b, 0)], every(ID.ga2, lo))
    step(ID.low2, 0.9, [(ID.low, 0), (ID.mid2, 0)])
    step(ID.near_k0a, 0.15, [(ID.low, 3.4), (ID.low2, 0)])
    step(ID.low3, 0.9, [(ID.low2, 0), (ID.mid1, 0)])
    step(ID.near_k0b, 0.15, [(ID.near_k0a, 0), (ID.low3, 0)])
    step(ID.own_hi, 1.7, [(ID.low3, 0)])
    step(ID.collect1, 0.9, [(ID.own_hi, 0), (ID.near_k1b, 7.0)], posts=[(ID.ga1, u, DS) for u in hi])
    step(ID.own_lo, 0.9, [(ID.collect1, 0)])
    step(ID.finish_w1, 0.3, [(ID.near_w1, 8.0), (ID.near_k0b, 0)], low=1)
    step(ID.aw, 0.6, [(ID.own_lo, 0)], low=1)
    step(ID.collect0, 0.9, [(ID.own_lo, 0), (ID.near_k0b, 7.0)], posts=[(ID.ga1, u, DS) for u in lo])
    step(ID.weights_c, 0.7, [(ID.collect0, 0), (ID.aw, 0)], low=1)
    step(ID.weights_d, 0.3, [(ID.weights_c, 3.0)], low=1)
    step(ID.near_w2, 0.2, [(ID.weights_d, 3.5)], low=1)
    step(ID.relay_w1, 0.05, [(ID.finish_w1, 6.5)], low=1)
    step(ID.finish_w2, 0.2, [(ID.near_w2, 5.0)], low=1)
    step(ID.relay_w2, 0.05, [(ID.finish_w2, 4.0)], low=1)
    step(ID.pair_w1, 0.05, [(ID.relay_w1, 5.0)], low=1)
    step(ID.give_w1, 0.05, [(ID.pair_w1, 4.5)], low=1)
    step(ID.give_o, 0.1, [((ID.out_, U - 1), 2.0)], every(ID.out, range(U)), low=1)
    step(ID.sums, 0.2, needs=every(ID.small, [0]), low=1)
    step(ID.pair_w2, 0.05, [(ID.relay_w2, 3.5)], low=1)
    step(ID.give_v, 0.1, [(ID.sums, 3.0)], low=1)
    step(ID.give_w2, 0.05, [(ID.pair_w2, 3.0)], low=1)
    step(ID.give_hi, 0.1, [(ID.give_o, 0)], every(ID.ga1, hi), low=1)
    step(ID.end, 0.0, [(ID.give_v, 0), (ID.give_hi, 0), (ID.give_w1, 0), (ID.give_w2, 0)], every(ID.ga1, range(U)))
    return jobs, m


def scratch_list(R, T, D, F, nh):
    NG = R // 2
    N = 4 * BLK
    v = pltpu.VMEM
    rows = v((8, 64, D), BF)
    return dict(
        tok_raw=(rows),
        cot_raw=(rows),
        stage=(v((2, 2, 2, 64, D), BF)),
        x=(rows),
        cot=(rows),
        wqt=(v((640, D), BF)),
        wo=(v((T, 2, nh * HEAD // 2, D), BF)),
        wolo=(v((nh, T, BLK, D), BF)),
        wohi=(v((nh, T, BLK, D), BF)),
        wopad=(v((nh * BLK, D), BF)),
        fc=(v((D, F), BF)),
        pw=(v((F, D), BF)),
        brow=(v((1, 640), F32)),
        act1=(rows),
        q=(v((nh, N, 128), BF)),
        kv=(v((NG, nh, N, 128), BF)),
        pre=(v((N, D), F32)),
        ga=(v((N, F), F32)),
        hid=(v((8, 64, D), F32)),
        act2=(v((N, D), BF)),
        actd=(v((N, F), BF)),
        gpre=(v((N, F), BF)),
        mlo=(v((4 if NG == 4 else 1, 256, 256), F32)),
        mhi=(v((4 if NG == 4 else 1, 256, 256), F32)),
        m=(v((2 * nh, 1, 256), F32)),
        l=(v((2 * nh, 1, 256), F32)),
        delta=(v((2 * nh, 1, 256), F32)),
        acc=(v((2 * nh, 128, 256), F32)),
        attp=(v((nh, N, 128), BF)),
        attn=(v((N, 256), BF)),
        ab=(v((T, nh, 256, 128), BF)),
        p1=(rows), r1=(rows), l1=(rows),
        r2=(rows), l2=(rows),
        r3=(rows), l3=(rows),
        gh=(v((2, 64, D), F32)),
        h=(rows),
        do=(v((nh, N, 128), BF)),
        dkf=(v((4 if NG == 4 else 1, nh, 256, 128), F32)),
        dk=(v((NG, nh, N, 128), BF)),
        dkr=(v((NG, nh, N, 128), BF)),
        dka=(v((2, 2, nh, 128, 128), BF)),
        gn=(v((N, 640), BF)),
        w1=(v((2, NG, D // NG, D), BF)),
        w1r=(v((NG, D // NG, D), BF)),
        w1s=(v((NG, D // NG, D), BF)),
        w1a=(v((2, D // NG // 2, D), BF)),
        w1f=(v((2, NG, D // NG, D), BF)),
        w2=(v((2, NG, D // 2 // NG, D), BF)),
        w2r=(v((NG, D // 2 // NG, D), BF)),
        w2s=(v((NG, D // 2 // NG, D), BF)),
        w2a=(v((2, D // 2 // NG // 2, D), BF)),
        w2f=(v((2, NG, D // 2 // NG, D), BF)),
        yo=(rows),
        yg=(rows),
        mo=(v((2, 2, 64, D), BF)),
        mg=(v((2, 2, 64, D), BF)),
        vsum=(v((16, D), F32)),
        vz=(v((T, 16, D), BF)),
        vc=(v((R, 16, D), BF)),
        ss=(pltpu.SemaphoreType.DMA((SENDS if NG == 4 else 200,))),
        rs=(pltpu.SemaphoreType.DMA((ARRIVALS if NG == 4 else 400,))),
        ls=(pltpu.SemaphoreType.DMA((24,))),
    )


def layer_kernel(R, T, D, F, nh, names, *refs):
    (pos_ref, seq_ref, tok_hbm, cot_hbm, g1_ref, b1_ref, wqt_hbm, qvb_ref, wo_hbm, ob_ref, g2_ref,
     b2_ref, fc_hbm, fcb_ref, pw_hbm, pb_ref, w1_out, w2_out, fo_out, fg_out, v_out) = refs[:21]
    s = SimpleNamespace(**dict(zip(names, refs[21:])))
    s.p2, s.p3 = s.tok_raw, s.cot_raw
    NG = R // 2
    N = 4 * BLK
    Q1 = D // NG
    Q2 = D // 2 // NG
    SUB = U // 2
    RU = 64 // SUB
    r = lax.axis_index("ctx")
    z = lax.axis_index("tp")
    c = lax.rem(r, 2)
    o = 1 - c
    g = lax.div(r, 2)
    mate = 2 * g + o
    zp, zm = z + 1, z - 1
    not_core = [c != 0, c != 1]
    if NG == 4:
        ga_ = g + 1 - 2 * lax.rem(g, 2)
        gb_ = g + 2 - 4 * lax.div(g, 2)
        gc_ = ga_ + 2 - 4 * lax.div(ga_, 2)
        peers = [g, ga_, gb_, gc_]
        sources = peers
    else:
        peers = [lax.rem(g + t, NG) for t in range(NG)]
        sources = [lax.rem(g + NG - t, NG) for t in range(NG)]

    most = {ID.common: 0, ID.line: 0}
    spare = {ID.common: [], 0: [], 1: [], 2: [], 3: []}
    started = [[], []]
    ids = [0]
    SPLIT = SPLIT_AT if NG == 4 else 100

    def take(pool):
        if spare[pool]:
            return spare[pool].pop(0)
        kind = ID.common if pool == ID.common else pool
        most[kind] = most.get(kind, 0) + 1
        return most[kind] - 1 + (0 if pool == ID.common else SPLIT)

    def flush(last=False):
        for batch in ([started[0]] if not last else started):
            for pool in (ID.common, 0, 1, 2, 3):
                mine = [e for e in batch if e[0] == pool]
                if pool == ID.common:
                    for _, _, done in mine:
                        done()
                elif mine:
                    @pl.when(z == pool)
                    def _(mine=mine):
                        for _, _, done in mine:
                            done()
                spare[pool].extend(e[1] for e in mine)
        started[0] = started[1]
        started[1] = []

    def new(count=1):
        first = ids[0]
        ids[0] += count
        return first

    def remote(src, dst, mine, slot, dev):
        src = src() if callable(src) else src
        dst = dst() if callable(dst) else dst
        return pltpu.make_async_remote_copy(
            src_ref=src, dst_ref=dst, send_sem=s.ss.at[mine], recv_sem=s.rs.at[slot],
            device_id=dev, device_id_type=MESH)

    def send(src, dst, slot, dev, cond=None, at=None):
        pool = ID.common if at is None else at
        mine = take(pool)

        def go():
            remote(src, dst, mine, slot, dev).start()

        def done():
            remote(src, dst, mine, slot, dev).wait_send()

        if cond is None:
            go()
            started[1].append((pool, mine, done))
        else:
            pl.when(cond)(go)
            started[1].append((pool, mine, lambda: pl.when(cond)(done)))

    def arrived(dst, slot, cond=None):
        def go():
            remote(dst, dst, 0, slot, (r, z)).wait_recv()

        if cond is None:
            go()
        else:
            pl.when(cond)(go)

    loads = {}

    def load(name, src, dst, k):
        loads[name] = pltpu.make_async_copy(src, dst, s.ls.at[k])
        loads[name].start()

    load(ID.tok, tok_hbm, s.tok_raw, 0)
    load(ID.wqt, wqt_hbm, s.wqt.at[pl.ds(0, 3 * nh * HEAD)], 1)
    load(ID.wo, wo_hbm, s.wo.at[z], 3)
    load(ID.cot, cot_hbm, s.cot_raw, 2)
    load(ID.pw, pw_hbm, s.pw, 4)
    load(ID.fc, fc_hbm, s.fc, 5)

    barrier = pltpu.get_barrier_semaphore()
    for t in range(1, R):
        pl.semaphore_signal(barrier, inc=1, device_id=(lax.rem(r + t, R), z), device_id_type=MESH)

    for t in range(1, T):
        pl.semaphore_signal(barrier, inc=1, device_id=(r, lax.rem(z + t, T)), device_id_type=MESH)
    pl.semaphore_wait(barrier, R + T - 2)

    def find(seq):
        low = jnp.int32(0)
        high = jnp.int32(0)
        for b in range(4):
            same = seq_ref[4 * r + b] == seq
            first = pos_ref[4 * r + b] < R
            low = jnp.where(same & first, b, low)
            high = jnp.where(same & jnp.logical_not(first), b, high)
        return low, high

    def low_pos(rank):
        total = jnp.int32(0)
        for b in range(4):
            here = (seq_ref[4 * rank + b] == c) & (pos_ref[4 * rank + b] < R)
            total = total + jnp.where(here, pos_ref[4 * rank + b], 0)
        return total

    other = find(o)
    own = find(c)
    q_low = (low_pos(2 * g), low_pos(2 * g + 1))

    def swap(raw, k_stage, dst, base):
        for k in range(2):
            s.stage[k_stage, k] = raw[pl.ds(2 * other[k], 2)]
            send(s.stage.at[k_stage, k], dst.at[pl.ds(4 * k + 2 * c, 2)], base + k, (mate, z))
        for k in range(2):
            dst[pl.ds(4 * k + 2 * c, 2)] = raw[pl.ds(2 * own[k], 2)]

    def swapped(dst, base):
        for k in range(2):
            arrived(dst.at[pl.ds(4 * k + 2 * o, 2)], base + k)

    sx = new(4)
    loads[ID.tok].wait()
    swap(s.tok_raw, 0, s.x, sx)

    class Gather:
        def __init__(self, at, pieces, pass_on=None):
            self.at, self.hand = at, pass_on
            self.base = [new(T) for _ in range(pieces)]

        def start(self, u):
            for zz in range(T):
                @pl.when(z == zz)
                def _(zz=zz):
                    a = lambda: self.at(zz, u)
                    if zz < T - 1:
                        send(a, a, self.base[u] + zz, (r, zp), at=zz)
                    if zz > 0:
                        send(a, a, self.base[u] + zz, (r, zm), at=zz)

        def one(self, op, at):
            _, i, u, _ = op
            slot = self.base[u] + i
            a = lambda: self.at(i, u)
            arrived(a, slot)
            if at > i and at < T - 1:
                send(a, a, slot, (r, zp), at=at)
            if at < i and at > 0:
                send(a, a, slot, (r, zm), at=at)
            if self.hand is not None:
                self.hand(i, u, at)

    class Direct:
        def __init__(self, at, pieces):
            self.at = at
            self.base = [new(T) for _ in range(pieces)]

        def start(self, u):
            a = self.at(z, u)
            for t in range(1, T):
                send(a, a, self.base[u] + t, (r, lax.rem(z + t, T)))

        def one(self, op, at):
            _, i, u, _ = op
            arrived(lambda: self.at(i, u), self.base[u] + (at - i) % T)

    def piece(buf, i, u):
        half = 1 if u < SUB else 0
        if SUB == 1:
            return buf.at[4 * half + i]
        return buf.at[4 * half + i, pl.ds(RU * (u % SUB), RU)]

    class Sum:
        def __init__(self, part, from_left, from_right, whole, landing=None, slots=None):
            self.part, self.fl, self.fr = part, from_left, from_right
            self.whole, self.landing = whole, landing
            self.rl = [new(T + 1) for _ in range(U)] if slots is None else slots
            self.ag = self.rl
            self.hand = [new(2) for _ in range(U)] if landing is not None else None

            @pl.when(z == 0)
            def _():
                from_left[0] = jnp.zeros((64, D), BF)
                from_left[4] = jnp.zeros((64, D), BF)

            @pl.when(z == T - 1)
            def _():
                from_right[T - 1] = jnp.zeros((64, D), BF)
                from_right[4 + T - 1] = jnp.zeros((64, D), BF)

        def begin(self, u, ds=(3, 2, 1)):
            @pl.when(z == 0)
            def _():
                for d in ds:
                    send(self.see(self.part, d, u), self.see(self.fl, d, u), self.rl[u] + d, (r, zp), at=0)

            @pl.when(z == T - 1)
            def _():
                for d in ds:
                    e = T - 1 - d
                    send(self.see(self.part, e, u), self.see(self.fr, e, u), self.slot(u, e, T - 2), (r, zm), at=T - 1)

        def slot(self, u, d, to):
            return self.rl[u] + (T if d == to else d)

        def see(self, buf, i, u):
            return lambda: piece(buf, i, u)

        def one(self, op, at):
            kind, i, u, _ = op
            if kind == ID.A:
                slot = self.ag[u] + i
                a = self.see(self.whole, i, u)
                arrived(a, slot)
                if at > i and at < T - 1:
                    send(a, a, slot, (r, zp), at=at)
                if at < i and at > 0:
                    send(a, a, slot, (r, zm), at=at)
                self.pass_on(i, u, at)
                return
            right = kind == ID.R
            buf = self.fl if right else self.fr
            arrived(self.see(buf, i, u), self.rl[u] + i)
            slot = self.rl[u] + i if right else self.slot(u, i, at - 1)
            a = piece(self.part, i, u)
            a[...] = (a[...].astype(F32) + piece(buf, i, u)[...].astype(F32)).astype(BF)
            send(self.see(self.part, i, u), self.see(buf, i, u), slot, (r, zp if right else zm), at=at)

        def spot(self, i, u):
            half = 1 if u < SUB else 0
            if SUB == 1:
                return self.landing.at[half, i % 2]
            return self.landing.at[half, i % 2, pl.ds(RU * (u % SUB), RU)]

        def pass_on(self, i, u, at):
            if self.landing is None:
                return
            send(self.see(self.whole, i, u), lambda: self.spot(i, u), self.hand[u] + i % 2, (mate, z),
                 not_core[i // 2], at=at)

        def last(self, u):
            for at in range(T):
                @pl.when(z == at)
                def _(at=at):
                    if at > 0:
                        arrived(self.see(self.fl, at, u), self.rl[u] + at)
                    if at < T - 1:
                        arrived(self.see(self.fr, at, u), self.rl[u] + T)

        def total(self, index, rows):
            return (self.part[index, rows, :].astype(F32) + self.fl[index, rows, :].astype(F32)
                    + self.fr[index, rows, :].astype(F32))

        def gather(self, u):
            for at in range(T):
                @pl.when(z == at)
                def _(at=at):
                    a = self.see(self.whole, at, u)
                    if at < T - 1:
                        send(a, a, self.ag[u] + at, (r, zp), at=at)
                    if at > 0:
                        send(a, a, self.ag[u] + at, (r, zm), at=at)
                    self.pass_on(at, u, at)

        def handed(self, pieces):
            for u in pieces:
                for k in range(2):
                    arrived(self.spot(k, u), self.hand[u] + k)

    class PlaneSum:
        def __init__(self, part, cut, far, near):
            self.part, self.cut, self.fl, self.near_buf = part, cut, far, near
            self.base = new(max(4, NG))

        def far(self):
            if NG == 4:
                for k in range(2):
                    send(self.part(peers[3], k), self.fl(k), self.base + k, (2 * peers[1 + k] + c, z))

        def near(self, ks=(0, 1)):
            if NG == 4:
                for k in ks:
                    to = peers[2 - k]
                    arrived(self.fl(k), self.base + k)
                    self.cut(to, k)
                    send(self.part(to, None), self.near_buf(2 - k), self.base + 2 + k, (2 * to + c, z))
            else:
                for t in range(1, NG):
                    send(self.part(peers[t], None), self.near_buf(t), self.base + t, (2 * peers[t] + c, z))

        def arrived(self):
            if NG == 4:
                for k in range(2):
                    arrived(self.near_buf(2 - k), self.base + 2 + k)
            else:
                for t in range(1, NG):
                    arrived(self.near_buf(t), self.base + t)

    class PlaneGather:
        def __init__(self, at):
            self.at = at
            self.base = new(max(6, NG))

        def start(self):
            if NG == 4:
                for t, first in ((1, 0), (2, 1)):
                    for leg, half in ((0, first), (1, 1 - first)):
                        a = self.at(g, half)
                        send(a, a, self.base + 2 * (t - 1) + leg, (2 * peers[t] + c, z))
            else:
                for t in range(1, NG):
                    send(self.at(g, None), self.at(g, None), self.base + t, (2 * peers[t] + c, z))

        def relay(self):
            if NG == 4:
                for t, half in ((1, 0), (2, 1)):
                    a = self.at(peers[t], half)
                    arrived(a, self.base + 2 * (t - 1))
                    send(a, a, self.base + 3 + t, (2 * peers[3 - t] + c, z))

        def arrived(self):
            if NG == 4:
                for t, half in ((1, 1), (2, 0)):
                    arrived(self.at(peers[t], half), self.base + 2 * (t - 1) + 1)
                for t, half in ((1, 0), (2, 1)):
                    arrived(self.at(peers[3], half), self.base + 3 + t)
            else:
                for t in range(1, NG):
                    arrived(self.at(sources[t], None), self.base + t)

    WP = nh * HEAD // 4
    swo = new(2 * T)

    def wo_at(i, u, core=None):
        return s.wo.at[i, c if core is None else core, pl.ds(WP * u, WP)]

    def hand_wo(i, u, at):
        send(lambda: wo_at(i, u), lambda: wo_at(i, u), swo + T * u + i, (mate, z), at=at)

    wo_line = Gather(wo_at, 2, hand_wo)
    loads[ID.wo].wait()
    wo_line.start(0)
    wo_line.start(1)
    s.wqt[pl.ds(3 * nh * HEAD, 640 - 3 * nh * HEAD), :] = jnp.zeros((640 - 3 * nh * HEAD, D), BF)
    s.brow[...] = jnp.zeros((1, 640), F32)
    s.brow[:, 0:192] = qvb_ref[0:1, :]
    s.brow[:, 384:576] = qvb_ref[1:2, :]
    g1 = g1_ref[...].reshape(1, -1)
    b1 = b1_ref[...].reshape(1, -1)
    lo_a, hi_a = pl.ds(0, 256), pl.ds(256, 256)

    def project(first):
        for k in range(2):
            for i in range(2):
                j = 4 * k + 2 * first + i
                n, _inv = normed(s.x[j].astype(F32))
                s.act1[j] = (n * g1 + b1).astype(BF)
        a = jnp.concatenate([s.act1[pl.ds(4 * k + 2 * first, 2)].reshape(BLK, D) for k in range(2)], axis=0)
        s.pre[0:256, 0:640] = dg(a, s.wqt[...], 1, 1)
        low = lax.broadcasted_iota(jnp.int32, (BLK, 128), 1) < HEAD
        zero = jnp.zeros((BLK, 128), F32)
        for k in range(2):
            t = [s.pre[BLK * k:BLK * k + BLK, 128 * i:128 * i + 128] + s.brow[:, 128 * i:128 * i + 128]
                 for i in range(5)]
            rows = pl.ds(pl.multiple_of((2 * k + first) * BLK, BLK), BLK)
            s.kv[g, 0, rows, :] = jnp.where(low, roll64(t[1]), roll64(t[3])).astype(BF)
            s.kv[g, 1, rows, :] = jnp.where(low, t[2], t[3]).astype(BF)
            s.kv[g, 2, rows, :] = jnp.where(low, roll64(t[2]), roll64(t[4])).astype(BF)
            s.q[0, rows, :] = (jnp.where(low, t[0], zero) * 0.125).astype(BF)
            s.q[1, rows, :] = (jnp.where(low, roll64(t[0]), zero) * 0.125).astype(BF)
            s.q[2, rows, :] = (jnp.where(low, t[1], zero) * 0.125).astype(BF)

    loads[ID.wqt].wait()
    project(c)
    swapped(s.x, sx)
    project(o)

    skv = new(max(6 * nh, NG))

    def kv_go(h, leg):
        for t, halves in ((1, (lo_a, hi_a)), (2, (hi_a, lo_a))):
            a = s.kv.at[g, h, halves[leg]]
            send(a, a, skv + 6 * h + 2 * (t - 1) + leg, (2 * peers[t] + c, z))

    def kv_relay(h):
        for t, to, half in ((1, 2, lo_a), (2, 1, hi_a)):
            a = s.kv.at[peers[t], h, half]
            arrived(a, skv + 6 * h + 2 * (t - 1))
            send(a, a, skv + 6 * h + 3 + t, (2 * peers[to] + c, z))

    def kv_rest(h):
        for t, half in ((1, hi_a), (2, lo_a)):
            arrived(s.kv.at[peers[t], h, half], skv + 6 * h + 2 * (t - 1) + 1)

    def kv_far(h):
        for t, half in ((1, lo_a), (2, hi_a)):
            arrived(s.kv.at[peers[3], h, half], skv + 6 * h + 3 + t)

    def masks(src):
        k_low = (low_pos(2 * src), low_pos(2 * src + 1))
        i0 = lax.broadcasted_iota(jnp.int32, (256, 256), 0)
        i1 = lax.broadcasted_iota(jnp.int32, (256, 256), 1)

        def token(i, a, b):
            return i + jnp.where(i < BLK, a * BLK, b * BLK - BLK)

        last = 2 * R - 1
        low_mask = jnp.where(token(i0, *k_low) <= token(i1, *q_low), 0.0, NEG)
        high_mask = jnp.where(
            token(i0, last - k_low[0], last - k_low[1])
            <= token(i1, last - q_low[0], last - q_low[1]), 0.0, NEG)
        return low_mask, high_mask

    def all_masks():
        for t in range(4):
            s.mlo[t], s.mhi[t] = masks(peers[t])

    def keys_of(src, h):
        return s.kv[src, h, 0:256, :], s.kv[src, h, 256:512, :]

    def attend(groups, h, fresh=False):
        for half in range(2):
            at = 2 * h + half
            qs = s.q[h, 256 * half:256 * half + 256, :]
            tiles = []
            for src, mlo, mhi in groups:
                klo, khi = keys_of(src, h)
                if half == 0:
                    tiles.append((klo, dg(klo, qs, 1, 1) + mlo[...]))
                else:
                    tiles.append((klo, dg(klo, qs, 1, 1)))
                    tiles.append((khi, dg(khi, qs, 1, 1) + mhi[...]))
            now = None if fresh else s.m[at]
            old = now
            for _, sc in tiles:
                top = jnp.max(sc, axis=0, keepdims=True)
                now = top if now is None else jnp.maximum(now, top)
            total = value = None
            for k, sc in tiles:
                e = jnp.exp(sc - now)
                part = jnp.sum(e, axis=0, keepdims=True)
                total = part if total is None else total + part
                part = dg(k, e.astype(BF), 0, 0)
                value = part if value is None else value + part
            if fresh:
                s.l[at] = total
                s.acc[at] = value
            else:
                f = jnp.exp(old - now)
                s.l[at] = s.l[at] * f + total
                s.acc[at] = s.acc[at] * f + value
            s.m[at] = now

    low = lax.broadcasted_iota(jnp.int32, (256, 128), 1) < HEAD
    low_s = lax.broadcasted_iota(jnp.int32, (BLK, 128), 1) < HEAD

    def settle(h):
        outs = []
        for half in range(2):
            rows = pl.ds(256 * half, 256)
            outs.append(jnp.transpose(s.acc[2 * h + half] / s.l[2 * h + half]))
            s.attp[h, rows, :] = outs[half].astype(BF)
            s.m[2 * h + half] = s.m[2 * h + half] + jnp.log(s.l[2 * h + half])
        if h < nh - 1:
            s.ab[z, h] = jnp.where(low, roll64(outs[0]), outs[1]).astype(BF)
        else:
            for place, half in ((0, 1), (1, 0)):
                v = outs[half]
                s.ab[z, h, BLK * place:BLK * place + BLK, :] = jnp.where(
                    low_s, roll64(v[0:BLK]), v[BLK:256]).astype(BF)

    ab_line = Gather(lambda i, u: s.ab.at[i, u], nh - 1)
    ac_line = Gather(lambda i, u: s.ab.at[i, nh - 1, pl.ds(BLK * u, BLK)], 2)

    sum1 = Sum(s.p1, s.r1, s.l1, s.h)
    sum2 = Sum(s.p2, s.r2, s.l2, s.yo, s.mo)
    sum3 = Sum(s.p3, s.r3, s.l3, s.yg, s.mg, sum1.rl)
    s.vsum[...] = jnp.zeros((16, D), F32)

    def upstream():
        swapped(s.cot, sx + 2)
        loads[ID.pw].wait()
        for half in range(2):
            s.ga[256 * half:256 * half + 256, :] = dg(
                s.cot[4 * half:4 * half + 4].reshape(256, D), s.pw[...], 1, 1)

    zeros = jnp.zeros((HEAD, D), BF)

    def pad_own():
        mine = s.wo[z].reshape(nh * HEAD, D)
        for h in range(nh):
            s.wopad[BLK * h:BLK * h + HEAD, :] = zeros
            s.wopad[BLK * h + HEAD:BLK * h + BLK, :] = mine[HEAD * h:HEAD * h + HEAD]

    def pad_all():
        for t in range(1, T):
            for u in range(2):
                arrived(wo_at(lax.rem(z + t, T), u, o), swo + T * u + lax.rem(z + t, T))
        for t in range(T):
            w = s.wo[t].reshape(nh * HEAD, D)
            for h in range(nh):
                part = w[HEAD * h:HEAD * h + HEAD]
                s.wolo[h, t, 0:HEAD, :] = part
                s.wolo[h, t, HEAD:BLK, :] = zeros
                s.wohi[h, t, 0:HEAD, :] = zeros
                s.wohi[h, t, HEAD:BLK, :] = part

    def early_mix():
        for half, w in ((1, s.wohi), (0, s.wolo)):
            total = None
            for h in range(nh - 1):
                a = jnp.concatenate([s.ab[t, h] for t in range(T)], axis=1)
                part = dg(a, w[h].reshape(T * BLK, D), 1, 0)
                total = part if total is None else total + part
            s.pre[256 * half:256 * half + 256, :] = total

    def group(t):
        return peers[t], s.mlo.at[t], s.mhi.at[t]

    def own_keys():
        all_masks()
        for h in range(nh):
            attend([group(0)], h, True)

    def near_keys(h):
        attend([group(1), group(2)], h)

    def far_keys(h):
        kv_far(h)
        attend([group(3)], h)
        settle(h)
        if h < nh - 1:
            ab_line.start(h)
        else:
            ac_line.start(0)
            ac_line.start(1)

    def step_a():
        kv_relay(0)
        kv_go(1, 1)

    def step_b():
        kv_rest(0)
        near_keys(0)

    def step_c():
        kv_relay(1)
        kv_go(2, 0)
        kv_go(2, 1)

    def step_d():
        kv_rest(1)
        near_keys(1)

    def step_e():
        kv_rest(2)
        near_keys(2)

    def whole():
        def one_group(src, fresh):
            s.mlo[0], s.mhi[0] = masks(src)
            for h in range(nh):
                attend([(src, s.mlo.at[0], s.mhi.at[0])], h, fresh)

        one_group(g, True)
        for t in range(1, NG):
            arrived(s.kv.at[sources[t]], skv + t)

        def rest(t, _):
            one_group(lax.rem(g + t, NG), False)
            return 0

        lax.fori_loop(1, NG, rest, 0)
        for h in range(nh):
            settle(h)

    def pads():
        pad_own()
        pad_all()

    g2 = g2_ref[...].reshape(1, -1)
    b2 = b2_ref[...].reshape(1, -1)
    ob = ob_ref[...].reshape(1, -1)
    fcb = fcb_ref[...].reshape(1, -1)
    pb = pb_ref[...].reshape(1, -1)

    def feed(half, total):
        place = 1 - half
        a = jnp.concatenate([s.ab[t, nh - 1, BLK * place:BLK * place + BLK, :] for t in range(T)], axis=1)
        base = 256 * half
        for k, w in ((0, s.wolo), (1, s.wohi)):
            s.pre[base + BLK * k:base + BLK * k + BLK, :] += dg(a, w[nh - 1].reshape(T * BLK, D), 1, 0)

        def norm2(i, _):
            j = 4 * half + i
            rows = pl.ds(pl.multiple_of(base + i * 64, 64), 64)
            x = s.x[j].astype(F32) + s.pre[rows, :] + ob
            s.hid[j] = x
            n, _inv = normed(x)
            s.act2[rows, :] = (n * g2 + b2).astype(BF)
            return 0

        lax.fori_loop(0, 4, norm2, 0)
        part = pl.ds(base, 256)
        s.pre[part, :] = dg(s.act2[part, :], s.fc[...], 1, 0)

        def gelu(i, total):
            rows = pl.ds(pl.multiple_of(base + i * 32, 32), 32)
            v = s.pre[rows, :] + fcb
            square = v * v
            th = jnp.tanh(C0 * (v + C1 * square * v))
            one = 1.0 + th
            s.actd[rows, :] = (0.5 * v * one).astype(BF)
            slope = 0.5 * one + (0.5 * v) * (1.0 - th * th) * (C0 * (1.0 + 3.0 * C1 * square))
            grad = slope * s.ga[rows, :]
            s.gpre[rows, :] = grad.astype(BF)
            return total + fold8(grad)

        total = lax.fori_loop(0, 8, gelu, total)
        s.p1[4 * half:4 * half + 4] = dg(s.gpre[part, :], s.fc[...], 1, 1).astype(BF).reshape(4, 64, D)
        return total

    bias = []

    def feed1():
        loads[ID.fc].wait()
        bias.append(feed(1, jnp.zeros((8, F), F32)))
        for u in range(SUB):
            sum1.begin(u)

    def feed0():
        s.vsum[8:9, :] = jnp.sum(feed(0, bias[0]), axis=0, keepdims=True)
        for u in range(SUB, U):
            sum1.begin(u)

    sw1 = new(2)

    def weight(dst, index, lhs, rhs):
        for i in range(3):
            part = dg(lhs[:, 256 * i:256 * i + 256], rhs, 0, 0).astype(BF)
            lo, hi = 256 * i, 256 * i + 256
            for qd in range(NG):
                a, b = max(lo, qd * Q1), min(hi, qd * Q1 + Q1)
                if a < b:
                    dst[index, qd, a - qd * Q1:b - qd * Q1, :] = part[a - lo:b - lo]

    def add_into(buf, index, extra):
        def body(i, _):
            buf[index, i] = (buf[index, i].astype(F32) + extra[i].astype(F32)).astype(BF)
            return 0

        lax.fori_loop(0, NG, body, 0)

    def weights_a():
        weight(s.w1, 0, s.actd, s.cot[...].reshape(N, D))

    def weights_a2():
        weight(s.w1, 1, s.act2, s.gpre[...])
        send(s.w1.at[o], s.w1r, sw1, (mate, z))

    def plane(part, land, near, whole, size):
        half = size // 2

        def of(buf):
            return lambda i, k: buf.at[c, i] if k is None else buf.at[c, i, pl.ds(half * k, half)]

        def cut(to, k):
            rows = pl.ds(half * k, half)
            part[c, to, rows, :] = (part[c, to, rows, :].astype(F32) + land[k].astype(F32)).astype(BF)

        total = PlaneSum(of(part), cut, lambda k: land.at[k], lambda t: near.at[t])
        share = PlaneGather(of(whole))

        def finish():
            total.arrived()
            step = size // 3

            def body(i, _):
                rows = pl.ds(pl.multiple_of(i * step, step), step)
                v = part[c, g, rows, :].astype(F32)
                for t in got:
                    v = v + near[t, rows, :].astype(F32)
                whole[c, g, rows, :] = v.astype(BF)
                return 0

            lax.fori_loop(0, 3, body, 0)
            share.start()

        return total, share, finish

    got = [1, 2] if NG == 4 else list(range(1, NG))
    total1, share1, finish1 = plane(s.w1, s.w1a, s.w1s, s.w1f, Q1)
    total2, share2, finish2 = plane(s.w2, s.w2a, s.w2s, s.w2f, Q2)

    def weights_b():
        arrived(s.w1r, sw1)
        add_into(s.w1, c, s.w1r)
        total1.far()

    def out_partial():
        for half in range(2):
            base = 256 * half
            s.p2[4 * half:4 * half + 4] = dg(
                s.actd[base:base + 256, :], s.pw[...], 1, 0).astype(BF).reshape(4, 64, D)

    def spans(u):
        half = 1 if u < SUB else 0
        step = min(RU, 32)
        return half, 4 * half + z, [pl.ds(RU * (u % SUB) + step * i, step) for i in range(RU // step)]

    def back2(u):
        sum1.last(u)
        half, index, parts = spans(u)
        sums = [jnp.zeros((8, D), F32)] * 4
        for rows in parts:
            n, inv = normed(s.hid[index, rows, :])
            grad = sum1.total(index, rows)
            up = s.cot[index, rows, :].astype(F32)
            qg = grad * g2
            gh = up + inv * (qg - jnp.mean(qg, axis=-1, keepdims=True)
                             - n * jnp.mean(qg * n, axis=-1, keepdims=True))
            s.gh[half, rows, :] = gh
            s.h[index, rows, :] = gh.astype(BF)
            for k, part in enumerate((grad * n, grad, gh, up)):
                sums[k] = sums[k] + fold8(part)
        sum1.gather(u)
        for k in range(4):
            s.vsum[2 + k:3 + k, :] += jnp.sum(sums[k], axis=0, keepdims=True)

    def slopes(half):
        rows = pl.ds(256 * half, 256)
        grads = dg(s.h[4 * half:4 * half + 4].reshape(256, D), s.wopad[...], 1, 1)
        for h in range(nh):
            d = grads[:, 128 * h:128 * h + 128].astype(BF)
            s.do[h, rows, :] = d
            both = d.astype(F32) * s.attp[h, rows, :].astype(F32)
            s.delta[2 * h + half] = jnp.sum(jnp.transpose(both), axis=0, keepdims=True)

    def tile(k, h, half, mask):
        qs = s.q[h, 256 * half:256 * half + 256, :]
        ds_ = s.do[h, 256 * half:256 * half + 256, :]
        sc = dg(k, qs, 1, 1)
        if mask is not None:
            sc = sc + mask[...]
        p = jnp.exp(sc - s.m[2 * h + half])
        d = p * (dg(k, ds_, 1, 1) - s.delta[2 * h + half])
        p = p.astype(BF)
        d = d.astype(BF)
        return d, dg(d, qs, 1, 0) + dg(p, ds_, 1, 0)

    def back_high(src, mhi, fresh):
        for h in range(nh):
            _, khi = keys_of(src, h)
            d3, k3 = tile(khi, h, 1, mhi)
            s.dk[src, h, 256:512, :] = k3.astype(BF)
            if fresh:
                s.acc[2 * h + 1] = dg(khi, d3, 0, 0)
            else:
                s.acc[2 * h + 1] += dg(khi, d3, 0, 0)

    def back_mid(src, t):
        for h in range(nh):
            klo, _ = keys_of(src, h)
            d2, k2 = tile(klo, h, 1, None)
            s.dkf[t, h] = k2
            s.acc[2 * h + 1] += dg(klo, d2, 0, 0)

    def back_low(src, t, mlo, fresh):
        for h in range(nh):
            klo, _ = keys_of(src, h)
            d1, k1 = tile(klo, h, 0, mlo)
            s.dk[src, h, 0:256, :] = (s.dkf[t, h] + k1).astype(BF)
            if fresh:
                s.acc[2 * h] = dg(klo, d1, 0, 0)
            else:
                s.acc[2 * h] += dg(klo, d1, 0, 0)

    def key_sum(half):
        rows = pl.ds(256 * half, 256)

        def part(i, k):
            return s.dk.at[i, :, rows if k is None else pl.ds(256 * half + BLK * k, BLK)]

        def cut(to, k):
            some = pl.ds(256 * half + BLK * k, BLK)
            for h in range(nh):
                s.dk[to, h, some, :] = (s.dk[to, h, some, :].astype(F32) + s.dka[half, k, h].astype(F32)).astype(BF)

        return PlaneSum(part, cut, lambda k: s.dka.at[half, k], lambda t: s.dkr.at[t, :, rows])

    keys = [key_sum(0), key_sum(1)]

    def finish_output(u):
        sum2.last(u)
        half, index, parts = spans(u)
        for rows in parts:
            s.yo[index, rows, :] = (s.hid[index, rows, :] + sum2.total(index, rows) + pb).astype(BF)
        sum2.gather(u)

    col = [jnp.zeros((1, 128), F32) for _ in range(5)]

    def collect(half):
        keys[half].arrived()
        rows = pl.ds(256 * half, 256)
        dq = [jnp.transpose(s.acc[2 * h + half]) * 0.125 for h in range(nh)]
        dkv = []
        for h in range(nh):
            total = s.dk[g, h, rows, :].astype(F32)
            for t in got:
                total = total + s.dkr[t, h, rows, :].astype(F32)
            dkv.append(total)
        tiles = [
            jnp.where(low, dq[0], roll64(dq[1])),
            jnp.where(low, dq[2], roll64(dkv[0])),
            jnp.where(low, dkv[1], roll64(dkv[2])),
            jnp.where(low, roll64(dkv[0]), dkv[1]),
            jnp.where(low, roll64(dkv[2]), 0.0),
        ]
        for j in range(5):
            col[j] = col[j] + jnp.sum(tiles[j], axis=0, keepdims=True)
            s.gn[rows, 128 * j:128 * j + 128] = tiles[j].astype(BF)
        back = dg(s.gn[rows, :], s.wqt[...], 1, 0)
        s.p3[4 * half:4 * half + 4] = back.astype(BF).reshape(4, 64, D)
        s.ga[rows, 0:D] = back
        for u in range(SUB) if half == 1 else range(SUB, U):
            sum3.begin(u)

    def put2(first, value, rows):
        done = 0
        while done < rows:
            at, off = divmod(first + done, Q2)
            n = min(Q2 - off, rows - done)
            s.w2[at // NG, at % NG, off:off + n, :] = value[done:done + n].astype(BF)
            done += n

    sw2 = new(2)

    def attention_weight():
        for half in range(2):
            rows = pl.ds(256 * half, 256)
            a = [s.attp[h, rows, :].astype(F32) for h in range(nh)]
            s.attn[rows, 0:128] = jnp.where(low, roll64(a[0]), a[1]).astype(BF)
            s.attn[rows, 128:256] = jnp.where(low, roll64(a[2]), 0.0).astype(BF)
        gout = dg(s.attn[...], s.h[...].reshape(N, D), 0, 0)
        put2(3 * nh * HEAD, gout, nh * HEAD)

    def do_high():
        slopes(1)
        back_high(peers[3], s.mhi.at[3], True)
        keys[1].far()

    def do_low():
        slopes(0)
        back_low(peers[3], 3, s.mlo.at[3], True)
        keys[0].far()

    def own_hi():
        back_high(g, s.mhi.at[0], False)
        back_mid(g, 0)

    def whole_part():
        slopes(0)
        slopes(1)
        for i in range(2 * nh):
            s.acc[i] = jnp.zeros((128, 256), F32)

        def rest_back(t, _):
            src = lax.rem(g + t, NG)
            s.mlo[0], s.mhi[0] = masks(src)
            back_high(src, s.mhi.at[0], False)
            back_mid(src, 0)
            back_low(src, 0, s.mlo.at[0], False)
            return 0

        lax.fori_loop(0, NG, rest_back, 0)
        for half in (1, 0):
            keys[half].near()

    def weights_c():
        for j in range(5):
            s.vsum[9:10, 128 * j:128 * j + 128] = col[j]
        act1 = s.act1[...].reshape(N, D)
        for j in range(5):
            n = min(128, 3 * nh * HEAD - 128 * j)
            put2(128 * j, dg(s.gn[:, 128 * j:128 * j + 128], act1, 0, 0), n)
        send(s.w2.at[o], s.w2r, sw2, (mate, z))

    def weights_d():
        arrived(s.w2r, sw2)
        add_into(s.w2, c, s.w2r)
        total2.far()

    def back1(u):
        sum3.last(u)
        half, index, parts = spans(u)
        for rows in parts:
            n, inv = normed(s.x[index, rows, :].astype(F32))
            qg = sum3.total(index, rows) * g1
            gx = s.gh[half, rows, :] + inv * (qg - jnp.mean(qg, axis=-1, keepdims=True)
                                              - n * jnp.mean(qg * n, axis=-1, keepdims=True))
            s.yg[index, rows, :] = gx.astype(BF)
        sum3.gather(u)

    def norm_sums():
        def body(i, sums):
            n, _inv = normed(s.x[i].astype(F32))
            grad = s.ga[pl.ds(pl.multiple_of(i * 64, 64), 64), 0:D]
            return sums[0] + fold8(grad * n), sums[1] + fold8(grad)

        sums = lax.fori_loop(0, 8, body, (z8, z8))
        for k in range(2):
            s.vsum[k:k + 1, :] = jnp.sum(sums[k], axis=0, keepdims=True)
        s.vz[z] = s.vsum[...].astype(BF)
        v_line.start(0)

    z8 = jnp.zeros((8, D), F32)
    v_line = Direct(lambda i, u: s.vz.at[i], 1)
    svc = new(R)
    copies = []

    def give(src, dst):
        copy = pltpu.make_async_copy(src, dst, s.ls.at[6 + len(copies)])
        copy.start()
        copies.append(copy)

    def give_rows(whole, landing, out, halves=(0, 1)):
        for k in halves:
            give(whole.at[pl.ds(4 * k + 2 * c, 2)], out.at[k, c])
            give(landing.at[k], out.at[k, o])

    def outputs_a():
        share1.arrived()
        send(s.w1f.at[c], s.w1f.at[c], sw1 + 1, (mate, z))

    def outputs_b():
        arrived(s.w1f.at[o], sw1 + 1)
        give(s.w1f, w1_out)

    def outputs_o():
        sum2.handed(range(U))
        give_rows(s.yo, s.mo, fo_out)

    def outputs_c():
        share2.arrived()
        send(s.w2f.at[c], s.w2f.at[c], sw2 + 1, (mate, z))

    def give_v():
        for t in range(1, R):
            arrived(s.vc.at[lax.rem(r + R - t, R)], svc + t)
        total = s.vc[0].astype(F32)
        for t in range(1, R):
            total = total + s.vc[t].astype(F32)
        s.vsum[...] = total
        give(s.vsum, v_out)

    def give_w2():
        arrived(s.w2f.at[o], sw2 + 1)
        give(s.w2f, w2_out)

    def give_hi():
        sum3.handed(range(SUB))
        give_rows(s.yg, s.mg, fg_out, (1,))

    def small_sums():
        upper = s.vz[0, 0:8, :].astype(F32)
        for t in range(1, T):
            upper = upper + s.vz[t, 0:8, :].astype(F32)
        s.vc[r] = jnp.concatenate([upper, s.vsum[8:16, :]], axis=0).astype(BF)
        for t in range(1, R):
            send(s.vc.at[r], s.vc.at[r], svc + t, (lax.rem(r + t, R), z))

    def go():
        if NG == 4:
            kv_go(0, 0)
            kv_go(0, 1)
            kv_go(1, 0)
        else:
            for t in range(1, NG):
                send(s.kv.at[g], s.kv.at[g], skv + t, (2 * peers[t] + c, z))
        loads[ID.cot].wait()
        swap(s.cot_raw, 1, s.cot, sx + 2)

    steps = {
        ID.go: go, ID.pads: pads, ID.mix: early_mix, ID.feed1: feed1, ID.feed0: feed0, ID.weights_a: weights_a,
        ID.weights_a2: weights_a2, ID.out_partial: out_partial, ID.weights_b: weights_b, ID.near_w1: total1.near,
        ID.collect1: functools.partial(collect, 1), ID.collect0: functools.partial(collect, 0), ID.finish_w1: finish1,
        ID.aw: attention_weight, ID.weights_c: weights_c, ID.weights_d: weights_d, ID.near_w2: total2.near,
        ID.relay_w1: share1.relay, ID.finish_w2: finish2, ID.relay_w2: share2.relay, ID.pair_w1: outputs_a,
        ID.give_w1: outputs_b, ID.give_o: outputs_o, ID.sums: small_sums, ID.norm_sums: norm_sums, ID.pair_w2: outputs_c, ID.give_v: give_v, ID.give_w2: give_w2, ID.give_hi: give_hi,
        ID.upstream: upstream,
    }
    for u in range(U):
        steps[ID.n2_, u] = functools.partial(back2, u)
        for d in DS:
            steps[ID.begin_out, u, d] = functools.partial(sum2.begin, u, (d,))
        steps[ID.out_, u] = functools.partial(finish_output, u)
        steps[ID.n1_, u] = functools.partial(back1, u)
    if NG == 4:
        steps.update({
            ID.own: own_keys, ID.relay0: step_a, ID.near0: step_b, ID.relay1: step_c,
            ID.far0: functools.partial(far_keys, 0), ID.near1: step_d, ID.relay2: functools.partial(kv_relay, 2),
            ID.far1: functools.partial(far_keys, 1), ID.near2: step_e, ID.far2: functools.partial(far_keys, 2),
            ID.high: do_high, ID.high2: functools.partial(back_high, peers[2], s.mhi.at[2], False),
            ID.high3: functools.partial(back_high, peers[1], s.mhi.at[1], False),
            ID.near_k1a: functools.partial(keys[1].near, (0,)), ID.near_k1b: functools.partial(keys[1].near, (1,)),
            ID.mid3: functools.partial(back_mid, peers[3], 3), ID.low: do_low,
            ID.mid2: functools.partial(back_mid, peers[2], 2), ID.mid1: functools.partial(back_mid, peers[1], 1),
            ID.low2: functools.partial(back_low, peers[2], 2, s.mlo.at[2], False),
            ID.low3: functools.partial(back_low, peers[1], 1, s.mlo.at[1], False),
            ID.near_k0a: functools.partial(keys[0].near, (0,)), ID.near_k0b: functools.partial(keys[0].near, (1,)),
            ID.own_hi: own_hi, ID.own_lo: functools.partial(back_low, g, 0, s.mlo.at[0], False),
        })
    else:
        steps.update({
            ID.own: whole, ID.far0: lambda: ab_line.start(0), ID.far1: lambda: ab_line.start(1),
            ID.far2: lambda: (ac_line.start(0), ac_line.start(1)), ID.low: whole_part,
        })
    jobs, marks = timetable(U, T)
    timeline, _ = simulate(T, jobs, marks, LAT)
    emit(T, z, timeline, jobs, marks,
         {ID.wo: wo_line, ID.ab: ab_line, ID.ac: ac_line, ID.ga2: sum1, ID.out: sum2, ID.ga1: sum3, ID.small: v_line}, steps, flush)

    sum3.handed(range(SUB, U))
    give_rows(s.yg, s.mg, fg_out, (0,))
    flush(True)
    assert max(v for k, v in most.items() if k != ID.common) + SPLIT <= (SENDS if NG == 4 else 200)
    assert most[ID.common] <= SPLIT and ids[0] <= (ARRIVALS if NG == 4 else 400)
    for copy in copies:
        copy.wait()


def finish_kernel(R, pos_ref, seq_ref, rank_ref, w1_hbm, w2_hbm, fo_hbm, fg_hbm, v_hbm, out_hbm, gt_hbm,
                  ln1g_ref, ln1b_ref, gq_hbm, gqv_ref, go_hbm, ob_ref, ln2g_ref, ln2b_ref, gf_hbm, fb_ref,
                  gp_hbm, pb_ref, w1_in, w2_in, fo_in, fg_in, v_in, w1_wide, w2_wide, sems, back):
    parts = 2
    D = w2_in.shape[0]
    step = D // parts
    reads = []

    def read(src, dst):
        copy = pltpu.make_async_copy(src, dst, sems.at[len(reads)])
        copy.start()
        reads.append(copy)

    for k in range(parts):
        rows = pl.ds(step * k, step)
        for i in range(2):
            read(w1_hbm.at[i, rows], w1_in.at[i, rows])
        read(w2_hbm.at[rows], w2_in.at[rows])
    read(v_hbm, v_in)
    read(fo_hbm, fo_in)
    read(fg_hbm, fg_in)
    writes = []

    def write(src, dst):
        copy = pltpu.make_async_copy(src, dst, back.at[len(writes)])
        copy.start()
        writes.append(copy)

    for k in range(parts):
        rows = pl.ds(step * k, step)
        for i, dst in enumerate((gp_hbm, gf_hbm)):
            reads[3 * k + i].wait()
            w1_wide[i, rows] = w1_in[i, rows].astype(F32)
            write(w1_wide.at[i, rows], dst.at[rows])
        reads[3 * k + 2].wait()
        w2_wide[rows] = w2_in[rows].astype(F32)
        low, most = step * k, min(step * k + step, gq_hbm.shape[0])
        write(w2_wide.at[pl.ds(low, most - low)], gq_hbm.at[pl.ds(low, most - low)])
    write(w2_wide.at[pl.ds(most, D - most)], go_hbm)
    for copy in reads[3 * parts:]:
        copy.wait()
    for b in range(4):
        at = 4 * rank_ref[0] + b
        high = jnp.where(pos_ref[at] < R, 0, 1)
        write(fo_in.at[high, seq_ref[at]], out_hbm.at[pl.ds(BLK * b, BLK)])
        write(fg_in.at[high, seq_ref[at]], gt_hbm.at[pl.ds(BLK * b, BLK)])
    for ref, k in ((ln1g_ref, 0), (ln1b_ref, 1), (ln2g_ref, 2), (ln2b_ref, 3), (ob_ref, 4), (pb_ref, 5),
                   (fb_ref, 8)):
        ref[...] = v_in[k:k + 1, :].reshape(-1)
    gqv_ref[0:1, :] = v_in[9:10, 0:192]
    gqv_ref[1:2, :] = v_in[9:10, 384:576]
    for copy in writes:
        copy.wait()


def per_device(R, T, tokens, cotangent, block_pos, block_seq, ln1_gain, ln1_bias, qkv_weight, qv_bias,
               out_weight, out_bias, ln2_gain, ln2_bias, fc_weight, fc_bias, proj_weight, proj_bias):
    D = tokens.shape[1]
    F = fc_weight.shape[1]
    local = qkv_weight.shape[2]
    nh = local // HEAD
    NG = R // 2
    sizes = scratch_list(R, T, D, F, nh)
    names = list(sizes)
    row = lambda v: v
    wqt = jnp.transpose(qkv_weight, (1, 2, 0)).reshape(3 * local, D)
    sm = pl.BlockSpec(memory_space=pltpu.SMEM)
    vm = pl.BlockSpec(memory_space=pltpu.VMEM)
    hb = pl.BlockSpec(memory_space=pl.ANY)
    w1, w2, fo, fg, vs = pl.pallas_call(
        functools.partial(layer_kernel, R, T, D, F, nh, names),
        out_shape=(
            jax.ShapeDtypeStruct((2, NG, D // NG, D), BF),
            jax.ShapeDtypeStruct((2, NG, D // 2 // NG, D), BF),
            jax.ShapeDtypeStruct((2, 2, 2, 64, D), BF),
            jax.ShapeDtypeStruct((2, 2, 2, 64, D), BF),
            jax.ShapeDtypeStruct((16, D), F32),
        ),
        in_specs=[sm, sm, hb, hb, vm, vm, hb, vm, hb, vm, vm, vm, hb, vm, hb, vm],
        out_specs=(hb, hb, hb, hb, hb),
        scratch_shapes=list(sizes.values()),
        compiler_params=pltpu.CompilerParams(
            collective_id=0, has_side_effects=True, vmem_limit_bytes=67043328),
        name="layer",
    )(block_pos, block_seq, tokens.reshape(8, 64, D), cotangent.reshape(8, 64, D), row(ln1_gain),
      row(ln1_bias), wqt, qv_bias, out_weight.reshape(2, local // 2, D), row(out_bias), row(ln2_gain), row(ln2_bias), fc_weight,
      row(fc_bias), proj_weight, row(proj_bias))

    rank = lax.axis_index("ctx").astype(jnp.int32).reshape(1)
    vec = jax.ShapeDtypeStruct((D,), F32)
    outs = pl.pallas_call(
        functools.partial(finish_kernel, R),
        out_shape=(
            jax.ShapeDtypeStruct((4 * BLK, D), BF),
            jax.ShapeDtypeStruct((4 * BLK, D), BF),
            vec, vec,
            jax.ShapeDtypeStruct((3 * local, D), F32),
            jax.ShapeDtypeStruct((2, local), F32),
            jax.ShapeDtypeStruct((local, D), F32),
            vec, vec, vec,
            jax.ShapeDtypeStruct((D, F), F32),
            vec,
            jax.ShapeDtypeStruct((F, D), F32),
            vec,
        ),
        in_specs=[sm, sm, sm, hb, hb, hb, hb, hb],
        out_specs=(hb, hb, vm, vm, hb, vm, hb, vm, vm, vm, hb, vm, hb, vm),
        scratch_shapes=[
            pltpu.VMEM((2, D, D), BF), pltpu.VMEM((D, D), BF), pltpu.VMEM((2, 2, BLK, D), BF),
            pltpu.VMEM((2, 2, BLK, D), BF), pltpu.VMEM((16, D), F32), pltpu.VMEM((2, D, D), F32),
            pltpu.VMEM((D, D), F32), pltpu.SemaphoreType.DMA((9,)), pltpu.SemaphoreType.DMA((15,)),
        ],
        name="finish",
    )(block_pos, block_seq, rank, w1.reshape(2, D, D), w2.reshape(D, D),
      fo.reshape(2, 2, BLK, D), fg.reshape(2, 2, BLK, D), vs)
    (output, grad_tokens, ln1g, ln1b, gq, gqv, go, ob, ln2g, ln2b, gf, fb, gp, pb) = outs
    flat = lambda v: v
    return (output, grad_tokens, flat(ln1g), flat(ln1b),
            jnp.transpose(gq.reshape(3, local, D), (2, 0, 1)), gqv, go, flat(ob), flat(ln2g), flat(ln2b),
            gf, flat(fb), gp, flat(pb))


def solution(mesh):
    R = mesh.shape["ctx"]
    T = mesh.shape["tp"]
    return jax.shard_map(
        functools.partial(per_device, R, T),
        mesh=mesh,
        in_specs=(
            P("ctx", None), P("ctx", None), P(), P(), P(), P(), P(None, None, "tp"), P(None, "tp"),
            P("tp", None), P(), P(), P(), P(None, "tp"), P("tp"), P("tp", None), P(),
        ),
        out_specs=(
            P("ctx", None), P("ctx", None), P(), P(), P(None, None, "tp"), P(None, "tp"), P("tp", None),
            P(), P(), P(), P(None, "tp"), P("tp"), P("tp", None), P(),
        ),
        check_vma=False,
    )
```
